256 devices in a mesh: group: 2 (over z_lo), dp: 32 (over y, z_hi, core), mp: 4 (over x).
Axes of the slice: x: 4, y: 4, z: 8 (z_hi: 4, z_lo: 2; z = z_hi * 2 + z_lo), core: 2. Of those that a mesh axis runs over, the one named last changes fastest.
Arguments:
- image_features: bfloat16 [8192, 6144], P('dp', 'mp'), may hold values from -6 to 6
- text_features: bfloat16 [8192, 1024], P('dp', 'mp'), may hold values from -6 to 6
- image_gain: float32 [6144], P('mp'), may hold values from 0.25 to 1.75
- text_gain: float32 [1024], P('mp'), may hold values from 0.25 to 1.75
- image_proj: bfloat16 [6144, 1024], P('mp'), may hold values from -1 to 1
- text_proj: bfloat16 [1024, 1024], P('mp'), may hold values from -1 to 1
- pair: int32 [8192], replicated, may hold values from 0 to 8191, each once
- logit_scale: float32 [], replicated, may hold values from 10 to 100
Outputs:
- embedding_grads: float32 [2, 8192, 1024], P('group', ('dp', 'mp'))
- loss: float32 [], replicated
The draws below stay inside these ranges and needn't reach their ends.
Inputs may be any that keep to these rules, and one draw needn't show every extreme that they name: `pair`: each caption belongs to exactly one image.
All inputs are finite; a program needn't handle non-finite values.
Results may differ from the reference program's by a relative error of at most 0.0061.
Values may be sent and summed in bfloat16 or wider, within the bound.
A program may use at most 128 MiB of HBM per device.

```python
import jax
import jax.numpy as jnp
from jax import lax

D = 6144
DT = 1024
E = 1024
N = 8192


def caption_rows(key):
    base = jax.random.truncated_normal(jax.random.fold_in(key, 11), -6.0, 6.0, (N, DT), jnp.float32)
    return base


def caption_weights(key):
    values = jax.random.truncated_normal(jax.random.fold_in(key, 31), -4.0, 4.0, (DT, E), jnp.float32)
    return values * DT ** (-0.5)


def draw_text_features(key, part):
    return caption_rows(key).astype(jnp.bfloat16)


def draw_image_features(key, part):
    base = jax.random.truncated_normal(jax.random.fold_in(key, 21), -6.0, 6.0, (N, D), jnp.float32)
    return base.astype(jnp.bfloat16)


def draw_text_proj(key, part):
    return caption_weights(key).astype(jnp.bfloat16)


def draw_image_proj(key, part):
    values = jax.random.truncated_normal(jax.random.fold_in(key, 41), -4.0, 4.0, (D, E), jnp.float32) * D ** (-0.5)
    return values.astype(jnp.bfloat16)


def draw_logit_scale(key, part):
    return jax.random.uniform(key, (), jnp.float32, 10.0, 60.0)


def setup_inputs(seed: int = 0) -> dict:
    key_list = jax.random.split(jax.random.key(seed), 9)
    return {
        "image_features": draw_image_features(jax.random.fold_in(key_list[8], 71), 0),
        "text_features": draw_text_features(jax.random.fold_in(key_list[8], 71), 0),
        "image_gain": jnp.clip(1.0 + 0.15 * jax.random.normal(key_list[2], (D,), jnp.float32), 0.25, 1.75),
        "text_gain": jnp.clip(1.0 + 0.15 * jax.random.normal(key_list[3], (DT,), jnp.float32), 0.25, 1.75),
        "image_proj": draw_image_proj(jax.random.fold_in(key_list[8], 71), 0),
        "text_proj": draw_text_proj(jax.random.fold_in(key_list[8], 71), 0),
        "pair": jax.random.permutation(key_list[6], N).astype(jnp.int32),
        "logit_scale": draw_logit_scale(jax.random.fold_in(key_list[8], 71), 0),
    }


epsilon = 1e-05

def encode_tower(features, gain, projection):
    values = features.astype(jnp.float32)
    width = values.shape[1]
    average = lax.optimization_barrier(jnp.sum(values, axis=1)) / width
    spread = lax.optimization_barrier(jnp.sum(values * values, axis=1)) / width - average * average
    inverse = lax.rsqrt(spread + epsilon)
    normed = ((values - average[:, None]) * inverse[:, None] * gain[None, :]).astype(jnp.bfloat16)
    embedded = jnp.dot(normed, projection, preferred_element_type=jnp.float32)
    unit = embedded * lax.rsqrt(lax.optimization_barrier(jnp.sum(embedded * embedded, axis=1, keepdims=True)) + 1e-06)
    return unit.astype(jnp.bfloat16)

def row_totals(own, other, multiplier, span):
    blocks = own.reshape(-1, span, own.shape[1])

    def single(block):
        scores = multiplier * jnp.dot(block, other.T, preferred_element_type=jnp.float32)
        peak = lax.optimization_barrier(jnp.max(scores, axis=1))
        return peak + jnp.log(lax.optimization_barrier(jnp.sum(jnp.exp(scores - peak[:, None]), axis=1)))
    return lax.map(single, blocks).reshape(-1)

def side_grads(own, other, own_total, other_total, pair, multiplier, span, image_side):
    count_all = own.shape[0]
    starts = jnp.arange(count_all // span, dtype=jnp.int32) * span
    column_ids = jnp.arange(count_all, dtype=jnp.int32)

    def single(first):
        block = lax.dynamic_slice_in_dim(own, first, span, 0)
        totals = lax.dynamic_slice_in_dim(own_total, first, span, 0)
        scores = multiplier * jnp.dot(block, other.T, preferred_element_type=jnp.float32)
        row_ids = first + jnp.arange(span, dtype=jnp.int32)
        if image_side:
            matched = jnp.take(pair, row_ids)[:, None] == column_ids[None, :]
        else:
            matched = pair[None, :] == row_ids[:, None]
        flags = matched.astype(jnp.float32)
        target = jnp.sum(flags * scores)
        weights = multiplier * (jnp.exp(scores - totals[:, None]) + jnp.exp(scores - other_total[None, :]) - 2.0 * flags)
        grads = jnp.dot(weights.astype(jnp.bfloat16), other, preferred_element_type=jnp.float32)
        return (grads, target)
    grads, targets = lax.map(single, starts)
    return (grads.reshape(count_all, -1), jnp.sum(targets))

def reference(image_features, text_features, image_gain, text_gain, image_proj, text_proj, pair, logit_scale):
    image_unit = encode_tower(image_features, image_gain, image_proj)
    text_unit = encode_tower(text_features, text_gain, text_proj)
    count_all = image_unit.shape[0]
    span = min(512, count_all)
    image_total = row_totals(image_unit, text_unit, logit_scale, span)
    text_total = row_totals(text_unit, image_unit, logit_scale, span)
    image_grads, image_target = side_grads(image_unit, text_unit, image_total, text_total, pair, logit_scale, span, True)
    text_grads, text_target = side_grads(text_unit, image_unit, text_total, image_total, pair, logit_scale, span, False)
    loss = (jnp.sum(image_total) + jnp.sum(text_total) - image_target - text_target) / (2.0 * count_all)
    return (jnp.stack([image_grads, text_grads]), loss)
```

```python
import functools

import jax
import jax.numpy as jnp
from jax import lax
from jax.experimental import pallas as pl
from jax.experimental.pallas import tpu as pltpu
from jax.sharding import Mesh
from jax.sharding import PartitionSpec as P

DP_MP = ("dp_0", "dp_1", "dp_2", "mp")
DP = ("dp_0", "dp_1", "dp_2")
MESH = pl.DeviceIdType.MESH

X, Y, ZH, ZL, C = 4, 4, 4, 2, 2
Z = ZH * ZL
XY = X * Y
ZC = Z * C
PIECE = 32
HALF = X * PIECE
BLOCK = XY * PIECE
ROWS = 2 * PIECE
SIDE = Z * PIECE

epsilon = 1e-05
f32 = jnp.float32
bf16 = jnp.bfloat16


def dot(a, b, dims=((1,), (0,))):
    return lax.dot_general(a, b, (dims, ((), ())), preferred_element_type=f32)


def each(low, high, step):
    def turn(i, carry):
        step(i)
        return carry

    lax.fori_loop(low, high, turn, 0)


def kernel(
    feat_i, feat_t, gain_i, gain_t, proj_i, proj_t, pair, scale_ref,
    out, loss_out,
    fi, ft, pi, pt, stats, part_i, part_t, own_i, own_t, got_i, got_t,
    ibuf, tbuf, scores, weights, lse_r, lse_c, loss_1, loss_2,
    img_d2d, img_d2d_got, img_send, img_own, img_got, txt_send, txt_got, fin, fin_got,
    load_sem, stat_s, stat_r, rsi_s, rsi_r, rst_s, rst_r,
    agi_s, agi_r, fwd_s, fwd_r, agt_s, agt_r,
    lr_s, lr_r, lc_s, lc_r, l1_s, l1_r, l2_s, l2_r,
    d2d_s, d2d_r, gi_s, gi_r, gt_s, gt_r, fin_s, fin_r,
):
    x, y = lax.axis_index("mp"), lax.axis_index("dp_0")
    zh, c, zl = lax.axis_index("dp_1"), lax.axis_index("dp_2"), lax.axis_index("group")
    z = zh * ZL + zl
    xy = y * X + x
    zc = c * Z + z

    def remote(src, dst, send, recv, **where):
        return pltpu.make_async_remote_copy(
            src_ref=src, dst_ref=dst, send_sem=send, recv_sem=recv,
            device_id=where, device_id_type=MESH,
        )

    def plane(d):
        return {"mp": (x + d % X) % X, "dp_0": (y + d // X) % Y}

    def column(d):
        there = (z + d % Z) % Z
        return {"dp_1": there // ZL, "group": there % ZL, "dp_2": (c + d // Z) % C}

    loads = []
    for k in range(X):
        rows = pl.ds(pl.multiple_of(k * ROWS + zl * PIECE, PIECE), PIECE)
        here = pl.ds(k * PIECE, PIECE)
        loads.append(pltpu.make_async_copy(feat_i.at[rows], fi.at[here], load_sem.at[k]))
        loads.append(pltpu.make_async_copy(feat_t.at[rows], ft.at[here], load_sem.at[X + k]))
    loads_p = [
        pltpu.make_async_copy(proj_t, pt, load_sem.at[2 * X]),
        pltpu.make_async_copy(proj_i, pi, load_sem.at[2 * X + 1]),
    ]
    for copy in loads + loads_p:
        copy.start()

    barrier = pltpu.get_barrier_semaphore()

    def greet_plane(d):
        pl.semaphore_signal(barrier, inc=1, device_id=plane(d), device_id_type=MESH)

    def greet_column(d):
        pl.semaphore_signal(barrier, inc=1, device_id=column(d), device_id_type=MESH)

    each(1, XY, greet_plane)
    each(1, ZC, greet_column)

    for copy in loads:
        copy.wait()
    vi = fi[...].astype(f32)
    vt = ft[...].astype(f32)
    lane = lax.broadcasted_iota(jnp.int32, (HALF, 128), 1)
    packed = jnp.where(lane == 0, jnp.sum(vi, axis=1, keepdims=True), 0.0)
    packed = jnp.where(lane == 1, jnp.sum(vi * vi, axis=1, keepdims=True), packed)
    packed = jnp.where(lane == 2, jnp.sum(vt, axis=1, keepdims=True), packed)
    packed = jnp.where(lane == 3, jnp.sum(vt * vt, axis=1, keepdims=True), packed)
    stats[x] = packed.T[:8]

    pl.semaphore_wait(barrier, XY - 1 + ZC - 1)

    def stat_copy(d):
        return remote(stats.at[x], stats.at[x], stat_s.at[d], stat_r.at[d], mp=(x + d) % X)

    each(1, X, lambda d: stat_copy(d).start())
    each(1, X, lambda d: stat_copy(d).wait_recv())
    total = stats[0] + stats[1] + stats[2] + stats[3]
    total = jnp.concatenate([total] * 16, axis=0).T

    def normed(values, first, width, gain):
        average = total[:, first : first + 1] / width
        inverse = lax.rsqrt(total[:, first + 1 : first + 2] / width - average * average + epsilon)
        return ((values - average) * inverse * gain).astype(bf16)

    def share_copy(d, part, got, send, recv):
        there = (x + d) % X
        rows = pl.ds(pl.multiple_of(there * PIECE, PIECE), PIECE)
        return remote(part.at[rows], got.at[d], send.at[d], recv.at[d], mp=there)

    share_t = lambda d: share_copy(d, part_t, got_t, rst_s, rst_r)
    share_i = lambda d: share_copy(d, part_i, got_i, rsi_s, rsi_r)
    loads_p[0].wait()
    value = dot(normed(ft[...].astype(f32), 2, f32(X * ft.shape[1]), gain_t[...]), pt[...])
    own_t[...] = value
    part_t[...] = value.astype(bf16)
    each(1, X, lambda d: share_t(d).start())
    loads_p[1].wait()
    value = dot(normed(fi[...].astype(f32), 0, f32(X * fi.shape[1]), gain_i[...]), pi[...])
    own_i[...] = value
    part_i[...] = value.astype(bf16)
    each(1, X, lambda d: share_i(d).start())

    def unit_of(own, got):
        value = own[pl.ds(pl.multiple_of(x * PIECE, PIECE), PIECE)]
        for d in range(1, X):
            value = value + got[d].astype(f32)
        return (value * lax.rsqrt(jnp.sum(value * value, axis=1, keepdims=True) + 1e-06)).astype(bf16)

    def slot(buffer, index):
        return buffer.at[pl.ds(pl.multiple_of(index * PIECE, PIECE), PIECE)]

    def text_copy(d):
        mine = slot(tbuf, xy)
        return remote(mine, mine, agt_s.at[d], agt_r.at[d], **plane(d))

    def image_copy(d):
        mine = slot(ibuf, zc)
        return remote(mine, mine, agi_s.at[d], agi_r.at[d], **column(d))

    def forward(d):
        held = slot(ibuf, c * Z + (z + Z - d) % Z)
        return remote(held, held, fwd_s.at[d], fwd_r.at[d], dp_2=1 - c)

    each(1, X, lambda d: share_t(d).wait_recv())
    tbuf[pl.ds(pl.multiple_of(xy * PIECE, PIECE), PIECE)] = unit_of(own_t, got_t)
    each(1, XY, lambda d: text_copy(d).start())
    each(1, X, lambda d: share_i(d).wait_recv())
    ibuf[pl.ds(pl.multiple_of(zc * PIECE, PIECE), PIECE)] = unit_of(own_i, got_i)
    each(1, Z, lambda d: image_copy(d).start())
    forward(0).start()
    for d in (1, 7, 2, 6, 3, 5, 4):
        image_copy(d).wait_recv()
        forward(d).start()
    each(0, Z, lambda d: forward(d).wait_recv())
    each(1, XY, lambda d: text_copy(d).wait_recv())

    scale = scale_ref[0, 0]
    quarters = [pl.ds(k * 128, 128) for k in range(BLOCK // 128)]
    packed = jnp.zeros((128, 128), f32)
    peak_c = None
    for k, rows in enumerate(quarters):
        s = scale * dot(ibuf[rows], tbuf[...], ((1,), (1,)))
        scores[rows] = s
        peak = jnp.max(s, axis=1, keepdims=True)
        log_sum = peak + jnp.log(jnp.sum(jnp.exp(s - peak), axis=1, keepdims=True))
        packed = jnp.where(lane == k, log_sum, packed)
        high = jnp.max(s, axis=0, keepdims=True)
        peak_c = high if peak_c is None else jnp.maximum(peak_c, high)
    lse_r[zc] = packed.T[:8]

    def lse_r_copy(d):
        return remote(lse_r.at[zc], lse_r.at[zc], lr_s.at[d], lr_r.at[d], **column(d))

    def lse_c_copy(d):
        return remote(lse_c.at[xy], lse_c.at[xy], lc_s.at[d], lc_r.at[d], **plane(d))

    each(1, ZC, lambda d: lse_r_copy(d).start())
    sum_c = jnp.zeros((1, BLOCK), f32)
    for rows in quarters:
        sum_c = sum_c + jnp.sum(jnp.exp(scores[rows] - peak_c), axis=0, keepdims=True)
    log_sum = peak_c + jnp.log(sum_c)

    def as_tile(line):
        return jnp.concatenate(
            [line[:, k * 128 : (k + 1) * 128] for k in range(4)] + [jnp.zeros((4, 128), f32)], axis=0
        )

    lse_c[xy] = as_tile(log_sum)
    each(1, XY, lambda d: lse_c_copy(d).start())

    def combined(parts):
        values = parts[...]
        peak = jnp.max(values, axis=0)
        return peak + jnp.log(jnp.sum(jnp.exp(values - peak[None]), axis=0))

    held = pair[pl.ds(y * 16 + x // 2, 8, stride=2), :]
    held = jnp.where(x % 2 == 1, pltpu.roll(held, 64, 1), held)
    held = jnp.concatenate([held] * 16, axis=0).T
    captions = jnp.concatenate([held[:64, h * C + k : h * C + k + 1] for k in range(C) for h in range(ZH)], axis=0)
    j = lax.broadcasted_iota(jnp.int32, (1, BLOCK), 1)
    ids = ((j // 128) * 8 + zh * C + c) * 256 + ((j // PIECE) % X) * ROWS + zl * PIECE + j % PIECE

    each(1, ZC, lambda d: lse_r_copy(d).wait_recv())
    total_r = combined(lse_r)
    turned = jnp.concatenate([total_r] * 16, axis=0).T
    each(1, XY, lambda d: lse_c_copy(d).wait_recv())
    total_c = combined(lse_c)
    line_c = jnp.concatenate([total_c[k : k + 1] for k in range(4)], axis=1)
    target = jnp.zeros((1, BLOCK), f32)
    for k, rows in enumerate(quarters):
        s = scores[rows]
        flags = (captions[k * 128 : (k + 1) * 128] == ids).astype(f32)
        target = target + jnp.sum(flags * s, axis=0, keepdims=True)
        w = scale * (jnp.exp(s - turned[:, k : k + 1]) + jnp.exp(s - line_c) - 2.0 * flags)
        weights[rows] = w.astype(bf16)
    row = lax.broadcasted_iota(jnp.int32, (8, 128), 0)
    shared = jnp.where(row < 4, total_r + total_c, 0.0) * (1.0 / 16)
    loss_1[zc] = shared - 2.0 * as_tile(target)

    def loss_1_copy(d):
        return remote(loss_1.at[zc], loss_1.at[zc], l1_s.at[d], l1_r.at[d], **column(d))

    def loss_2_copy(d):
        return remote(loss_2.at[xy], loss_2.at[xy], l2_s.at[d], l2_r.at[d], **plane(d))

    each(1, ZC, lambda d: loss_1_copy(d).start())

    d2d = remote(img_d2d, img_d2d_got, d2d_s, d2d_r, dp_2=1 - c)
    rows = pl.ds(pl.multiple_of((1 - c) * SIDE, SIDE), SIDE)
    img_d2d[...] = dot(weights[rows], tbuf[...]).astype(bf16)
    d2d.start()

    def grad_t_copy(d):
        there = plane(d)
        piece = slot(txt_send, there["dp_0"] * X + there["mp"])
        return remote(piece, txt_got.at[d], gt_s.at[d], gt_r.at[d], **there)

    for k in range(4):
        cols = pl.ds(k * 128, 128)
        txt_send[cols] = dot(weights[:, cols], ibuf[...], ((0,), (0,))).astype(bf16)
    each(1, XY, lambda d: grad_t_copy(d).start())

    def grad_i_copy(d):
        there = (zh + d) % ZH
        piece = img_send.at[pl.ds(pl.multiple_of(there * ROWS, ROWS), ROWS)]
        gap = (there * ZL + Z - z) % Z
        return remote(piece, img_got.at[gap], gi_s.at[d], gi_r.at[gap], dp_1=there, group=0)

    rows = pl.ds(pl.multiple_of(c * SIDE, SIDE), SIDE)
    value = dot(weights[rows], tbuf[...])
    d2d.wait_recv()
    value = value + img_d2d_got[...].astype(f32)
    img_own[...] = value
    img_send[...] = value.astype(bf16)

    @pl.when(zl == 1)
    def _():
        grad_i_copy(0).start()

    each(1, ZH, lambda d: grad_i_copy(d).start())

    each(1, ZC, lambda d: loss_1_copy(d).wait_recv())
    loss_2[xy] = jnp.sum(loss_1[...], axis=0)
    each(1, XY, lambda d: loss_2_copy(d).start())

    each(1, XY, lambda d: grad_t_copy(d).wait_recv())
    value = txt_send[pl.ds(pl.multiple_of(xy * PIECE, PIECE), PIECE)].astype(f32)
    for d in range(1, XY):
        value = value + txt_got[d].astype(f32)

    last = remote(fin, fin_got, fin_s, fin_r, group=1)

    @pl.when(zl == 0)
    def _():
        fin[...] = value.astype(bf16)
        last.start()
        own = img_own[pl.ds(pl.multiple_of(zh * ROWS, ROWS), ROWS)]

        def arrived(gap):
            remote(img_send.at[:ROWS], img_got.at[gap], gi_s.at[0], gi_r.at[gap], group=0).wait_recv()

        each(1, Z, arrived)
        for gap in range(1, Z):
            own = own + img_got[gap].astype(f32)
        out[0] = own
        last.wait_send()

    @pl.when(zl == 1)
    def _():
        out[0, PIECE:] = value
        grad_i_copy(0).wait_send()
        last.wait_recv()
        out[0, :PIECE] = fin_got[...].astype(f32)

    each(1, XY, lambda d: loss_2_copy(d).wait_recv())
    loss_out[0, 0] = jnp.sum(jnp.sum(loss_2[...], axis=0)) * (1.0 / (2 * XY * BLOCK))

    def sent_x(d):
        stat_copy(d).wait_send()
        share_t(d).wait_send()
        share_i(d).wait_send()
        grad_i_copy(d).wait_send()

    def sent_plane(d):
        text_copy(d).wait_send()
        lse_r_copy(d).wait_send()
        lse_c_copy(d).wait_send()
        loss_1_copy(d).wait_send()
        loss_2_copy(d).wait_send()
        grad_t_copy(d).wait_send()

    each(1, X, sent_x)
    each(1, Z, lambda d: image_copy(d).wait_send())
    each(0, Z, lambda d: forward(d).wait_send())
    each(1, XY, sent_plane)
    d2d.wait_send()


def body(
    image_features, text_features, image_gain, text_gain, image_proj, text_proj, pair, logit_scale
):
    width_i, width_t = image_features.shape[1], text_features.shape[1]
    emb = image_proj.shape[1]
    vmem = pl.BlockSpec(memory_space=pltpu.VMEM)
    smem = pl.BlockSpec(memory_space=pltpu.SMEM)
    hbm = pl.BlockSpec(memory_space=pl.ANY)
    dma = lambda *n: pltpu.SemaphoreType.DMA(n)
    grads, loss = pl.pallas_call(
        kernel,
        out_shape=(
            jax.ShapeDtypeStruct((1, ROWS, emb), f32),
            jax.ShapeDtypeStruct((1, 1), f32),
        ),
        in_specs=[hbm, hbm, vmem, vmem, hbm, hbm, vmem, smem],
        out_specs=(vmem, smem),
        scratch_shapes=[
            pltpu.VMEM((HALF, width_i), bf16),
            pltpu.VMEM((HALF, width_t), bf16),
            pltpu.VMEM((width_i, emb), bf16),
            pltpu.VMEM((width_t, emb), bf16),
            pltpu.VMEM((X, 8, 128), f32),
            pltpu.VMEM((HALF, emb), bf16),
            pltpu.VMEM((HALF, emb), bf16),
            pltpu.VMEM((HALF, emb), f32),
            pltpu.VMEM((HALF, emb), f32),
            pltpu.VMEM((X, PIECE, emb), bf16),
            pltpu.VMEM((X, PIECE, emb), bf16),
            pltpu.VMEM((BLOCK, emb), bf16),
            pltpu.VMEM((BLOCK, emb), bf16),
            pltpu.VMEM((BLOCK, BLOCK), f32),
            pltpu.VMEM((BLOCK, BLOCK), bf16),
            pltpu.VMEM((ZC, 8, 128), f32),
            pltpu.VMEM((XY, 8, 128), f32),
            pltpu.VMEM((ZC, 8, 128), f32),
            pltpu.VMEM((XY, 8, 128), f32),
            pltpu.VMEM((SIDE, emb), bf16),
            pltpu.VMEM((SIDE, emb), bf16),
            pltpu.VMEM((SIDE, emb), bf16),
            pltpu.VMEM((SIDE, emb), f32),
            pltpu.VMEM((Z, ROWS, emb), bf16),
            pltpu.VMEM((BLOCK, emb), bf16),
            pltpu.VMEM((XY, PIECE, emb), bf16),
            pltpu.VMEM((PIECE, emb), bf16),
            pltpu.VMEM((PIECE, emb), bf16),
            dma(2 * X + 2),
            dma(X), dma(X), dma(X), dma(X), dma(X), dma(X),
            dma(Z), dma(Z), dma(Z), dma(Z), dma(XY), dma(XY),
            dma(ZC), dma(ZC), dma(XY), dma(XY), dma(ZC), dma(ZC), dma(XY), dma(XY),
            pltpu.SemaphoreType.DMA, pltpu.SemaphoreType.DMA,
            dma(ZH), dma(Z), dma(XY), dma(XY),
            pltpu.SemaphoreType.DMA, pltpu.SemaphoreType.DMA,
        ],
        compiler_params=pltpu.CompilerParams(
            collective_id=0, has_side_effects=True, vmem_limit_bytes=48 * 1024 * 1024
        ),
        name="contrastive",
    )(
        image_features, text_features, image_gain.reshape(1, -1), text_gain.reshape(1, -1),
        image_proj, text_proj, pair.reshape(-1, 128), logit_scale.reshape(1, 1),
    )
    return grads, loss.reshape(())


def solution(mesh):
    split = Mesh(
        mesh.devices.reshape(mesh.shape["group"], 4, 4, 2, mesh.shape["mp"]),
        ("group", "dp_0", "dp_1", "dp_2", "mp"),
    )
    placed = (P(DP, "mp"), P(DP, "mp"), P("mp"), P("mp"), P("mp", None), P("mp", None), P(), P())
    return jax.shard_map(
        body, mesh=split, in_specs=placed, out_specs=(P("group", DP_MP, None), P()), check_vma=False
    )
```

```python
import functools

import jax
import jax.numpy as jnp
from jax import lax
from jax.experimental import pallas as pl
from jax.experimental.pallas import tpu as pltpu
from jax.sharding import Mesh
from jax.sharding import PartitionSpec as P

DP_MP = ("dp_0", "dp_1", "dp_2", "mp")
DP = ("dp_0", "dp_1", "dp_2")
MESH = pl.DeviceIdType.MESH

X, Y, ZH, ZL, C = 4, 4, 4, 2, 2
Z = ZH * ZL
XY = X * Y
ZC = Z * C
PIECE = 32
HALF = X * PIECE
BLOCK = XY * PIECE
ROWS = 2 * PIECE
SIDE = Z * PIECE

epsilon = 1e-05
f32 = jnp.float32
bf16 = jnp.bfloat16


def dot(a, b, dims=((1,), (0,))):
    return lax.dot_general(a, b, (dims, ((), ())), preferred_element_type=f32)


def each(low, high, step):
    def turn(i, carry):
        step(i)
        return carry

    lax.fori_loop(low, high, turn, 0)


def kernel(
    feat_i, feat_t, gain_i, gain_t, proj_i, proj_t, pair_hbm, scale_ref,
    out, loss_out,
    fi, ft, gi, gt, pair, pi, pt, lhs_i, lhs_t, stats, moments, part_i, part_t, own_i, own_t, got_i, got_t,
    ibuf, tbuf, scores, weights, lse_r, lse_c, loss_1, loss_2,
    img_d2d, img_d2d_got, img_send, img_own, img_got, txt_send, txt_got, fin, fin_got,
    load_sem, stat_s, stat_r, rsi_s, rsi_r, rst_s, rst_r,
    agi_s, agi_r, fwd_s, fwd_r, agt_s, agt_r,
    lr_s, lr_r, lc_s, lc_r, l1_s, l1_r, l2_s, l2_r,
    d2d_s, d2d_r, gi_s, gi_r, gt_s, gt_r, fin_s, fin_r,
):
    x, y = lax.axis_index("mp"), lax.axis_index("dp_0")
    zh, c, zl = lax.axis_index("dp_1"), lax.axis_index("dp_2"), lax.axis_index("group")
    z = zh * ZL + zl
    xy = y * X + x
    zc = c * Z + z

    def remote(src, dst, send, recv, **where):
        return pltpu.make_async_remote_copy(
            src_ref=src, dst_ref=dst, send_sem=send, recv_sem=recv,
            device_id=where, device_id_type=MESH,
        )

    def plane(d):
        return {"mp": (x + d % X) % X, "dp_0": (y + d // X) % Y}

    def column(d):
        there = (z + d % Z) % Z
        return {"dp_1": there // ZL, "group": there % ZL, "dp_2": (c + d // Z) % C}

    loads = []
    for k in range(X):
        rows = pl.ds(pl.multiple_of(k * ROWS + zl * PIECE, PIECE), PIECE)
        here = pl.ds(k * PIECE, PIECE)
        loads.append(pltpu.make_async_copy(feat_i.at[rows], fi.at[here], load_sem.at[k]))
        loads.append(pltpu.make_async_copy(feat_t.at[rows], ft.at[here], load_sem.at[X + k]))
    loads += [
        pltpu.make_async_copy(gain_i, gi, load_sem.at[2 * X + 2]),
        pltpu.make_async_copy(gain_t, gt, load_sem.at[2 * X + 3]),
    ]
    loads_p = [
        pltpu.make_async_copy(proj_t, pt, load_sem.at[2 * X]),
        pltpu.make_async_copy(proj_i, pi, load_sem.at[2 * X + 1]),
    ]
    load_pair = pltpu.make_async_copy(pair_hbm, pair, load_sem.at[2 * X + 4])
    for copy in loads + loads_p + [load_pair]:
        copy.start()

    barrier = pltpu.get_barrier_semaphore()

    def greet_plane(d):
        pl.semaphore_signal(barrier, inc=1, device_id=plane(d), device_id_type=MESH)

    def greet_column(d):
        pl.semaphore_signal(barrier, inc=1, device_id=column(d), device_id_type=MESH)

    each(1, XY, greet_plane)
    each(1, ZC, greet_column)

    for copy in loads:
        copy.wait()
    lane = lax.broadcasted_iota(jnp.int32, (HALF, 128), 1)
    row = lax.broadcasted_iota(jnp.int32, (8, 128), 0)

    def centred(features, gain, lhs):
        values = features[...].astype(f32)
        mean = jnp.sum(values, axis=1, keepdims=True) * (1.0 / values.shape[1])
        squares = jnp.sum(values * values, axis=1, keepdims=True)
        line = jnp.concatenate([gain[k : k + 1, :] for k in range(gain.shape[0])], axis=1)
        lhs[:HALF] = ((values - mean) * line).astype(bf16)
        coarse = line.astype(bf16)
        fine = (line - coarse.astype(f32)).astype(bf16)
        lhs[HALF:] = jnp.concatenate([coarse, fine, jnp.zeros((14, line.shape[1]), bf16)], axis=0)
        return mean, squares

    def lines(row_of_all):
        return jnp.concatenate([row_of_all[:, k * 128 : (k + 1) * 128] for k in range(8)], axis=0)

    def share_copy(d, part, got, send, recv):
        there = (x + d) % X
        rows = pl.ds(pl.multiple_of(there * PIECE, PIECE), PIECE)
        return remote(part.at[rows], got.at[d], send.at[d], recv.at[d], mp=there)

    share_t = lambda d: share_copy(d, part_t, got_t, rst_s, rst_r)
    share_i = lambda d: share_copy(d, part_i, got_i, rsi_s, rsi_r)

    def stat_copy(d):
        return remote(stats.at[x], stats.at[x], stat_s.at[d], stat_r.at[d], mp=(x + d) % X)

    mean_t, squares_t = centred(ft, gt, lhs_t)
    loads_p[0].wait()
    value = dot(lhs_t[...], pt[...])
    own_t[...] = value[:HALF]
    part_t[...] = value[:HALF].astype(bf16)
    stats[x, 16:] = lines(value[HALF : HALF + 1] + value[HALF + 1 : HALF + 2])
    mean_i, squares_i = centred(fi, gi, lhs_i)
    packed = jnp.where(lane == 0, mean_i, 0.0)
    packed = jnp.where(lane == 1, squares_i, packed)
    packed = jnp.where(lane == 2, mean_t, packed)
    packed = jnp.where(lane == 3, squares_t, packed)
    stats[x, :8] = packed.T[:8]
    pl.semaphore_wait(barrier, XY - 1 + ZC - 1)
    for d in (2, 1, 3):
        share_t(d).start()
    loads_p[1].wait()
    value = dot(lhs_i[...], pi[...])
    own_i[...] = value[:HALF]
    part_i[...] = value[:HALF].astype(bf16)
    stats[x, 8:16] = lines(value[HALF : HALF + 1] + value[HALF + 1 : HALF + 2])
    for d in (2, 1, 3):
        stat_copy(d).start()
    for d in (2, 1, 3):
        share_i(d).start()

    each(1, X, lambda d: stat_copy(d).wait_recv())
    turned = jnp.concatenate([stats[k, :8] for k in range(X)] + [jnp.zeros((96, 128), f32)], axis=0).T
    moments[...] = turned
    moment = moments[pl.ds(pl.multiple_of(x * PIECE, PIECE), PIECE)]

    def unit_of(own, got, which, width):
        means = [moment[:, 8 * k + 2 * which : 8 * k + 2 * which + 1] for k in range(X)]
        squares = [moment[:, 8 * k + 2 * which + 1 : 8 * k + 2 * which + 2] for k in range(X)]
        average = (means[0] + means[1] + means[2] + means[3]) * (1.0 / X)
        spread = (squares[0] + squares[1] + squares[2] + squares[3]) / width - average * average
        value = own[pl.ds(pl.multiple_of(x * PIECE, PIECE), PIECE)]
        for d in range(1, X):
            value = value + got[d].astype(f32)
        for k in range(X):
            gained = stats[k, 8 * (1 + which) : 8 * (2 + which)]
            gained = jnp.concatenate([gained[q : q + 1] for q in range(8)], axis=1)
            value = value + (means[k] - average) * gained
        size = jnp.sum(value * value, axis=1, keepdims=True) + 1e-06 * (spread + epsilon)
        return (value * lax.rsqrt(size)).astype(bf16)

    def slot(buffer, index):
        return buffer.at[pl.ds(pl.multiple_of(index * PIECE, PIECE), PIECE)]

    def text_copy(d):
        mine = slot(tbuf, xy)
        return remote(mine, mine, agt_s.at[d], agt_r.at[d], **plane(d))

    def image_copy(d):
        mine = slot(ibuf, zc)
        return remote(mine, mine, agi_s.at[d], agi_r.at[d], **column(d))

    def forward(d):
        held = slot(ibuf, c * Z + (z + Z - d) % Z)
        return remote(held, held, fwd_s.at[d], fwd_r.at[d], dp_2=1 - c)

    each(1, X, lambda d: share_t(d).wait_recv())
    tbuf[pl.ds(pl.multiple_of(xy * PIECE, PIECE), PIECE)] = unit_of(own_t, got_t, 1, f32(X * ft.shape[1]))
    each(1, XY, lambda d: text_copy(d).start())
    each(1, X, lambda d: share_i(d).wait_recv())
    ibuf[pl.ds(pl.multiple_of(zc * PIECE, PIECE), PIECE)] = unit_of(own_i, got_i, 0, f32(X * fi.shape[1]))
    each(1, Z, lambda d: image_copy(d).start())
    forward(0).start()
    for d in (1, 7, 2, 6, 3, 5, 4):
        image_copy(d).wait_recv()
        forward(d).start()
    each(0, Z, lambda d: forward(d).wait_recv())
    each(1, XY, lambda d: text_copy(d).wait_recv())

    scale = scale_ref[0, 0]
    quarters = [pl.ds(k * 128, 128) for k in range(BLOCK // 128)]
    packed = jnp.zeros((128, 128), f32)
    peak_c = None
    for k, rows in enumerate(quarters):
        s = scale * dot(ibuf[rows], tbuf[...], ((1,), (1,)))
        scores[rows] = s
        peak = jnp.max(s, axis=1, keepdims=True)
        log_sum = peak + jnp.log(jnp.sum(jnp.exp(s - peak), axis=1, keepdims=True))
        packed = jnp.where(lane == k, log_sum, packed)
        high = jnp.max(s, axis=0, keepdims=True)
        peak_c = high if peak_c is None else jnp.maximum(peak_c, high)
    lse_r[zc] = packed.T[:8]

    def lse_r_copy(d):
        return remote(lse_r.at[zc], lse_r.at[zc], lr_s.at[d], lr_r.at[d], **column(d))

    def lse_c_copy(d):
        return remote(lse_c.at[xy], lse_c.at[xy], lc_s.at[d], lc_r.at[d], **plane(d))

    each(1, ZC, lambda d: lse_r_copy(d).start())
    sum_c = jnp.zeros((1, BLOCK), f32)
    for rows in quarters:
        sum_c = sum_c + jnp.sum(jnp.exp(scores[rows] - peak_c), axis=0, keepdims=True)
    log_sum = peak_c + jnp.log(sum_c)

    def as_tile(line):
        return jnp.concatenate(
            [line[:, k * 128 : (k + 1) * 128] for k in range(4)] + [jnp.zeros((4, 128), f32)], axis=0
        )

    lse_c[xy] = as_tile(log_sum)
    each(1, XY, lambda d: lse_c_copy(d).start())

    def combined(parts):
        values = parts[...]
        peak = jnp.max(values, axis=0)
        return peak + jnp.log(jnp.sum(jnp.exp(values - peak[None]), axis=0))

    load_pair.wait()
    held = pair[pl.ds(y * 16 + x // 2, 8, stride=2), :]
    held = jnp.where(x % 2 == 1, pltpu.roll(held, 64, 1), held)
    held = jnp.concatenate([held] * 16, axis=0).T
    captions = jnp.concatenate([held[:64, h * C + k : h * C + k + 1] for k in range(C) for h in range(ZH)], axis=0)
    j = lax.broadcasted_iota(jnp.int32, (1, BLOCK), 1)
    ids = ((j // 128) * 8 + zh * C + c) * 256 + ((j // PIECE) % X) * ROWS + zl * PIECE + j % PIECE

    each(1, ZC, lambda d: lse_r_copy(d).wait_recv())
    total_r = combined(lse_r)
    turned = jnp.concatenate([total_r] * 16, axis=0).T
    each(1, XY, lambda d: lse_c_copy(d).wait_recv())
    total_c = combined(lse_c)
    line_c = jnp.concatenate([total_c[k : k + 1] for k in range(4)], axis=1)
    target = jnp.zeros((1, BLOCK), f32)
    for k, rows in enumerate(quarters):
        s = scores[rows]
        flags = (captions[k * 128 : (k + 1) * 128] == ids).astype(f32)
        target = target + jnp.sum(flags * s, axis=0, keepdims=True)
        w = scale * (jnp.exp(s - turned[:, k : k + 1]) + jnp.exp(s - line_c) - 2.0 * flags)
        weights[rows] = w.astype(bf16)
    shared = jnp.where(row < 4, total_r + total_c, 0.0) * (1.0 / 16)
    loss_1[zc] = shared - 2.0 * as_tile(target)

    def loss_1_copy(d):
        return remote(loss_1.at[zc], loss_1.at[zc], l1_s.at[d], l1_r.at[d], **column(d))

    def loss_2_copy(d):
        return remote(loss_2.at[xy], loss_2.at[xy], l2_s.at[d], l2_r.at[d], **plane(d))

    each(1, ZC, lambda d: loss_1_copy(d).start())

    d2d = remote(img_d2d, img_d2d_got, d2d_s, d2d_r, dp_2=1 - c)
    rows = pl.ds(pl.multiple_of((1 - c) * SIDE, SIDE), SIDE)
    img_d2d[...] = dot(weights[rows], tbuf[...]).astype(bf16)
    d2d.start()

    def grad_t_copy(d):
        there = plane(d)
        piece = slot(txt_send, there["dp_0"] * X + there["mp"])
        return remote(piece, txt_got.at[d], gt_s.at[d], gt_r.at[d], **there)

    for k in range(4):
        cols = pl.ds(k * 128, 128)
        txt_send[cols] = dot(weights[:, cols], ibuf[...], ((0,), (0,))).astype(bf16)
    each(1, XY, lambda d: grad_t_copy(d).start())

    def grad_i_copy(d):
        there = (zh + d) % ZH
        piece = img_send.at[pl.ds(pl.multiple_of(there * ROWS, ROWS), ROWS)]
        gap = (there * ZL + Z - z) % Z
        return remote(piece, img_got.at[gap], gi_s.at[d], gi_r.at[gap], dp_1=there, group=0)

    rows = pl.ds(pl.multiple_of(c * SIDE, SIDE), SIDE)
    value = dot(weights[rows], tbuf[...])
    d2d.wait_recv()
    value = value + img_d2d_got[...].astype(f32)
    img_own[...] = value
    img_send[...] = value.astype(bf16)

    @pl.when(zl == 1)
    def _():
        grad_i_copy(0).start()

    each(1, ZH, lambda d: grad_i_copy(d).start())

    each(1, ZC, lambda d: loss_1_copy(d).wait_recv())
    loss_2[xy] = jnp.sum(loss_1[...], axis=0)
    each(1, XY, lambda d: loss_2_copy(d).start())

    each(1, XY, lambda d: grad_t_copy(d).wait_recv())
    value = txt_send[pl.ds(pl.multiple_of(xy * PIECE, PIECE), PIECE)].astype(f32)
    for d in range(1, XY):
        value = value + txt_got[d].astype(f32)

    last = remote(fin, fin_got, fin_s, fin_r, group=1)

    @pl.when(zl == 0)
    def _():
        fin[...] = value.astype(bf16)
        last.start()
        own = img_own[pl.ds(pl.multiple_of(zh * ROWS, ROWS), ROWS)]

        def arrived(gap):
            remote(img_send.at[:ROWS], img_got.at[gap], gi_s.at[0], gi_r.at[gap], group=0).wait_recv()

        each(1, Z, arrived)
        for gap in range(1, Z):
            own = own + img_got[gap].astype(f32)
        out[0] = own
        last.wait_send()

    @pl.when(zl == 1)
    def _():
        out[0, PIECE:] = value
        grad_i_copy(0).wait_send()
        last.wait_recv()
        out[0, :PIECE] = fin_got[...].astype(f32)

    each(1, XY, lambda d: loss_2_copy(d).wait_recv())
    loss_out[0, 0] = jnp.sum(jnp.sum(loss_2[...], axis=0)) * (1.0 / (2 * XY * BLOCK))

    def sent_x(d):
        stat_copy(d).wait_send()
        share_t(d).wait_send()
        share_i(d).wait_send()
        grad_i_copy(d).wait_send()

    def sent_plane(d):
        text_copy(d).wait_send()
        lse_r_copy(d).wait_send()
        lse_c_copy(d).wait_send()
        loss_1_copy(d).wait_send()
        loss_2_copy(d).wait_send()
        grad_t_copy(d).wait_send()

    each(1, X, sent_x)
    each(1, Z, lambda d: image_copy(d).wait_send())
    each(0, Z, lambda d: forward(d).wait_send())
    each(1, XY, sent_plane)
    d2d.wait_send()


def body(
    image_features, text_features, image_gain, text_gain, image_proj, text_proj, pair, logit_scale
):
    width_i, width_t = image_features.shape[1], text_features.shape[1]
    emb = image_proj.shape[1]
    vmem = pl.BlockSpec(memory_space=pltpu.VMEM)
    smem = pl.BlockSpec(memory_space=pltpu.SMEM)
    hbm = pl.BlockSpec(memory_space=pl.ANY)
    dma = lambda *n: pltpu.SemaphoreType.DMA(n)
    grads, loss = pl.pallas_call(
        kernel,
        out_shape=(
            jax.ShapeDtypeStruct((1, ROWS, emb), f32),
            jax.ShapeDtypeStruct((1, 1), f32),
        ),
        in_specs=[hbm, hbm, hbm, hbm, hbm, hbm, hbm, smem],
        out_specs=(vmem, smem),
        scratch_shapes=[
            pltpu.VMEM((HALF, width_i), bf16),
            pltpu.VMEM((HALF, width_t), bf16),
            pltpu.VMEM((width_i // 128, 128), f32),
            pltpu.VMEM((width_t // 128, 128), f32),
            pltpu.VMEM((pair.size // 128, 128), jnp.int32),
            pltpu.VMEM((width_i, emb), bf16),
            pltpu.VMEM((width_t, emb), bf16),
            pltpu.VMEM((HALF + 16, width_i), bf16),
            pltpu.VMEM((HALF + 16, width_t), bf16),
            pltpu.VMEM((X, 24, 128), f32),
            pltpu.VMEM((128, 128), f32),
            pltpu.VMEM((HALF, emb), bf16),
            pltpu.VMEM((HALF, emb), bf16),
            pltpu.VMEM((HALF, emb), f32),
            pltpu.VMEM((HALF, emb), f32),
            pltpu.VMEM((X, PIECE, emb), bf16),
            pltpu.VMEM((X, PIECE, emb), bf16),
            pltpu.VMEM((BLOCK, emb), bf16),
            pltpu.VMEM((BLOCK, emb), bf16),
            pltpu.VMEM((BLOCK, BLOCK), f32),
            pltpu.VMEM((BLOCK, BLOCK), bf16),
            pltpu.VMEM((ZC, 8, 128), f32),
            pltpu.VMEM((XY, 8, 128), f32),
            pltpu.VMEM((ZC, 8, 128), f32),
            pltpu.VMEM((XY, 8, 128), f32),
            pltpu.VMEM((SIDE, emb), bf16),
            pltpu.VMEM((SIDE, emb), bf16),
            pltpu.VMEM((SIDE, emb), bf16),
            pltpu.VMEM((SIDE, emb), f32),
            pltpu.VMEM((Z, ROWS, emb), bf16),
            pltpu.VMEM((BLOCK, emb), bf16),
            pltpu.VMEM((XY, PIECE, emb), bf16),
            pltpu.VMEM((PIECE, emb), bf16),
            pltpu.VMEM((PIECE, emb), bf16),
            dma(2 * X + 5),
            dma(X), dma(X), dma(X), dma(X), dma(X), dma(X),
            dma(Z), dma(Z), dma(Z), dma(Z), dma(XY), dma(XY),
            dma(ZC), dma(ZC), dma(XY), dma(XY), dma(ZC), dma(ZC), dma(XY), dma(XY),
            pltpu.SemaphoreType.DMA, pltpu.SemaphoreType.DMA,
            dma(ZH), dma(Z), dma(XY), dma(XY),
            pltpu.SemaphoreType.DMA, pltpu.SemaphoreType.DMA,
        ],
        compiler_params=pltpu.CompilerParams(
            collective_id=0, has_side_effects=True, vmem_limit_bytes=67043328
        ),
        name="contrastive",
    )(
        image_features, text_features, image_gain.reshape(-1, 128), text_gain.reshape(-1, 128),
        image_proj, text_proj, pair.reshape(-1, 128), logit_scale.reshape(1, 1),
    )
    return grads, loss.reshape(())


def solution(mesh):
    split = Mesh(
        mesh.devices.reshape(mesh.shape["group"], 4, 4, 2, mesh.shape["mp"]),
        ("group", "dp_0", "dp_1", "dp_2", "mp"),
    )
    placed = (P(DP, "mp"), P(DP, "mp"), P("mp"), P("mp"), P("mp", None), P("mp", None), P(), P())
    return jax.shard_map(
        body, mesh=split, in_specs=placed, out_specs=(P("group", DP_MP, None), P()), check_vma=False
    )
```

```python
import functools

import jax
import jax.numpy as jnp
from jax import lax
from jax.experimental import pallas as pl
from jax.experimental.pallas import tpu as pltpu
from jax.sharding import Mesh
from jax.sharding import PartitionSpec as P

DP_MP = ("dp_0", "dp_1", "dp_2", "mp")
DP = ("dp_0", "dp_1", "dp_2")
MESH = pl.DeviceIdType.MESH

X, Y, ZH, ZL, C = 4, 4, 4, 2, 2
Z = ZH * ZL
XY = X * Y
ZC = Z * C
PIECE = 32
HALF = X * PIECE
BLOCK = XY * PIECE
ROWS = 2 * PIECE
HALF_E = 512
SIDE = Z * PIECE

epsilon = 1e-05
f32 = jnp.float32
bf16 = jnp.bfloat16


def dot(a, b, dims=((1,), (0,))):
    return lax.dot_general(a, b, (dims, ((), ())), preferred_element_type=f32)


def hops(d, size):
    return min(d, size - d)


PLANE = sorted(range(1, XY), key=lambda d: -hops(d % X, X) - hops(d // X, Y))
COLUMN = sorted(range(1, ZC), key=lambda d: -hops(d % Z, Z))
RING = (2, 1, 3)


def each(low, high, step):
    def turn(i, carry):
        step(i)
        return carry

    lax.fori_loop(low, high, turn, 0)


def kernel(
    feat_i, feat_t, gain_i, gain_t, proj_i, proj_t, pair_hbm, scale_ref,
    out, loss_out,
    fi, ft, gi, gt, pair, pi, pt, lhs_i, lhs_t, stats, moments, part_i, part_t, own_i, own_t, got_i, got_t,
    ibuf, tbuf, scores, weights, lse_r, lse_c, loss_1, loss_2,
    img_d2d, img_d2d_got, img_send, img_own, img_got,
    txt_send, sum_x, sum_y, sent_x, sent_y, sum_xy, sum_yx, fin, fin_got,
    load_sem, stat_s, stat_r, rsi_s, rsi_r, rst_s, rst_r,
    agi_s, agi_r, agh_s, agh_r, fwd_s, fwd_r, agx_s, agx_r, agy_s, agy_r, axy_s, axy_r, ayx_s, ayx_r,
    lr_s, lr_r, lc_s, lc_r, l1_s, l1_r, l2_s, l2_r,
    d2d_s, d2d_r, gi_s, gi_r, gx_s, gx_r, gy_s, gy_r, gxy_s, gxy_r, gyx_s, gyx_r, fin_s, fin_r,
):
    x, y = lax.axis_index("mp"), lax.axis_index("dp_0")
    zh, c, zl = lax.axis_index("dp_1"), lax.axis_index("dp_2"), lax.axis_index("group")
    z = zh * ZL + zl
    xy = y * X + x
    zc = c * Z + z

    def remote(src, dst, send, recv, **where):
        return pltpu.make_async_remote_copy(
            src_ref=src, dst_ref=dst, send_sem=send, recv_sem=recv,
            device_id=where, device_id_type=MESH,
        )

    def plane(d):
        return {"mp": (x + d % X) % X, "dp_0": (y + d // X) % Y}

    def column(d):
        there = (z + d % Z) % Z
        return {"dp_1": there // ZL, "group": there % ZL, "dp_2": (c + d // Z) % C}

    loads = []
    for k in range(X):
        rows = pl.ds(pl.multiple_of(k * ROWS + zl * PIECE, PIECE), PIECE)
        here = pl.ds(k * PIECE, PIECE)
        loads.append(pltpu.make_async_copy(feat_i.at[rows], fi.at[here], load_sem.at[k]))
        loads.append(pltpu.make_async_copy(feat_t.at[rows], ft.at[here], load_sem.at[X + k]))
    loads += [
        pltpu.make_async_copy(gain_i, gi, load_sem.at[2 * X + 2]),
        pltpu.make_async_copy(gain_t, gt, load_sem.at[2 * X + 3]),
    ]
    loads_p = [
        pltpu.make_async_copy(proj_t, pt, load_sem.at[2 * X]),
        pltpu.make_async_copy(proj_i, pi, load_sem.at[2 * X + 1]),
    ]
    load_pair = pltpu.make_async_copy(pair_hbm, pair, load_sem.at[2 * X + 4])
    for copy in loads + loads_p + [load_pair]:
        copy.start()

    barrier = pltpu.get_barrier_semaphore()

    def greet_plane(d):
        pl.semaphore_signal(barrier, inc=1, device_id=plane(d), device_id_type=MESH)

    def greet_column(d):
        pl.semaphore_signal(barrier, inc=1, device_id=column(d), device_id_type=MESH)

    each(1, XY, greet_plane)
    each(1, ZC, greet_column)

    for copy in loads:
        copy.wait()
    lane = lax.broadcasted_iota(jnp.int32, (HALF, 128), 1)
    row = lax.broadcasted_iota(jnp.int32, (8, 128), 0)

    def centred(features, gain, lhs):
        values = features[...].astype(f32)
        mean = jnp.sum(values, axis=1, keepdims=True) * (1.0 / values.shape[1])
        squares = jnp.sum(values * values, axis=1, keepdims=True)
        line = jnp.concatenate([gain[k : k + 1, :] for k in range(gain.shape[0])], axis=1)
        lhs[:HALF] = ((values - mean) * line).astype(bf16)
        coarse = line.astype(bf16)
        fine = (line - coarse.astype(f32)).astype(bf16)
        lhs[HALF:] = jnp.concatenate([coarse, fine, jnp.zeros((14, line.shape[1]), bf16)], axis=0)
        return mean, squares

    def lines(row_of_all):
        return jnp.concatenate([row_of_all[:, k * 128 : (k + 1) * 128] for k in range(8)], axis=0)

    def share_copy(d, part, got, send, recv):
        there = (x + d) % X
        rows = pl.ds(pl.multiple_of(there * PIECE, PIECE), PIECE)
        return remote(part.at[rows], got.at[d], send.at[d], recv.at[d], mp=there)

    share_t = lambda d: share_copy(d, part_t, got_t, rst_s, rst_r)
    share_i = lambda d: share_copy(d, part_i, got_i, rsi_s, rsi_r)

    def stat_copy(d):
        return remote(stats.at[x], stats.at[x], stat_s.at[d], stat_r.at[d], mp=(x + d) % X)

    mean_t, squares_t = centred(ft, gt, lhs_t)
    loads_p[0].wait()
    value = dot(lhs_t[...], pt[...])
    own_t[...] = value[:HALF]
    part_t[...] = value[:HALF].astype(bf16)
    stats[x, 16:] = lines(value[HALF : HALF + 1] + value[HALF + 1 : HALF + 2])
    mean_i, squares_i = centred(fi, gi, lhs_i)
    packed = jnp.where(lane == 0, mean_i, 0.0)
    packed = jnp.where(lane == 1, squares_i, packed)
    packed = jnp.where(lane == 2, mean_t, packed)
    packed = jnp.where(lane == 3, squares_t, packed)
    stats[x, :8] = packed.T[:8]
    pl.semaphore_wait(barrier, XY - 1 + ZC - 1)
    for d in (2, 1, 3):
        share_t(d).start()
    loads_p[1].wait()
    value = dot(lhs_i[...], pi[...])
    own_i[...] = value[:HALF]
    part_i[...] = value[:HALF].astype(bf16)
    stats[x, 8:16] = lines(value[HALF : HALF + 1] + value[HALF + 1 : HALF + 2])
    for d in (2, 1, 3):
        stat_copy(d).start()
    for d in (2, 1, 3):
        share_i(d).start()

    each(1, X, lambda d: stat_copy(d).wait_recv())
    turned = jnp.concatenate([stats[k, :8] for k in range(X)] + [jnp.zeros((96, 128), f32)], axis=0).T
    moments[...] = turned
    moment = moments[pl.ds(pl.multiple_of(x * PIECE, PIECE), PIECE)]

    def unit_of(own, got, which, width):
        means = [moment[:, 8 * k + 2 * which : 8 * k + 2 * which + 1] for k in range(X)]
        squares = [moment[:, 8 * k + 2 * which + 1 : 8 * k + 2 * which + 2] for k in range(X)]
        average = (means[0] + means[1] + means[2] + means[3]) * (1.0 / X)
        spread = (squares[0] + squares[1] + squares[2] + squares[3]) / width - average * average
        value = own[pl.ds(pl.multiple_of(x * PIECE, PIECE), PIECE)]
        for d in range(1, X):
            value = value + got[d].astype(f32)
        for k in range(X):
            gained = stats[k, 8 * (1 + which) : 8 * (2 + which)]
            gained = jnp.concatenate([gained[q : q + 1] for q in range(8)], axis=1)
            value = value + (means[k] - average) * gained
        size = jnp.sum(value * value, axis=1, keepdims=True) + 1e-06 * (spread + epsilon)
        return (value * lax.rsqrt(size)).astype(bf16)

    def slot(buffer, index):
        return buffer.at[pl.ds(pl.multiple_of(index * PIECE, PIECE), PIECE)]

    def half(buffer, index, which):
        return buffer.at[pl.ds(pl.multiple_of(index * PIECE + which * (PIECE // 2), 16), PIECE // 2)]

    def text_x(d):
        mine = slot(tbuf, xy)
        return remote(mine, mine, agx_s.at[d], agx_r.at[d], mp=(x + d) % X)

    def text_y(d):
        mine = slot(tbuf, xy)
        return remote(mine, mine, agy_s.at[d], agy_r.at[d], dp_0=(y + d) % Y)

    def text_xy(d, e):
        held = half(tbuf, y * X + (x + X - d) % X, 0)
        return remote(held, held, axy_s.at[d * 4 + e], axy_r.at[d * 4 + e], dp_0=(y + e) % Y)

    def text_yx(d, e):
        held = half(tbuf, (y + Y - d) % Y * X + x, 1)
        return remote(held, held, ayx_s.at[d * 4 + e], ayx_r.at[d * 4 + e], mp=(x + e) % X)

    def along(d):
        there = (z + d) % Z
        return {"dp_1": there // ZL, "group": there % ZL}

    def image_copy(d):
        mine = slot(ibuf, zc)
        return remote(mine, mine, agi_s.at[d], agi_r.at[d], **along(d))

    def image_on(d):
        held = slot(ibuf, c * Z + (z + Z - (2 if d == 3 else 6)) % Z)
        return remote(held, held, agi_s.at[d], agi_r.at[d], **along(1 if d == 3 else 7))

    def image_half(which):
        held = half(ibuf, c * Z + (z + Z - (2, 6)[which]) % Z, which)
        return remote(held, held, agh_s.at[which], agh_r.at[which], **along((2, 6)[which]))

    def forward(d):
        held = slot(ibuf, c * Z + (z + Z - d) % Z)
        return remote(held, held, fwd_s.at[d], fwd_r.at[d], dp_2=1 - c)

    each(1, X, lambda d: share_t(d).wait_recv())
    tbuf[pl.ds(pl.multiple_of(xy * PIECE, PIECE), PIECE)] = unit_of(own_t, got_t, 1, f32(X * ft.shape[1]))
    for d in RING:
        text_x(d).start()
        text_y(d).start()
    each(1, X, lambda d: share_i(d).wait_recv())
    ibuf[pl.ds(pl.multiple_of(zc * PIECE, PIECE), PIECE)] = unit_of(own_i, got_i, 0, f32(X * fi.shape[1]))
    for d in (2, 6, 1, 7):
        image_copy(d).start()
    forward(0).start()
    for d in (1, 3, 2):
        text_x(d).wait_recv()
        for e in RING:
            text_xy(d, e).start()
        text_y(d).wait_recv()
        for e in RING:
            text_yx(d, e).start()
    for d in (2, 6):
        image_copy(d).wait_recv()
        image_half(0 if d == 2 else 1).start()
        image_on(3 if d == 2 else 5).start()
        forward(d).start()
    for d in (1, 7):
        image_copy(d).wait_recv()
        forward(d).start()
    for d in (3, 5):
        image_on(d).wait_recv()
        forward(d).start()
    image_half(0).wait_recv()
    image_half(1).wait_recv()
    forward(4).start()
    for d in range(1, X):
        for e in range(1, X):
            text_xy(d, e).wait_recv()
            text_yx(d, e).wait_recv()
    each(0, Z, lambda d: forward(d).wait_recv())

    scale = scale_ref[0, 0]
    quarters = [pl.ds(k * 128, 128) for k in range(BLOCK // 128)]
    packed = jnp.zeros((128, 128), f32)
    peak_c = None
    for k, rows in enumerate(quarters):
        s = scale * dot(ibuf[rows], tbuf[...], ((1,), (1,)))
        scores[rows] = s
        peak = jnp.max(s, axis=1, keepdims=True)
        log_sum = peak + jnp.log(jnp.sum(jnp.exp(s - peak), axis=1, keepdims=True))
        packed = jnp.where(lane == k, log_sum, packed)
        high = jnp.max(s, axis=0, keepdims=True)
        peak_c = high if peak_c is None else jnp.maximum(peak_c, high)
    lse_r[zc] = packed.T[:8]

    def lse_r_copy(d):
        return remote(lse_r.at[zc], lse_r.at[zc], lr_s.at[d], lr_r.at[d], **column(d))

    def lse_c_copy(d):
        return remote(lse_c.at[xy], lse_c.at[xy], lc_s.at[d], lc_r.at[d], **plane(d))

    for d in COLUMN:
        lse_r_copy(d).start()
    sum_c = jnp.zeros((1, BLOCK), f32)
    for rows in quarters:
        sum_c = sum_c + jnp.sum(jnp.exp(scores[rows] - peak_c), axis=0, keepdims=True)
    log_sum = peak_c + jnp.log(sum_c)

    def as_tile(line):
        return jnp.concatenate(
            [line[:, k * 128 : (k + 1) * 128] for k in range(4)] + [jnp.zeros((4, 128), f32)], axis=0
        )

    lse_c[xy] = as_tile(log_sum)
    for d in PLANE:
        lse_c_copy(d).start()

    def combined(parts):
        values = parts[...]
        peak = jnp.max(values, axis=0)
        return peak + jnp.log(jnp.sum(jnp.exp(values - peak[None]), axis=0))

    load_pair.wait()
    held = pair[pl.ds(y * 16 + x // 2, 8, stride=2), :]
    held = jnp.where(x % 2 == 1, pltpu.roll(held, 64, 1), held)
    held = jnp.concatenate([held] * 16, axis=0).T
    captions = jnp.concatenate([held[:64, h * C + k : h * C + k + 1] for k in range(C) for h in range(ZH)], axis=0)
    j = lax.broadcasted_iota(jnp.int32, (1, BLOCK), 1)
    ids = ((j // 128) * 8 + zh * C + c) * 256 + ((j // PIECE) % X) * ROWS + zl * PIECE + j % PIECE

    each(1, ZC, lambda d: lse_r_copy(d).wait_recv())
    total_r = combined(lse_r)
    turned = jnp.concatenate([total_r] * 16, axis=0).T
    each(1, XY, lambda d: lse_c_copy(d).wait_recv())
    total_c = combined(lse_c)
    line_c = jnp.concatenate([total_c[k : k + 1] for k in range(4)], axis=1)
    target = jnp.zeros((1, BLOCK), f32)
    for k, rows in enumerate(quarters):
        s = scores[rows]
        flags = (captions[k * 128 : (k + 1) * 128] == ids).astype(f32)
        target = target + jnp.sum(flags * s, axis=0, keepdims=True)
        w = scale * (jnp.exp(s - turned[:, k : k + 1]) + jnp.exp(s - line_c) - 2.0 * flags)
        weights[rows] = w.astype(bf16)
    shared = jnp.where(row < 4, total_r + total_c, 0.0) * (1.0 / 16)
    loss_1[zc] = shared - 2.0 * as_tile(target)

    def loss_1_copy(d):
        return remote(loss_1.at[zc], loss_1.at[zc], l1_s.at[d], l1_r.at[d], **column(d))

    def loss_2_copy(d):
        return remote(loss_2.at[xy], loss_2.at[xy], l2_s.at[d], l2_r.at[d], **plane(d))

    for d in COLUMN:
        loss_1_copy(d).start()

    d2d = remote(img_d2d, img_d2d_got, d2d_s, d2d_r, dp_2=1 - c)
    rows = pl.ds(pl.multiple_of((1 - c) * SIDE, SIDE), SIDE)
    img_d2d[...] = dot(weights[rows], tbuf[...]).astype(bf16)
    d2d.start()

    def grad_x(d):
        there = (x + d) % X
        return remote(txt_send.at[:, there, :, :HALF_E], sum_x.at[d], gx_s.at[d], gx_r.at[d], mp=there)

    def grad_y(d):
        there = (y + d) % Y
        return remote(txt_send.at[there, :, :, HALF_E:], sum_y.at[d], gy_s.at[d], gy_r.at[d], dp_0=there)

    def grad_xy(d):
        there = (y + d) % Y
        return remote(sent_x.at[there], sum_xy.at[d], gxy_s.at[d], gxy_r.at[d], dp_0=there)

    def grad_yx(d):
        there = (x + d) % X
        return remote(sent_y.at[there], sum_yx.at[d], gyx_s.at[d], gyx_r.at[d], mp=there)

    for k in range(4):
        cols = pl.ds(k * 128, 128)
        value = dot(weights[:, cols], ibuf[:, :HALF_E], ((0,), (0,)))
        txt_send[k, :, :, :HALF_E] = value.reshape(X, PIECE, HALF_E).astype(bf16)
    for d in RING:
        grad_x(d).start()
    for k in range(4):
        cols = pl.ds(k * 128, 128)
        value = dot(weights[:, cols], ibuf[:, HALF_E:], ((0,), (0,)))
        txt_send[k, :, :, HALF_E:] = value.reshape(X, PIECE, HALF_E).astype(bf16)
    for d in RING:
        grad_y(d).start()

    def grad_i_copy(d):
        there = (zh + d) % ZH
        piece = img_send.at[pl.ds(pl.multiple_of(there * ROWS, ROWS), ROWS)]
        gap = (there * ZL + Z - z) % Z
        return remote(piece, img_got.at[gap], gi_s.at[d], gi_r.at[gap], dp_1=there, group=0)

    rows = pl.ds(pl.multiple_of(c * SIDE, SIDE), SIDE)
    value = dot(weights[rows], tbuf[...])
    d2d.wait_recv()
    value = value + img_d2d_got[...].astype(f32)
    img_own[...] = value
    img_send[...] = value.astype(bf16)

    for d in (2, 3, 1):
        grad_i_copy(d).start()

    @pl.when(zl == 1)
    def _():
        grad_i_copy(0).start()

    each(1, ZC, lambda d: loss_1_copy(d).wait_recv())
    loss_2[xy] = jnp.sum(loss_1[...], axis=0)
    for d in PLANE:
        loss_2_copy(d).start()

    each(1, X, lambda d: grad_x(d).wait_recv())
    for k in range(Y):
        value = txt_send[k, x, :, :HALF_E].astype(f32)
        for d in range(1, X):
            value = value + sum_x[d, k].astype(f32)
        sent_x[k] = value.astype(bf16)
    for d in RING:
        grad_xy(d).start()
    each(1, Y, lambda d: grad_y(d).wait_recv())
    for k in range(X):
        value = txt_send[y, k, :, HALF_E:].astype(f32)
        for d in range(1, Y):
            value = value + sum_y[d, k].astype(f32)
        sent_y[k] = value.astype(bf16)
    for d in RING:
        grad_yx(d).start()
    each(1, Y, lambda d: grad_xy(d).wait_recv())
    first = sent_x[y].astype(f32)
    for d in range(1, Y):
        first = first + sum_xy[d].astype(f32)
    each(1, X, lambda d: grad_yx(d).wait_recv())
    second = sent_y[x].astype(f32)
    for d in range(1, X):
        second = second + sum_yx[d].astype(f32)

    last = remote(fin, fin_got, fin_s, fin_r, group=1)

    @pl.when(zl == 0)
    def _():
        fin[:, :HALF_E] = first.astype(bf16)
        fin[:, HALF_E:] = second.astype(bf16)
        last.start()
        own = img_own[pl.ds(pl.multiple_of(zh * ROWS, ROWS), ROWS)]

        def arrived(gap):
            remote(img_send.at[:ROWS], img_got.at[gap], gi_s.at[0], gi_r.at[gap], group=0).wait_recv()

        each(1, Z, arrived)
        for gap in range(1, Z):
            own = own + img_got[gap].astype(f32)
        out[0] = own
        last.wait_send()

    @pl.when(zl == 1)
    def _():
        out[0, PIECE:, :HALF_E] = first
        out[0, PIECE:, HALF_E:] = second
        grad_i_copy(0).wait_send()
        last.wait_recv()
        out[0, :PIECE] = fin_got[...].astype(f32)

    each(1, XY, lambda d: loss_2_copy(d).wait_recv())
    loss_out[0, 0] = jnp.sum(jnp.sum(loss_2[...], axis=0)) * (1.0 / (2 * XY * BLOCK))

    def sent_ring(d):
        stat_copy(d).wait_send()
        share_t(d).wait_send()
        share_i(d).wait_send()
        grad_i_copy(d).wait_send()
        text_x(d).wait_send()
        text_y(d).wait_send()
        grad_x(d).wait_send()
        grad_y(d).wait_send()
        grad_xy(d).wait_send()
        grad_yx(d).wait_send()
        for e in range(1, X):
            text_xy(d, e).wait_send()
            text_yx(d, e).wait_send()

    def sent_all(d):
        lse_r_copy(d).wait_send()
        lse_c_copy(d).wait_send()
        loss_1_copy(d).wait_send()
        loss_2_copy(d).wait_send()

    each(1, X, sent_ring)
    for d in (1, 2, 6, 7):
        image_copy(d).wait_send()
    image_on(3).wait_send()
    image_on(5).wait_send()
    image_half(0).wait_send()
    image_half(1).wait_send()
    each(0, Z, lambda d: forward(d).wait_send())
    each(1, XY, sent_all)
    d2d.wait_send()


def body(
    image_features, text_features, image_gain, text_gain, image_proj, text_proj, pair, logit_scale
):
    width_i, width_t = image_features.shape[1], text_features.shape[1]
    emb = image_proj.shape[1]
    vmem = pl.BlockSpec(memory_space=pltpu.VMEM)
    smem = pl.BlockSpec(memory_space=pltpu.SMEM)
    hbm = pl.BlockSpec(memory_space=pl.ANY)
    dma = lambda *n: pltpu.SemaphoreType.DMA(n)
    grads, loss = pl.pallas_call(
        kernel,
        out_shape=(
            jax.ShapeDtypeStruct((1, ROWS, emb), f32),
            jax.ShapeDtypeStruct((1, 1), f32),
        ),
        in_specs=[hbm, hbm, hbm, hbm, hbm, hbm, hbm, smem],
        out_specs=(vmem, smem),
        scratch_shapes=[
            pltpu.VMEM((HALF, width_i), bf16),
            pltpu.VMEM((HALF, width_t), bf16),
            pltpu.VMEM((width_i // 128, 128), f32),
            pltpu.VMEM((width_t // 128, 128), f32),
            pltpu.VMEM((pair.size // 128, 128), jnp.int32),
            pltpu.VMEM((width_i, emb), bf16),
            pltpu.VMEM((width_t, emb), bf16),
            pltpu.VMEM((HALF + 16, width_i), bf16),
            pltpu.VMEM((HALF + 16, width_t), bf16),
            pltpu.VMEM((X, 24, 128), f32),
            pltpu.VMEM((128, 128), f32),
            pltpu.VMEM((HALF, emb), bf16),
            pltpu.VMEM((HALF, emb), bf16),
            pltpu.VMEM((HALF, emb), f32),
            pltpu.VMEM((HALF, emb), f32),
            pltpu.VMEM((X, PIECE, emb), bf16),
            pltpu.VMEM((X, PIECE, emb), bf16),
            pltpu.VMEM((BLOCK, emb), bf16),
            pltpu.VMEM((BLOCK, emb), bf16),
            pltpu.VMEM((BLOCK, BLOCK), f32),
            pltpu.VMEM((BLOCK, BLOCK), bf16),
            pltpu.VMEM((ZC, 8, 128), f32),
            pltpu.VMEM((XY, 8, 128), f32),
            pltpu.VMEM((ZC, 8, 128), f32),
            pltpu.VMEM((XY, 8, 128), f32),
            pltpu.VMEM((SIDE, emb), bf16),
            pltpu.VMEM((SIDE, emb), bf16),
            pltpu.VMEM((SIDE, emb), bf16),
            pltpu.VMEM((SIDE, emb), f32),
            pltpu.VMEM((Z, ROWS, emb), bf16),
            pltpu.VMEM((Y, X, PIECE, emb), bf16),
            pltpu.VMEM((X, Y, PIECE, HALF_E), bf16),
            pltpu.VMEM((Y, X, PIECE, HALF_E), bf16),
            pltpu.VMEM((Y, PIECE, HALF_E), bf16),
            pltpu.VMEM((X, PIECE, HALF_E), bf16),
            pltpu.VMEM((Y, PIECE, HALF_E), bf16),
            pltpu.VMEM((X, PIECE, HALF_E), bf16),
            pltpu.VMEM((PIECE, emb), bf16),
            pltpu.VMEM((PIECE, emb), bf16),
            dma(2 * X + 5),
            dma(X), dma(X), dma(X), dma(X), dma(X), dma(X),
            dma(Z), dma(Z), dma(2), dma(2), dma(Z), dma(Z), dma(X), dma(X), dma(Y), dma(Y),
            dma(XY), dma(XY), dma(XY), dma(XY),
            dma(ZC), dma(ZC), dma(XY), dma(XY), dma(ZC), dma(ZC), dma(XY), dma(XY),
            pltpu.SemaphoreType.DMA, pltpu.SemaphoreType.DMA,
            dma(ZH), dma(Z), dma(X), dma(X), dma(Y), dma(Y), dma(Y), dma(Y), dma(X), dma(X),
            pltpu.SemaphoreType.DMA, pltpu.SemaphoreType.DMA,
        ],
        compiler_params=pltpu.CompilerParams(
            collective_id=0, has_side_effects=True, vmem_limit_bytes=67043328
        ),
        name="contrastive",
    )(
        image_features, text_features, image_gain.reshape(-1, 128), text_gain.reshape(-1, 128),
        image_proj, text_proj, pair.reshape(-1, 128), logit_scale.reshape(1, 1),
    )
    return grads, loss.reshape(())


def solution(mesh):
    split = Mesh(
        mesh.devices.reshape(mesh.shape["group"], 4, 4, 2, mesh.shape["mp"]),
        ("group", "dp_0", "dp_1", "dp_2", "mp"),
    )
    placed = (P(DP, "mp"), P(DP, "mp"), P("mp"), P("mp"), P("mp", None), P("mp", None), P(), P())
    return jax.shard_map(
        body, mesh=split, in_specs=placed, out_specs=(P("group", DP_MP, None), P()), check_vma=False
    )
```

```python
import functools

import jax
import jax.numpy as jnp
from jax import lax
from jax.experimental import pallas as pl
from jax.experimental.pallas import tpu as pltpu
from jax.sharding import Mesh
from jax.sharding import PartitionSpec as P

DP_MP = ("dp_0", "dp_1", "dp_2", "mp")
DP = ("dp_0", "dp_1", "dp_2")
MESH = pl.DeviceIdType.MESH

X, Y, ZH, ZL, C = 4, 4, 4, 2, 2
Z = ZH * ZL
XY = X * Y
ZC = Z * C
PIECE = 32
HALF = X * PIECE
BLOCK = XY * PIECE
ROWS = 2 * PIECE
HALF_E = 512
SIDE = Z * PIECE

epsilon = 1e-05
f32 = jnp.float32
bf16 = jnp.bfloat16


def dot(a, b, dims=((1,), (0,))):
    return lax.dot_general(a, b, (dims, ((), ())), preferred_element_type=f32)


def hops(d, size):
    return min(d, size - d)


PLANE = sorted(range(1, XY), key=lambda d: -hops(d % X, X) - hops(d // X, Y))
COLUMN = sorted(range(1, ZC), key=lambda d: -hops(d % Z, Z))
RING = (2, 1, 3)


def each(low, high, step):
    def turn(i, carry):
        step(i)
        return carry

    lax.fori_loop(low, high, turn, 0)


def kernel(
    feat_i, feat_t, gain_i, gain_t, proj_i, proj_t, pair_hbm, scale_ref,
    out, loss_out,
    fi, ft, gi, gt, pair, pi, pt, lhs_i, lhs_t, stats, moments, part_i, part_t, own_i, own_t, got_i, got_t,
    ibuf, tbuf, scores, weights, lse_r, lse_c, loss_1, loss_2,
    img_d2d, img_d2d_got, img_send, img_near, img_third_got, img_fourth_got, img_sum, img_far,
    txt_send, sum_x, sum_y, sent_x, sent_y, sum_xy, sum_yx, fin, fin_got,
    load_sem, stat_s, stat_r, rsi_s, rsi_r, rst_s, rst_r,
    agi_s, agi_r, agh_s, agh_r, fwd_s, fwd_r, agx_s, agx_r, agy_s, agy_r, axy_s, axy_r, ayx_s, ayx_r,
    lr_s, lr_r, lc_s, lc_r, l1_s, l1_r, l2_s, l2_r,
    d2d_s, d2d_r, in_s, in_r, i3_s, i3_r, i4_s, i4_r, if_s, if_r, gx_s, gx_r, gy_s, gy_r, gxy_s, gxy_r, gyx_s, gyx_r, fin_s, fin_r,
):
    x, y = lax.axis_index("mp"), lax.axis_index("dp_0")
    zh, c, zl = lax.axis_index("dp_1"), lax.axis_index("dp_2"), lax.axis_index("group")
    z = zh * ZL + zl
    xy = y * X + x
    zc = c * Z + z

    def remote(src, dst, send, recv, **where):
        return pltpu.make_async_remote_copy(
            src_ref=src, dst_ref=dst, send_sem=send, recv_sem=recv,
            device_id=where, device_id_type=MESH,
        )

    def plane(d):
        return {"mp": (x + d % X) % X, "dp_0": (y + d // X) % Y}

    def column(d):
        there = (z + d % Z) % Z
        return {"dp_1": there // ZL, "group": there % ZL, "dp_2": (c + d // Z) % C}

    loads_i, loads_t = [], []
    for k in range(X):
        rows = pl.ds(pl.multiple_of(k * ROWS + zl * PIECE, PIECE), PIECE)
        here = pl.ds(k * PIECE, PIECE)
        loads_i.append(pltpu.make_async_copy(feat_i.at[rows], fi.at[here], load_sem.at[k]))
        loads_t.append(pltpu.make_async_copy(feat_t.at[rows], ft.at[here], load_sem.at[X + k]))
    loads_i.append(pltpu.make_async_copy(gain_i, gi, load_sem.at[2 * X + 2]))
    loads_t.append(pltpu.make_async_copy(gain_t, gt, load_sem.at[2 * X + 3]))
    loads_p = [
        pltpu.make_async_copy(proj_t, pt, load_sem.at[2 * X]),
        pltpu.make_async_copy(proj_i, pi, load_sem.at[2 * X + 1]),
    ]
    load_pair = pltpu.make_async_copy(pair_hbm, pair, load_sem.at[2 * X + 4])
    for copy in loads_t + loads_p[:1] + loads_i + loads_p[1:] + [load_pair]:
        copy.start()

    barrier = pltpu.get_barrier_semaphore()

    def greet_plane(d):
        pl.semaphore_signal(barrier, inc=1, device_id=plane(d), device_id_type=MESH)

    def greet_column(d):
        pl.semaphore_signal(barrier, inc=1, device_id=column(d), device_id_type=MESH)

    each(1, XY, greet_plane)
    each(1, ZC, greet_column)

    lane = lax.broadcasted_iota(jnp.int32, (HALF, 128), 1)

    def centred(features, gain, lhs):
        values = features[...].astype(f32)
        mean = jnp.sum(values, axis=1, keepdims=True) * (1.0 / values.shape[1])
        squares = jnp.sum(values * values, axis=1, keepdims=True)
        line = jnp.concatenate([gain[k : k + 1, :] for k in range(gain.shape[0])], axis=1)
        lhs[:HALF] = ((values - mean) * line).astype(bf16)
        coarse = line.astype(bf16)
        fine = (line - coarse.astype(f32)).astype(bf16)
        lhs[HALF:] = jnp.concatenate([coarse, fine, jnp.zeros((14, line.shape[1]), bf16)], axis=0)
        return mean, squares

    def lines(row_of_all):
        return jnp.concatenate([row_of_all[:, k * 128 : (k + 1) * 128] for k in range(8)], axis=0)

    def share_copy(d, part, got, send, recv):
        there = (x + d) % X
        rows = pl.ds(pl.multiple_of(there * PIECE, PIECE), PIECE)
        return remote(part.at[rows], got.at[d], send.at[d], recv.at[d], mp=there)

    share_t = lambda d: share_copy(d, part_t, got_t, rst_s, rst_r)
    share_i = lambda d: share_copy(d, part_i, got_i, rsi_s, rsi_r)

    def stat_copy(d):
        return remote(stats.at[x], stats.at[x], stat_s.at[d], stat_r.at[d], mp=(x + d) % X)

    for copy in loads_t:
        copy.wait()
    mean_t, squares_t = centred(ft, gt, lhs_t)
    loads_p[0].wait()
    value = dot(lhs_t[...], pt[...])
    own_t[...] = value[:HALF]
    part_t[...] = value[:HALF].astype(bf16)
    pl.semaphore_wait(barrier, XY - 1 + ZC - 1)
    for d in (2, 1, 3):
        share_t(d).start()
    stats[x, 16:] = lines(value[HALF : HALF + 1] + value[HALF + 1 : HALF + 2])
    for copy in loads_i:
        copy.wait()
    mean_i, squares_i = centred(fi, gi, lhs_i)
    packed = jnp.where(lane == 0, mean_i, 0.0)
    packed = jnp.where(lane == 1, squares_i, packed)
    packed = jnp.where(lane == 2, mean_t, packed)
    packed = jnp.where(lane == 3, squares_t, packed)
    stats[x, :8] = packed.T[:8]
    loads_p[1].wait()
    value = dot(lhs_i[...], pi[...])
    own_i[...] = value[:HALF]
    part_i[...] = value[:HALF].astype(bf16)
    stats[x, 8:16] = lines(value[HALF : HALF + 1] + value[HALF + 1 : HALF + 2])
    for d in (2, 1, 3):
        stat_copy(d).start()
    for d in (2, 1, 3):
        share_i(d).start()

    each(1, X, lambda d: stat_copy(d).wait_recv())
    turned = jnp.concatenate([stats[k, :8] for k in range(X)] + [jnp.zeros((96, 128), f32)], axis=0).T
    moments[...] = turned
    moment = moments[pl.ds(pl.multiple_of(x * PIECE, PIECE), PIECE)]

    def unit_of(own, got, which, width):
        means = [moment[:, 8 * k + 2 * which : 8 * k + 2 * which + 1] for k in range(X)]
        squares = [moment[:, 8 * k + 2 * which + 1 : 8 * k + 2 * which + 2] for k in range(X)]
        average = (means[0] + means[1] + means[2] + means[3]) * (1.0 / X)
        spread = (squares[0] + squares[1] + squares[2] + squares[3]) / width - average * average
        value = own[pl.ds(pl.multiple_of(x * PIECE, PIECE), PIECE)]
        for d in range(1, X):
            value = value + got[d].astype(f32)
        for k in range(X):
            gained = stats[k, 8 * (1 + which) : 8 * (2 + which)]
            gained = jnp.concatenate([gained[q : q + 1] for q in range(8)], axis=1)
            value = value + (means[k] - average) * gained
        size = jnp.sum(value * value, axis=1, keepdims=True) + 1e-06 * (spread + epsilon)
        return (value * lax.rsqrt(size)).astype(bf16)

    def slot(buffer, index):
        return buffer.at[pl.ds(pl.multiple_of(index * PIECE, PIECE), PIECE)]

    def half(buffer, index, which):
        return buffer.at[pl.ds(pl.multiple_of(index * PIECE + which * (PIECE // 2), 16), PIECE // 2)]

    def text_x(d):
        mine = slot(tbuf, xy)
        return remote(mine, mine, agx_s.at[d], agx_r.at[d], mp=(x + d) % X)

    def text_y(d):
        mine = slot(tbuf, xy)
        return remote(mine, mine, agy_s.at[d], agy_r.at[d], dp_0=(y + d) % Y)

    def text_xy(d, e):
        held = half(tbuf, y * X + (x + X - d) % X, 0)
        return remote(held, held, axy_s.at[d * 4 + e], axy_r.at[d * 4 + e], dp_0=(y + e) % Y)

    def text_yx(d, e):
        held = half(tbuf, (y + Y - d) % Y * X + x, 1)
        return remote(held, held, ayx_s.at[d * 4 + e], ayx_r.at[d * 4 + e], mp=(x + e) % X)

    def along(d):
        there = (z + d) % Z
        return {"dp_1": there // ZL, "group": there % ZL}

    def image_copy(d):
        mine = slot(ibuf, zc)
        return remote(mine, mine, agi_s.at[d], agi_r.at[d], **along(d))

    def image_on(d):
        held = slot(ibuf, c * Z + (z + Z - (2 if d == 3 else 6)) % Z)
        return remote(held, held, agi_s.at[d], agi_r.at[d], **along(1 if d == 3 else 7))

    def image_half(which):
        held = half(ibuf, c * Z + (z + Z - (2, 6)[which]) % Z, which)
        return remote(held, held, agh_s.at[which], agh_r.at[which], **along((2, 6)[which]))

    def forward(d):
        held = slot(ibuf, c * Z + (z + Z - d) % Z)
        return remote(held, held, fwd_s.at[d], fwd_r.at[d], dp_2=1 - c)

    each(1, X, lambda d: share_t(d).wait_recv())
    tbuf[pl.ds(pl.multiple_of(xy * PIECE, PIECE), PIECE)] = unit_of(own_t, got_t, 1, f32(X * ft.shape[1]))
    for d in RING:
        text_x(d).start()
        text_y(d).start()
    each(1, X, lambda d: share_i(d).wait_recv())
    ibuf[pl.ds(pl.multiple_of(zc * PIECE, PIECE), PIECE)] = unit_of(own_i, got_i, 0, f32(X * fi.shape[1]))
    for d in (2, 6, 1, 7):
        image_copy(d).start()
    forward(0).start()
    for d in (1, 3, 2):
        text_x(d).wait_recv()
        for e in RING:
            text_xy(d, e).start()
        text_y(d).wait_recv()
        for e in RING:
            text_yx(d, e).start()
    for d in (2, 6):
        image_copy(d).wait_recv()
        image_half(0 if d == 2 else 1).start()
        image_on(3 if d == 2 else 5).start()
        forward(d).start()
    for d in (1, 7):
        image_copy(d).wait_recv()
        forward(d).start()
    for d in (3, 5):
        image_on(d).wait_recv()
        forward(d).start()
    image_half(0).wait_recv()
    image_half(1).wait_recv()
    forward(4).start()
    for d in range(1, X):
        for e in range(1, X):
            text_xy(d, e).wait_recv()
            text_yx(d, e).wait_recv()
    each(0, Z, lambda d: forward(d).wait_recv())

    scale = scale_ref[0, 0]
    quarters = [pl.ds(k * 128, 128) for k in range(BLOCK // 128)]
    packed = jnp.zeros((128, 128), f32)
    peak_c = None
    for k, rows in enumerate(quarters):
        s = scale * dot(ibuf[rows], tbuf[...], ((1,), (1,)))
        scores[rows] = s
        peak = jnp.max(s, axis=1, keepdims=True)
        log_sum = peak + jnp.log(jnp.sum(jnp.exp(s - peak), axis=1, keepdims=True))
        packed = jnp.where(lane == k, log_sum, packed)
        high = jnp.max(s, axis=0, keepdims=True)
        peak_c = high if peak_c is None else jnp.maximum(peak_c, high)
    lse_r[zc] = packed.T[:4]

    def lse_r_copy(d):
        return remote(lse_r.at[zc], lse_r.at[zc], lr_s.at[d], lr_r.at[d], **column(d))

    def lse_c_copy(d):
        return remote(lse_c.at[xy], lse_c.at[xy], lc_s.at[d], lc_r.at[d], **plane(d))

    for d in COLUMN:
        lse_r_copy(d).start()
    sum_c = jnp.zeros((1, BLOCK), f32)
    for rows in quarters:
        sum_c = sum_c + jnp.sum(jnp.exp(scores[rows] - peak_c), axis=0, keepdims=True)
    log_sum = peak_c + jnp.log(sum_c)

    def as_tile(line):
        return jnp.concatenate(
            [line[:, k * 128 : (k + 1) * 128] for k in range(4)], axis=0
        )

    lse_c[xy] = as_tile(log_sum)
    for d in PLANE:
        lse_c_copy(d).start()

    def combined(parts):
        values = parts[...]
        peak = jnp.max(values, axis=0)
        return peak + jnp.log(jnp.sum(jnp.exp(values - peak[None]), axis=0))

    load_pair.wait()
    held = pair[pl.ds(y * 16 + x // 2, 8, stride=2), :]
    held = jnp.where(x % 2 == 1, pltpu.roll(held, 64, 1), held)
    held = jnp.concatenate([held] * 16, axis=0).T
    captions = jnp.concatenate([held[:64, h * C + k : h * C + k + 1] for k in range(C) for h in range(ZH)], axis=0)
    j = lax.broadcasted_iota(jnp.int32, (1, BLOCK), 1)
    ids = ((j // 128) * 8 + zh * C + c) * 256 + ((j // PIECE) % X) * ROWS + zl * PIECE + j % PIECE

    each(1, ZC, lambda d: lse_r_copy(d).wait_recv())
    total_r = combined(lse_r)
    turned = jnp.concatenate([total_r] * 32, axis=0).T
    each(1, XY, lambda d: lse_c_copy(d).wait_recv())
    total_c = combined(lse_c)
    line_c = jnp.concatenate([total_c[k : k + 1] for k in range(4)], axis=1)
    target = jnp.zeros((1, BLOCK), f32)
    for k, rows in enumerate(quarters):
        s = scores[rows]
        flags = (captions[k * 128 : (k + 1) * 128] == ids).astype(f32)
        target = target + jnp.sum(flags * s, axis=0, keepdims=True)
        w = scale * (jnp.exp(s - turned[:, k : k + 1]) + jnp.exp(s - line_c) - 2.0 * flags)
        weights[rows] = w.astype(bf16)
    shared = (total_r + total_c) * (1.0 / 16)
    loss_1[zc] = shared - 2.0 * as_tile(target)

    def loss_1_copy(d):
        return remote(loss_1.at[zc], loss_1.at[zc], l1_s.at[d], l1_r.at[d], **column(d))

    def loss_2_copy(d):
        return remote(loss_2.at[xy], loss_2.at[xy], l2_s.at[d], l2_r.at[d], **plane(d))

    for d in COLUMN:
        loss_1_copy(d).start()

    d2d = remote(img_d2d, img_d2d_got, d2d_s, d2d_r, dp_2=1 - c)
    rows = pl.ds(pl.multiple_of((1 - c) * SIDE, SIDE), SIDE)
    img_d2d[...] = dot(weights[rows], tbuf[...]).astype(bf16)
    d2d.start()

    def grad_x(d):
        there = (x + d) % X
        return remote(txt_send.at[:, there, :, :HALF_E], sum_x.at[d], gx_s.at[d], gx_r.at[d], mp=there)

    def grad_y(d):
        there = (y + d) % Y
        return remote(txt_send.at[there, :, :, HALF_E:], sum_y.at[d], gy_s.at[d], gy_r.at[d], dp_0=there)

    def grad_xy(d):
        there = (y + d) % Y
        return remote(sent_x.at[there], sum_xy.at[d], gxy_s.at[d], gxy_r.at[d], dp_0=there)

    def grad_yx(d):
        there = (x + d) % X
        return remote(sent_y.at[there], sum_yx.at[d], gyx_s.at[d], gyx_r.at[d], mp=there)

    for k in range(4):
        cols = pl.ds(k * 128, 128)
        value = dot(weights[:, cols], ibuf[:, :HALF_E], ((0,), (0,)))
        txt_send[k, :, :, :HALF_E] = value.reshape(X, PIECE, HALF_E).astype(bf16)
    for d in RING:
        grad_x(d).start()
    def piece(index):
        return img_send.at[pl.ds(pl.multiple_of((z + index) % Z * PIECE, PIECE), PIECE)]

    def img_next(side):
        return remote(piece((1, 7)[side]), img_near.at[side], in_s.at[side], in_r.at[side], **along((1, 7)[side]))

    def img_third(side):
        return remote(piece((3, 5)[side]), img_third_got.at[side], i3_s.at[side], i3_r.at[side], **along((1, 7)[side]))

    def img_fourth(side):
        start = (z + 4) % Z * PIECE + side * (PIECE // 2)
        part = img_send.at[pl.ds(pl.multiple_of(start, 16), PIECE // 2)]
        return remote(part, img_fourth_got.at[side], i4_s.at[side], i4_r.at[side], **along((2, 6)[side]))

    def img_second(side):
        return remote(img_sum.at[side], img_far.at[side], if_s.at[side], if_r.at[side], **along((2, 6)[side]))

    rows = pl.ds(pl.multiple_of(c * SIDE, SIDE), SIDE)
    value = dot(weights[rows], tbuf[...])
    d2d.wait_recv()
    value = value + img_d2d_got[...].astype(f32)
    img_send[...] = value.astype(bf16)
    for send in (img_fourth, img_third, img_next):
        send(0).start()
        send(1).start()

    for k in range(4):
        cols = pl.ds(k * 128, 128)
        value = dot(weights[:, cols], ibuf[:, HALF_E:], ((0,), (0,)))
        txt_send[k, :, :, HALF_E:] = value.reshape(X, PIECE, HALF_E).astype(bf16)
    for d in RING:
        grad_y(d).start()

    each(1, ZC, lambda d: loss_1_copy(d).wait_recv())
    loss_2[xy] = jnp.sum(loss_1[...], axis=0)
    for d in PLANE:
        loss_2_copy(d).start()

    def image_rows(index, start, count):
        return img_send[pl.ds(pl.multiple_of((z + index) % Z * PIECE + start, 16), count)].astype(f32)

    for side in range(2):
        img_fourth(side).wait_recv()
        img_third(side).wait_recv()
        for part in range(2):
            rows = pl.ds(part * (PIECE // 2), PIECE // 2)
            value = image_rows((2, 6)[side], part * (PIECE // 2), PIECE // 2) + img_third_got[side, rows].astype(f32)
            if part == side:
                value = value + img_fourth_got[side].astype(f32)
            img_sum[side, rows] = value.astype(bf16)
        img_second(side).start()

    each(1, X, lambda d: grad_x(d).wait_recv())
    for k in range(Y):
        value = txt_send[k, x, :, :HALF_E].astype(f32)
        for d in range(1, X):
            value = value + sum_x[d, k].astype(f32)
        sent_x[k] = value.astype(bf16)
    for d in RING:
        grad_xy(d).start()
    each(1, Y, lambda d: grad_y(d).wait_recv())
    for k in range(X):
        value = txt_send[y, k, :, HALF_E:].astype(f32)
        for d in range(1, Y):
            value = value + sum_y[d, k].astype(f32)
        sent_y[k] = value.astype(bf16)
    for d in RING:
        grad_yx(d).start()
    each(1, Y, lambda d: grad_xy(d).wait_recv())
    first = sent_x[y].astype(f32)
    for d in range(1, Y):
        first = first + sum_xy[d].astype(f32)
    each(1, X, lambda d: grad_yx(d).wait_recv())
    second = sent_y[x].astype(f32)
    for d in range(1, X):
        second = second + sum_yx[d].astype(f32)

    last = remote(fin, fin_got, fin_s, fin_r, group=1 - zl)

    @pl.when(zl == 0)
    def _():
        fin[:, :HALF_E] = first.astype(bf16)
        fin[:, HALF_E:] = second.astype(bf16)
        last.start()

    @pl.when(zl == 1)
    def _():
        out[0, PIECE:, :HALF_E] = first
        out[0, PIECE:, HALF_E:] = second

    third = image_rows(0, 0, PIECE)
    for side in range(2):
        img_next(side).wait_recv()
        third = third + img_near[side].astype(f32)
    for side in range(2):
        img_second(side).wait_recv()
        third = third + img_far[side].astype(f32)

    @pl.when(zl == 0)
    def _():
        out[0, :PIECE] = third
        last.wait_recv()
        out[0, PIECE:] = fin_got[...].astype(f32)

    @pl.when(zl == 1)
    def _():
        fin[...] = third.astype(bf16)
        last.start()
        last.wait_recv()
        out[0, :PIECE] = fin_got[...].astype(f32)

    each(1, XY, lambda d: loss_2_copy(d).wait_recv())
    loss_out[0, 0] = jnp.sum(jnp.sum(loss_2[...], axis=0)) * (1.0 / (2 * XY * BLOCK))

    def sent_ring(d):
        stat_copy(d).wait_send()
        share_t(d).wait_send()
        share_i(d).wait_send()
        text_x(d).wait_send()
        text_y(d).wait_send()
        grad_x(d).wait_send()
        grad_y(d).wait_send()
        grad_xy(d).wait_send()
        grad_yx(d).wait_send()
        for e in range(1, X):
            text_xy(d, e).wait_send()
            text_yx(d, e).wait_send()

    def sent_all(d):
        lse_r_copy(d).wait_send()
        lse_c_copy(d).wait_send()
        loss_1_copy(d).wait_send()
        loss_2_copy(d).wait_send()

    each(1, X, sent_ring)
    for d in (1, 2, 6, 7):
        image_copy(d).wait_send()
    image_on(3).wait_send()
    image_on(5).wait_send()
    image_half(0).wait_send()
    image_half(1).wait_send()
    each(0, Z, lambda d: forward(d).wait_send())
    each(1, XY, sent_all)
    for side in range(2):
        img_next(side).wait_send()
        img_third(side).wait_send()
        img_fourth(side).wait_send()
        img_second(side).wait_send()
    last.wait_send()
    d2d.wait_send()


def body(
    image_features, text_features, image_gain, text_gain, image_proj, text_proj, pair, logit_scale
):
    width_i, width_t = image_features.shape[1], text_features.shape[1]
    emb = image_proj.shape[1]
    vmem = pl.BlockSpec(memory_space=pltpu.VMEM)
    smem = pl.BlockSpec(memory_space=pltpu.SMEM)
    hbm = pl.BlockSpec(memory_space=pl.ANY)
    dma = lambda *n: pltpu.SemaphoreType.DMA(n)
    grads, loss = pl.pallas_call(
        kernel,
        out_shape=(
            jax.ShapeDtypeStruct((1, ROWS, emb), f32),
            jax.ShapeDtypeStruct((1, 1), f32),
        ),
        in_specs=[hbm, hbm, hbm, hbm, hbm, hbm, hbm, smem],
        out_specs=(vmem, smem),
        scratch_shapes=[
            pltpu.VMEM((HALF, width_i), bf16),
            pltpu.VMEM((HALF, width_t), bf16),
            pltpu.VMEM((width_i // 128, 128), f32),
            pltpu.VMEM((width_t // 128, 128), f32),
            pltpu.VMEM((pair.size // 128, 128), jnp.int32),
            pltpu.VMEM((width_i, emb), bf16),
            pltpu.VMEM((width_t, emb), bf16),
            pltpu.VMEM((HALF + 16, width_i), bf16),
            pltpu.VMEM((HALF + 16, width_t), bf16),
            pltpu.VMEM((X, 24, 128), f32),
            pltpu.VMEM((128, 128), f32),
            pltpu.VMEM((HALF, emb), bf16),
            pltpu.VMEM((HALF, emb), bf16),
            pltpu.VMEM((HALF, emb), f32),
            pltpu.VMEM((HALF, emb), f32),
            pltpu.VMEM((X, PIECE, emb), bf16),
            pltpu.VMEM((X, PIECE, emb), bf16),
            pltpu.VMEM((BLOCK, emb), bf16),
            pltpu.VMEM((BLOCK, emb), bf16),
            pltpu.VMEM((BLOCK, BLOCK), f32),
            pltpu.VMEM((BLOCK, BLOCK), bf16),
            pltpu.VMEM((ZC, 4, 128), f32),
            pltpu.VMEM((XY, 4, 128), f32),
            pltpu.VMEM((ZC, 4, 128), f32),
            pltpu.VMEM((XY, 4, 128), f32),
            pltpu.VMEM((SIDE, emb), bf16),
            pltpu.VMEM((SIDE, emb), bf16),
            pltpu.VMEM((SIDE, emb), bf16),
            pltpu.VMEM((2, PIECE, emb), bf16),
            pltpu.VMEM((2, PIECE, emb), bf16),
            pltpu.VMEM((2, PIECE // 2, emb), bf16),
            pltpu.VMEM((2, PIECE, emb), bf16),
            pltpu.VMEM((2, PIECE, emb), bf16),
            pltpu.VMEM((Y, X, PIECE, emb), bf16),
            pltpu.VMEM((X, Y, PIECE, HALF_E), bf16),
            pltpu.VMEM((Y, X, PIECE, HALF_E), bf16),
            pltpu.VMEM((Y, PIECE, HALF_E), bf16),
            pltpu.VMEM((X, PIECE, HALF_E), bf16),
            pltpu.VMEM((Y, PIECE, HALF_E), bf16),
            pltpu.VMEM((X, PIECE, HALF_E), bf16),
            pltpu.VMEM((PIECE, emb), bf16),
            pltpu.VMEM((PIECE, emb), bf16),
            dma(2 * X + 5),
            dma(X), dma(X), dma(X), dma(X), dma(X), dma(X),
            dma(Z), dma(Z), dma(2), dma(2), dma(Z), dma(Z), dma(X), dma(X), dma(Y), dma(Y),
            dma(XY), dma(XY), dma(XY), dma(XY),
            dma(ZC), dma(ZC), dma(XY), dma(XY), dma(ZC), dma(ZC), dma(XY), dma(XY),
            pltpu.SemaphoreType.DMA, pltpu.SemaphoreType.DMA,
            dma(2), dma(2), dma(2), dma(2), dma(2), dma(2), dma(2), dma(2),
            dma(X), dma(X), dma(Y), dma(Y), dma(Y), dma(Y), dma(X), dma(X),
            pltpu.SemaphoreType.DMA, pltpu.SemaphoreType.DMA,
        ],
        compiler_params=pltpu.CompilerParams(
            collective_id=0, has_side_effects=True, vmem_limit_bytes=67043328
        ),
        name="contrastive",
    )(
        image_features, text_features, image_gain.reshape(-1, 128), text_gain.reshape(-1, 128),
        image_proj, text_proj, pair.reshape(-1, 128), logit_scale.reshape(1, 1),
    )
    return grads, loss.reshape(())


def solution(mesh):
    split = Mesh(
        mesh.devices.reshape(mesh.shape["group"], 4, 4, 2, mesh.shape["mp"]),
        ("group", "dp_0", "dp_1", "dp_2", "mp"),
    )
    placed = (P(DP, "mp"), P(DP, "mp"), P("mp"), P("mp"), P("mp", None), P("mp", None), P(), P())
    return jax.shard_map(
        body, mesh=split, in_specs=placed, out_specs=(P("group", DP_MP, None), P()), check_vma=False
    )
```

```python
import functools

import jax
import jax.numpy as jnp
from jax import lax
from jax.experimental import pallas as pl
from jax.experimental.pallas import tpu as pltpu
from jax.sharding import Mesh
from jax.sharding import PartitionSpec as P

DP_MP = ("dp_0", "dp_1", "dp_2", "mp")
DP = ("dp_0", "dp_1", "dp_2")
MESH = pl.DeviceIdType.MESH

X, Y, ZH, ZL, C = 4, 4, 4, 2, 2
Z = ZH * ZL
XY = X * Y
ZC = Z * C
PIECE = 32
HALF = X * PIECE
BLOCK = XY * PIECE
ROWS = 2 * PIECE
HALF_E = 512
SIDE = Z * PIECE

epsilon = 1e-05
f32 = jnp.float32
bf16 = jnp.bfloat16


def dot(a, b, dims=((1,), (0,))):
    return lax.dot_general(a, b, (dims, ((), ())), preferred_element_type=f32)


def hops(d, size):
    return min(d, size - d)


PLANE = sorted(range(1, XY), key=lambda d: -hops(d % X, X) - hops(d // X, Y))
COLUMN = sorted(range(1, ZC), key=lambda d: -hops(d % Z, Z))
RING = (2, 1, 3)


def each(low, high, step):
    def turn(i, carry):
        step(i)
        return carry

    lax.fori_loop(low, high, turn, 0)


def kernel(
    feat_i, feat_t, gain_i, gain_t, proj_i, proj_t, pair_hbm, scale_hbm,
    out, loss_out,
    scale_ref, result, loss_ref, fi, ft, gi, gt, pair, pi, pt, lhs_i, lhs_t, stats, moments, part_i, part_t, own_i, own_t, got_i, got_t,
    ibuf, tbuf, scores, weights, lse_r, lse_c, loss_1, loss_2,
    img_d2d, img_d2d_got, img_send, img_near, img_third_got, img_fourth_got, img_sum, img_far,
    txt_send, sum_x, sum_y, sent_x, sent_y, sum_xy, sum_yx, fin, fin_got,
    load_sem, store_sem, stat_s, stat_r, rsi_s, rsi_r, rst_s, rst_r,
    agi_s, agi_r, agh_s, agh_r, fwd_s, fwd_r, agx_s, agx_r, agy_s, agy_r, axy_s, axy_r, ayx_s, ayx_r,
    lr_s, lr_r, lc_s, lc_r, l1_s, l1_r, l2_s, l2_r,
    d2d_s, d2d_r, in_s, in_r, i3_s, i3_r, i4_s, i4_r, if_s, if_r, gx_s, gx_r, gy_s, gy_r, gxy_s, gxy_r, gyx_s, gyx_r, fin_s, fin_r,
):
    x, y = lax.axis_index("mp"), lax.axis_index("dp_0")
    zh, c, zl = lax.axis_index("dp_1"), lax.axis_index("dp_2"), lax.axis_index("group")
    z = zh * ZL + zl
    xy = y * X + x
    zc = c * Z + z

    def remote(src, dst, send, recv, **where):
        return pltpu.make_async_remote_copy(
            src_ref=src, dst_ref=dst, send_sem=send, recv_sem=recv,
            device_id=where, device_id_type=MESH,
        )

    def plane(d):
        return {"mp": (x + d % X) % X, "dp_0": (y + d // X) % Y}

    def column(d):
        there = (z + d % Z) % Z
        return {"dp_1": there // ZL, "group": there % ZL, "dp_2": (c + d // Z) % C}

    loads_i, loads_t = [], []
    for k in range(X):
        rows = pl.ds(pl.multiple_of(k * ROWS + zl * PIECE, PIECE), PIECE)
        here = pl.ds(k * PIECE, PIECE)
        loads_i.append(pltpu.make_async_copy(feat_i.at[rows], fi.at[here], load_sem.at[k]))
        loads_t.append(pltpu.make_async_copy(feat_t.at[rows], ft.at[here], load_sem.at[X + k]))
    loads_i.append(pltpu.make_async_copy(gain_i, gi, load_sem.at[2 * X + 2]))
    loads_t.append(pltpu.make_async_copy(gain_t, gt, load_sem.at[2 * X + 3]))
    loads_p = [
        pltpu.make_async_copy(proj_t, pt, load_sem.at[2 * X]),
        pltpu.make_async_copy(proj_i, pi, load_sem.at[2 * X + 1]),
    ]
    load_pair = pltpu.make_async_copy(pair_hbm, pair, load_sem.at[2 * X + 4])
    load_scale = pltpu.make_async_copy(scale_hbm, scale_ref, load_sem.at[2 * X + 5])
    for copy in loads_t + loads_p[:1] + loads_i + loads_p[1:] + [load_pair, load_scale]:
        copy.start()

    barrier = pltpu.get_barrier_semaphore()

    def greet_plane(d):
        pl.semaphore_signal(barrier, inc=1, device_id=plane(d), device_id_type=MESH)

    def greet_column(d):
        pl.semaphore_signal(barrier, inc=1, device_id=column(d), device_id_type=MESH)

    each(1, XY, greet_plane)
    each(1, ZC, greet_column)

    lane = lax.broadcasted_iota(jnp.int32, (HALF, 128), 1)

    def centred(features, gain, lhs):
        values = features[...].astype(f32)
        mean = jnp.sum(values, axis=1, keepdims=True) * (1.0 / values.shape[1])
        squares = jnp.sum(values * values, axis=1, keepdims=True)
        line = jnp.concatenate([gain[k : k + 1, :] for k in range(gain.shape[0])], axis=1)
        lhs[:HALF] = ((values - mean) * line).astype(bf16)
        coarse = line.astype(bf16)
        fine = (line - coarse.astype(f32)).astype(bf16)
        lhs[HALF:] = jnp.concatenate([coarse, fine, jnp.zeros((14, line.shape[1]), bf16)], axis=0)
        return mean, squares

    def lines(row_of_all):
        return jnp.concatenate([row_of_all[:, k * 128 : (k + 1) * 128] for k in range(8)], axis=0)

    def share_copy(d, part, got, send, recv):
        there = (x + d) % X
        rows = pl.ds(pl.multiple_of(there * PIECE, PIECE), PIECE)
        return remote(part.at[rows], got.at[d], send.at[d], recv.at[d], mp=there)

    share_t = lambda d: share_copy(d, part_t, got_t, rst_s, rst_r)
    share_i = lambda d: share_copy(d, part_i, got_i, rsi_s, rsi_r)

    def stat_copy(d):
        return remote(stats.at[x], stats.at[x], stat_s.at[d], stat_r.at[d], mp=(x + d) % X)

    for copy in loads_t:
        copy.wait()
    mean_t, squares_t = centred(ft, gt, lhs_t)
    loads_p[0].wait()
    value = dot(lhs_t[...], pt[...])
    own_t[...] = value[:HALF]
    part_t[...] = value[:HALF].astype(bf16)
    pl.semaphore_wait(barrier, XY - 1 + ZC - 1)
    for d in (2, 1, 3):
        share_t(d).start()
    stats[x, 16:] = lines(value[HALF : HALF + 1] + value[HALF + 1 : HALF + 2])
    for copy in loads_i:
        copy.wait()
    mean_i, squares_i = centred(fi, gi, lhs_i)
    packed = jnp.where(lane == 0, mean_i, 0.0)
    packed = jnp.where(lane == 1, squares_i, packed)
    packed = jnp.where(lane == 2, mean_t, packed)
    packed = jnp.where(lane == 3, squares_t, packed)
    stats[x, :8] = packed.T[:8]
    loads_p[1].wait()
    value = dot(lhs_i[...], pi[...])
    own_i[...] = value[:HALF]
    part_i[...] = value[:HALF].astype(bf16)
    stats[x, 8:16] = lines(value[HALF : HALF + 1] + value[HALF + 1 : HALF + 2])
    for d in (2, 1, 3):
        stat_copy(d).start()
    for d in (2, 1, 3):
        share_i(d).start()

    each(1, X, lambda d: stat_copy(d).wait_recv())
    turned = jnp.concatenate([stats[k, :8] for k in range(X)] + [jnp.zeros((96, 128), f32)], axis=0).T
    moments[...] = turned
    moment = moments[pl.ds(pl.multiple_of(x * PIECE, PIECE), PIECE)]

    def unit_of(own, got, which, width):
        means = [moment[:, 8 * k + 2 * which : 8 * k + 2 * which + 1] for k in range(X)]
        squares = [moment[:, 8 * k + 2 * which + 1 : 8 * k + 2 * which + 2] for k in range(X)]
        average = (means[0] + means[1] + means[2] + means[3]) * (1.0 / X)
        spread = (squares[0] + squares[1] + squares[2] + squares[3]) / width - average * average
        value = own[pl.ds(pl.multiple_of(x * PIECE, PIECE), PIECE)]
        for d in range(1, X):
            value = value + got[d].astype(f32)
        for k in range(X):
            gained = stats[k, 8 * (1 + which) : 8 * (2 + which)]
            gained = jnp.concatenate([gained[q : q + 1] for q in range(8)], axis=1)
            value = value + (means[k] - average) * gained
        size = jnp.sum(value * value, axis=1, keepdims=True) + 1e-06 * (spread + epsilon)
        return (value * lax.rsqrt(size)).astype(bf16)

    def slot(buffer, index):
        return buffer.at[pl.ds(pl.multiple_of(index * PIECE, PIECE), PIECE)]

    def half(buffer, index, which):
        return buffer.at[pl.ds(pl.multiple_of(index * PIECE + which * (PIECE // 2), 16), PIECE // 2)]

    def text_x(d):
        mine = slot(tbuf, xy)
        return remote(mine, mine, agx_s.at[d], agx_r.at[d], mp=(x + d) % X)

    def text_y(d):
        mine = slot(tbuf, xy)
        return remote(mine, mine, agy_s.at[d], agy_r.at[d], dp_0=(y + d) % Y)

    def text_xy(d, e):
        held = half(tbuf, y * X + (x + X - d) % X, 0)
        return remote(held, held, axy_s.at[d * 4 + e], axy_r.at[d * 4 + e], dp_0=(y + e) % Y)

    def text_yx(d, e):
        held = half(tbuf, (y + Y - d) % Y * X + x, 1)
        return remote(held, held, ayx_s.at[d * 4 + e], ayx_r.at[d * 4 + e], mp=(x + e) % X)

    def along(d):
        there = (z + d) % Z
        return {"dp_1": there // ZL, "group": there % ZL}

    def image_copy(d):
        mine = slot(ibuf, zc)
        return remote(mine, mine, agi_s.at[d], agi_r.at[d], **along(d))

    def image_on(d):
        held = slot(ibuf, c * Z + (z + Z - (2 if d == 3 else 6)) % Z)
        return remote(held, held, agi_s.at[d], agi_r.at[d], **along(1 if d == 3 else 7))

    def image_half(which):
        held = half(ibuf, c * Z + (z + Z - (2, 6)[which]) % Z, which)
        return remote(held, held, agh_s.at[which], agh_r.at[which], **along((2, 6)[which]))

    def forward(d):
        held = slot(ibuf, c * Z + (z + Z - d) % Z)
        return remote(held, held, fwd_s.at[d], fwd_r.at[d], dp_2=1 - c)

    each(1, X, lambda d: share_t(d).wait_recv())
    tbuf[pl.ds(pl.multiple_of(xy * PIECE, PIECE), PIECE)] = unit_of(own_t, got_t, 1, f32(X * ft.shape[1]))
    for d in RING:
        text_x(d).start()
        text_y(d).start()
    each(1, X, lambda d: share_i(d).wait_recv())
    ibuf[pl.ds(pl.multiple_of(zc * PIECE, PIECE), PIECE)] = unit_of(own_i, got_i, 0, f32(X * fi.shape[1]))
    for d in (2, 6, 1, 7):
        image_copy(d).start()
    forward(0).start()
    for d in (1, 3, 2):
        text_x(d).wait_recv()
        for e in RING:
            text_xy(d, e).start()
        text_y(d).wait_recv()
        for e in RING:
            text_yx(d, e).start()
    for d in (2, 6):
        image_copy(d).wait_recv()
        image_half(0 if d == 2 else 1).start()
        image_on(3 if d == 2 else 5).start()
        forward(d).start()
    for d in (1, 7):
        image_copy(d).wait_recv()
        forward(d).start()
    for d in (3, 5):
        image_on(d).wait_recv()
        forward(d).start()
    image_half(0).wait_recv()
    image_half(1).wait_recv()
    forward(4).start()
    for d in range(1, X):
        for e in range(1, X):
            text_xy(d, e).wait_recv()
            text_yx(d, e).wait_recv()
    each(0, Z, lambda d: forward(d).wait_recv())

    load_scale.wait()
    scale = scale_ref[...]
    quarters = [pl.ds(k * 128, 128) for k in range(BLOCK // 128)]
    packed = jnp.zeros((128, 128), f32)
    peak_c = None
    for k, rows in enumerate(quarters):
        s = scale * dot(ibuf[rows], tbuf[...], ((1,), (1,)))
        scores[rows] = s
        peak = jnp.max(s, axis=1, keepdims=True)
        log_sum = peak + jnp.log(jnp.sum(jnp.exp(s - peak), axis=1, keepdims=True))
        packed = jnp.where(lane == k, log_sum, packed)
        high = jnp.max(s, axis=0, keepdims=True)
        peak_c = high if peak_c is None else jnp.maximum(peak_c, high)
    lse_r[zc] = packed.T[:4]

    def lse_r_copy(d):
        return remote(lse_r.at[zc], lse_r.at[zc], lr_s.at[d], lr_r.at[d], **column(d))

    def lse_c_copy(d):
        return remote(lse_c.at[xy], lse_c.at[xy], lc_s.at[d], lc_r.at[d], **plane(d))

    for d in COLUMN:
        lse_r_copy(d).start()
    sum_c = jnp.zeros((1, BLOCK), f32)
    for rows in quarters:
        sum_c = sum_c + jnp.sum(jnp.exp(scores[rows] - peak_c), axis=0, keepdims=True)
    log_sum = peak_c + jnp.log(sum_c)

    def as_tile(line):
        return jnp.concatenate(
            [line[:, k * 128 : (k + 1) * 128] for k in range(4)], axis=0
        )

    lse_c[xy] = as_tile(log_sum)
    for d in PLANE:
        lse_c_copy(d).start()

    def combined(parts):
        values = parts[...]
        peak = jnp.max(values, axis=0)
        return peak + jnp.log(jnp.sum(jnp.exp(values - peak[None]), axis=0))

    load_pair.wait()
    held = pair[pl.ds(y * 16 + x // 2, 8, stride=2), :]
    held = jnp.where(x % 2 == 1, pltpu.roll(held, 64, 1), held)
    held = jnp.concatenate([held] * 16, axis=0).T
    captions = jnp.concatenate([held[:64, h * C + k : h * C + k + 1] for k in range(C) for h in range(ZH)], axis=0)
    j = lax.broadcasted_iota(jnp.int32, (1, BLOCK), 1)
    ids = ((j // 128) * 8 + zh * C + c) * 256 + ((j // PIECE) % X) * ROWS + zl * PIECE + j % PIECE

    each(1, ZC, lambda d: lse_r_copy(d).wait_recv())
    total_r = combined(lse_r)
    turned = jnp.concatenate([total_r] * 32, axis=0).T
    each(1, XY, lambda d: lse_c_copy(d).wait_recv())
    total_c = combined(lse_c)
    line_c = jnp.concatenate([total_c[k : k + 1] for k in range(4)], axis=1)
    target = jnp.zeros((1, BLOCK), f32)
    for k, rows in enumerate(quarters):
        s = scores[rows]
        flags = (captions[k * 128 : (k + 1) * 128] == ids).astype(f32)
        target = target + jnp.sum(flags * s, axis=0, keepdims=True)
        w = scale * (jnp.exp(s - turned[:, k : k + 1]) + jnp.exp(s - line_c) - 2.0 * flags)
        weights[rows] = w.astype(bf16)
    shared = (total_r + total_c) * (1.0 / 16)
    loss_1[zc] = shared - 2.0 * as_tile(target)

    def loss_1_copy(d):
        return remote(loss_1.at[zc], loss_1.at[zc], l1_s.at[d], l1_r.at[d], **column(d))

    def loss_2_copy(d):
        return remote(loss_2.at[xy], loss_2.at[xy], l2_s.at[d], l2_r.at[d], **plane(d))

    for d in COLUMN:
        loss_1_copy(d).start()

    def grad_x(d):
        there = (x + d) % X
        return remote(txt_send.at[:, there, :, :HALF_E], sum_x.at[d], gx_s.at[d], gx_r.at[d], mp=there)

    def grad_y(d):
        there = (y + d) % Y
        return remote(txt_send.at[there, :, :, HALF_E:], sum_y.at[d], gy_s.at[d], gy_r.at[d], dp_0=there)

    def grad_xy(d):
        there = (y + d) % Y
        return remote(sent_x.at[there], sum_xy.at[d], gxy_s.at[d], gxy_r.at[d], dp_0=there)

    def grad_yx(d):
        there = (x + d) % X
        return remote(sent_y.at[there], sum_yx.at[d], gyx_s.at[d], gyx_r.at[d], mp=there)

    for k in range(4):
        cols = pl.ds(k * 128, 128)
        value = dot(weights[:, cols], ibuf[:, :HALF_E], ((0,), (0,)))
        txt_send[k, :, :, :HALF_E] = value.reshape(X, PIECE, HALF_E).astype(bf16)
    for d in RING:
        grad_x(d).start()
    d2d = remote(img_d2d, img_d2d_got, d2d_s, d2d_r, dp_2=1 - c)
    rows = pl.ds(pl.multiple_of((1 - c) * SIDE, SIDE), SIDE)
    img_d2d[...] = dot(weights[rows], tbuf[...]).astype(bf16)
    d2d.start()

    for k in range(4):
        cols = pl.ds(k * 128, 128)
        value = dot(weights[:, cols], ibuf[:, HALF_E:], ((0,), (0,)))
        txt_send[k, :, :, HALF_E:] = value.reshape(X, PIECE, HALF_E).astype(bf16)
    for d in RING:
        grad_y(d).start()

    def piece(index):
        return img_send.at[pl.ds(pl.multiple_of((z + index) % Z * PIECE, PIECE), PIECE)]

    def img_next(side):
        return remote(piece((1, 7)[side]), img_near.at[side], in_s.at[side], in_r.at[side], **along((1, 7)[side]))

    def img_third(side):
        return remote(piece((3, 5)[side]), img_third_got.at[side], i3_s.at[side], i3_r.at[side], **along((1, 7)[side]))

    def img_fourth(side):
        start = (z + 4) % Z * PIECE + side * (PIECE // 2)
        part = img_send.at[pl.ds(pl.multiple_of(start, 16), PIECE // 2)]
        return remote(part, img_fourth_got.at[side], i4_s.at[side], i4_r.at[side], **along((2, 6)[side]))

    def img_second(side):
        return remote(img_sum.at[side], img_far.at[side], if_s.at[side], if_r.at[side], **along((2, 6)[side]))

    rows = pl.ds(pl.multiple_of(c * SIDE, SIDE), SIDE)
    value = dot(weights[rows], tbuf[...])
    d2d.wait_recv()
    value = value + img_d2d_got[...].astype(f32)
    img_send[...] = value.astype(bf16)
    for send in (img_fourth, img_third, img_next):
        send(0).start()
        send(1).start()

    each(1, ZC, lambda d: loss_1_copy(d).wait_recv())
    loss_2[xy] = jnp.sum(loss_1[...], axis=0)
    for d in PLANE:
        loss_2_copy(d).start()

    def image_rows(index, start, count):
        return img_send[pl.ds(pl.multiple_of((z + index) % Z * PIECE + start, 16), count)].astype(f32)

    for side in range(2):
        img_fourth(side).wait_recv()
        img_third(side).wait_recv()
        for part in range(2):
            rows = pl.ds(part * (PIECE // 2), PIECE // 2)
            value = image_rows((2, 6)[side], part * (PIECE // 2), PIECE // 2) + img_third_got[side, rows].astype(f32)
            if part == side:
                value = value + img_fourth_got[side].astype(f32)
            img_sum[side, rows] = value.astype(bf16)
        img_second(side).start()

    each(1, X, lambda d: grad_x(d).wait_recv())
    for k in range(Y):
        value = txt_send[k, x, :, :HALF_E].astype(f32)
        for d in range(1, X):
            value = value + sum_x[d, k].astype(f32)
        sent_x[k] = value.astype(bf16)
    for d in RING:
        grad_xy(d).start()
    each(1, Y, lambda d: grad_y(d).wait_recv())
    for k in range(X):
        value = txt_send[y, k, :, HALF_E:].astype(f32)
        for d in range(1, Y):
            value = value + sum_y[d, k].astype(f32)
        sent_y[k] = value.astype(bf16)
    for d in RING:
        grad_yx(d).start()
    def last(part):
        cols = pl.ds(part * HALF_E, HALF_E)
        return remote(fin.at[:, cols], fin_got.at[:, cols], fin_s.at[part], fin_r.at[part], group=1 - zl)

    mine = pl.ds(pl.multiple_of(zl * PIECE, PIECE), PIECE)
    theirs = pl.ds(pl.multiple_of((1 - zl) * PIECE, PIECE), PIECE)
    store = pltpu.make_async_copy(result.at[mine], out.at[0, mine], store_sem.at[0])
    store_theirs = pltpu.make_async_copy(result.at[theirs], out.at[0, theirs], store_sem.at[1])

    def finished_text(part, value):
        cols = pl.ds(part * HALF_E, HALF_E)

        @pl.when(zl == 0)
        def _():
            fin[:, cols] = value.astype(bf16)
            last(part).start()

        @pl.when(zl == 1)
        def _():
            result[PIECE:, cols] = value

    each(1, Y, lambda d: grad_xy(d).wait_recv())
    value = sent_x[y].astype(f32)
    for d in range(1, Y):
        value = value + sum_xy[d].astype(f32)
    finished_text(0, value)
    each(1, X, lambda d: grad_yx(d).wait_recv())
    value = sent_y[x].astype(f32)
    for d in range(1, X):
        value = value + sum_yx[d].astype(f32)
    finished_text(1, value)

    value = image_rows(0, 0, PIECE)
    for side in range(2):
        img_next(side).wait_recv()
        value = value + img_near[side].astype(f32)
    for side in range(2):
        img_second(side).wait_recv()
        value = value + img_far[side].astype(f32)

    @pl.when(zl == 0)
    def _():
        result[:PIECE] = value

    @pl.when(zl == 1)
    def _():
        fin[...] = value.astype(bf16)
        last(0).start()
        last(1).start()

    store.start()
    each(1, XY, lambda d: loss_2_copy(d).wait_recv())
    total = jnp.sum(jnp.sum(loss_2[...], axis=0), axis=0, keepdims=True)
    loss_ref[...] = jnp.sum(total, axis=1, keepdims=True) * (1.0 / (2 * XY * BLOCK))
    store_loss = pltpu.make_async_copy(loss_ref, loss_out, store_sem.at[2])
    store_loss.start()
    last(0).wait_recv()
    last(1).wait_recv()
    result[theirs] = fin_got[...].astype(f32)
    store_theirs.start()

    def sent_ring(d):
        stat_copy(d).wait_send()
        share_t(d).wait_send()
        share_i(d).wait_send()
        text_x(d).wait_send()
        text_y(d).wait_send()
        grad_x(d).wait_send()
        grad_y(d).wait_send()
        grad_xy(d).wait_send()
        grad_yx(d).wait_send()
        for e in range(1, X):
            text_xy(d, e).wait_send()
            text_yx(d, e).wait_send()

    def sent_all(d):
        lse_r_copy(d).wait_send()
        lse_c_copy(d).wait_send()
        loss_1_copy(d).wait_send()
        loss_2_copy(d).wait_send()

    each(1, X, sent_ring)
    for d in (1, 2, 6, 7):
        image_copy(d).wait_send()
    image_on(3).wait_send()
    image_on(5).wait_send()
    image_half(0).wait_send()
    image_half(1).wait_send()
    each(0, Z, lambda d: forward(d).wait_send())
    each(1, XY, sent_all)
    for side in range(2):
        img_next(side).wait_send()
        img_third(side).wait_send()
        img_fourth(side).wait_send()
        img_second(side).wait_send()
    last(0).wait_send()
    last(1).wait_send()
    d2d.wait_send()
    store.wait()
    store_loss.wait()
    store_theirs.wait()


def body(
    image_features, text_features, image_gain, text_gain, image_proj, text_proj, pair, logit_scale
):
    width_i, width_t = image_features.shape[1], text_features.shape[1]
    emb = image_proj.shape[1]
    hbm = pl.BlockSpec(memory_space=pl.ANY)
    dma = lambda *n: pltpu.SemaphoreType.DMA(n)
    grads, loss = pl.pallas_call(
        kernel,
        out_shape=(
            jax.ShapeDtypeStruct((1, ROWS, emb), f32),
            jax.ShapeDtypeStruct((1, 1), f32),
        ),
        in_specs=[hbm] * 8,
        out_specs=(hbm, hbm),
        scratch_shapes=[
            pltpu.VMEM((1, 1), f32),
            pltpu.VMEM((ROWS, emb), f32),
            pltpu.VMEM((1, 1), f32),
            pltpu.VMEM((HALF, width_i), bf16),
            pltpu.VMEM((HALF, width_t), bf16),
            pltpu.VMEM((width_i // 128, 128), f32),
            pltpu.VMEM((width_t // 128, 128), f32),
            pltpu.VMEM((pair.size // 128, 128), jnp.int32),
            pltpu.VMEM((width_i, emb), bf16),
            pltpu.VMEM((width_t, emb), bf16),
            pltpu.VMEM((HALF + 16, width_i), bf16),
            pltpu.VMEM((HALF + 16, width_t), bf16),
            pltpu.VMEM((X, 24, 128), f32),
            pltpu.VMEM((128, 128), f32),
            pltpu.VMEM((HALF, emb), bf16),
            pltpu.VMEM((HALF, emb), bf16),
            pltpu.VMEM((HALF, emb), f32),
            pltpu.VMEM((HALF, emb), f32),
            pltpu.VMEM((X, PIECE, emb), bf16),
            pltpu.VMEM((X, PIECE, emb), bf16),
            pltpu.VMEM((BLOCK, emb), bf16),
            pltpu.VMEM((BLOCK, emb), bf16),
            pltpu.VMEM((BLOCK, BLOCK), f32),
            pltpu.VMEM((BLOCK, BLOCK), bf16),
            pltpu.VMEM((ZC, 4, 128), f32),
            pltpu.VMEM((XY, 4, 128), f32),
            pltpu.VMEM((ZC, 4, 128), f32),
            pltpu.VMEM((XY, 4, 128), f32),
            pltpu.VMEM((SIDE, emb), bf16),
            pltpu.VMEM((SIDE, emb), bf16),
            pltpu.VMEM((SIDE, emb), bf16),
            pltpu.VMEM((2, PIECE, emb), bf16),
            pltpu.VMEM((2, PIECE, emb), bf16),
            pltpu.VMEM((2, PIECE // 2, emb), bf16),
            pltpu.VMEM((2, PIECE, emb), bf16),
            pltpu.VMEM((2, PIECE, emb), bf16),
            pltpu.VMEM((Y, X, PIECE, emb), bf16),
            pltpu.VMEM((X, Y, PIECE, HALF_E), bf16),
            pltpu.VMEM((Y, X, PIECE, HALF_E), bf16),
            pltpu.VMEM((Y, PIECE, HALF_E), bf16),
            pltpu.VMEM((X, PIECE, HALF_E), bf16),
            pltpu.VMEM((Y, PIECE, HALF_E), bf16),
            pltpu.VMEM((X, PIECE, HALF_E), bf16),
            pltpu.VMEM((PIECE, emb), bf16),
            pltpu.VMEM((PIECE, emb), bf16),
            dma(2 * X + 6), dma(3),
            dma(X), dma(X), dma(X), dma(X), dma(X), dma(X),
            dma(Z), dma(Z), dma(2), dma(2), dma(Z), dma(Z), dma(X), dma(X), dma(Y), dma(Y),
            dma(XY), dma(XY), dma(XY), dma(XY),
            dma(ZC), dma(ZC), dma(XY), dma(XY), dma(ZC), dma(ZC), dma(XY), dma(XY),
            pltpu.SemaphoreType.DMA, pltpu.SemaphoreType.DMA,
            dma(2), dma(2), dma(2), dma(2), dma(2), dma(2), dma(2), dma(2),
            dma(X), dma(X), dma(Y), dma(Y), dma(Y), dma(Y), dma(X), dma(X),
            dma(2), dma(2),
        ],
        compiler_params=pltpu.CompilerParams(
            collective_id=0, has_side_effects=True, vmem_limit_bytes=67043328
        ),
        name="contrastive",
    )(
        image_features, text_features, image_gain.reshape(-1, 128), text_gain.reshape(-1, 128),
        image_proj, text_proj, pair.reshape(-1, 128), logit_scale.reshape(1, 1),
    )
    return grads, loss.reshape(())


def solution(mesh):
    split = Mesh(
        mesh.devices.reshape(mesh.shape["group"], 4, 4, 2, mesh.shape["mp"]),
        ("group", "dp_0", "dp_1", "dp_2", "mp"),
    )
    placed = (P(DP, "mp"), P(DP, "mp"), P("mp"), P("mp"), P("mp", None), P("mp", None), P(), P())
    return jax.shard_map(
        body, mesh=split, in_specs=placed, out_specs=(P("group", DP_MP, None), P()), check_vma=False
    )
```

```python
import functools

import jax
import jax.numpy as jnp
from jax import lax
from jax.experimental import pallas as pl
from jax.experimental.pallas import tpu as pltpu
from jax.sharding import Mesh
from jax.sharding import PartitionSpec as P

DP_MP = ("dp_0", "dp_1", "dp_2", "mp")
DP = ("dp_0", "dp_1", "dp_2")
MESH = pl.DeviceIdType.MESH

X, Y, ZH, ZL, C = 4, 4, 4, 2, 2
Z = ZH * ZL
XY = X * Y
ZC = Z * C
PIECE = 32
HALF = X * PIECE
BLOCK = XY * PIECE
ROWS = 2 * PIECE
HALF_E = 512
SIDE = Z * PIECE

epsilon = 1e-05
f32 = jnp.float32
bf16 = jnp.bfloat16


def dot(a, b, dims=((1,), (0,))):
    return lax.dot_general(a, b, (dims, ((), ())), preferred_element_type=f32)


def hops(d, size):
    return min(d, size - d)


PLANE = sorted(range(1, XY), key=lambda d: -hops(d % X, X) - hops(d // X, Y))
COLUMN = sorted(range(1, ZC), key=lambda d: -hops(d % Z, Z))
RING = (2, 1, 3)


def each(low, high, step):
    def turn(i, carry):
        step(i)
        return carry

    lax.fori_loop(low, high, turn, 0)


def kernel(
    feat_i, feat_t, gain_i, gain_t, proj_i, proj_t, pair_hbm, scale_hbm,
    out, loss_out,
    scale_ref, result, loss_ref, fi, ft, gi, gt, pair, pi, pt, lhs_i, lhs_t, stats, moments, part_i, part_t, own_i, own_t, got_i, got_t,
    ibuf, tbuf, scores, weights, lse_r, lse_c, loss_1, loss_2,
    img_d2d, img_d2d_got, img_send, img_near, img_third_got, img_fourth_got, img_sum, img_far,
    txt_send, sum_x, sum_y, sent_x, sent_y, sum_xy, sum_yx, fin, fin_got,
    load_sem, store_sem, stat_s, stat_r, rsi_s, rsi_r, rst_s, rst_r,
    agi_s, agi_r, agh_s, agh_r, fwd_s, fwd_r, agx_s, agx_r, agy_s, agy_r, axy_s, axy_r, ayx_s, ayx_r,
    lr_s, lr_r, lc_s, lc_r, l1_s, l1_r, l2_s, l2_r,
    d2d_s, d2d_r, in_s, in_r, i3_s, i3_r, i4_s, i4_r, if_s, if_r, gx_s, gx_r, gy_s, gy_r, gxy_s, gxy_r, gyx_s, gyx_r, fin_s, fin_r,
):
    x, y = lax.axis_index("mp"), lax.axis_index("dp_0")
    zh, c, zl = lax.axis_index("dp_1"), lax.axis_index("dp_2"), lax.axis_index("group")
    z = zh * ZL + zl
    xy = y * X + x
    zc = c * Z + z

    def remote(src, dst, send, recv, **where):
        return pltpu.make_async_remote_copy(
            src_ref=src, dst_ref=dst, send_sem=send, recv_sem=recv,
            device_id=where, device_id_type=MESH,
        )

    def plane(d):
        return {"mp": (x + d % X) % X, "dp_0": (y + d // X) % Y}

    def column(d):
        there = (z + d % Z) % Z
        return {"dp_1": there // ZL, "group": there % ZL, "dp_2": (c + d // Z) % C}

    loads_i, loads_t = [], []
    for k in range(X):
        rows = pl.ds(pl.multiple_of(k * ROWS + zl * PIECE, PIECE), PIECE)
        here = pl.ds(k * PIECE, PIECE)
        loads_i.append(pltpu.make_async_copy(feat_i.at[rows], fi.at[here], load_sem.at[k]))
        loads_t.append(pltpu.make_async_copy(feat_t.at[rows], ft.at[here], load_sem.at[X + k]))
    loads_i.append(pltpu.make_async_copy(gain_i, gi, load_sem.at[2 * X + 2]))
    loads_t.append(pltpu.make_async_copy(gain_t, gt, load_sem.at[2 * X + 3]))
    loads_p = [
        pltpu.make_async_copy(proj_t, pt, load_sem.at[2 * X]),
        pltpu.make_async_copy(proj_i, pi, load_sem.at[2 * X + 1]),
    ]
    load_pair = pltpu.make_async_copy(pair_hbm, pair, load_sem.at[2 * X + 4])
    load_scale = pltpu.make_async_copy(scale_hbm, scale_ref, load_sem.at[2 * X + 5])
    for copy in loads_i + loads_p[1:] + loads_t + loads_p[:1] + [load_pair, load_scale]:
        copy.start()

    barrier = pltpu.get_barrier_semaphore()

    def greet_plane(d):
        pl.semaphore_signal(barrier, inc=1, device_id=plane(d), device_id_type=MESH)

    def greet_column(d):
        pl.semaphore_signal(barrier, inc=1, device_id=column(d), device_id_type=MESH)

    for d in PLANE:
        greet_plane(d)
    for d in COLUMN:
        greet_column(d)

    lane = lax.broadcasted_iota(jnp.int32, (HALF, 128), 1)

    def centred(features, gain, lhs):
        values = features[...].astype(f32)
        mean = jnp.sum(values, axis=1, keepdims=True) * (1.0 / values.shape[1])
        squares = jnp.sum(values * values, axis=1, keepdims=True)
        line = jnp.concatenate([gain[k : k + 1, :] for k in range(gain.shape[0])], axis=1)
        lhs[:HALF] = ((values - mean) * line).astype(bf16)
        coarse = line.astype(bf16)
        fine = (line - coarse.astype(f32)).astype(bf16)
        lhs[HALF:] = jnp.concatenate([coarse, fine, jnp.zeros((14, line.shape[1]), bf16)], axis=0)
        return mean, squares

    def lines(row_of_all):
        return jnp.concatenate([row_of_all[:, k * 128 : (k + 1) * 128] for k in range(8)], axis=0)

    def share_copy(d, part, got, send, recv):
        there = (x + d) % X
        rows = pl.ds(pl.multiple_of(there * PIECE, PIECE), PIECE)
        return remote(part.at[rows], got.at[d], send.at[d], recv.at[d], mp=there)

    share_t = lambda d: share_copy(d, part_t, got_t, rst_s, rst_r)
    share_i = lambda d: share_copy(d, part_i, got_i, rsi_s, rsi_r)

    def stat_copy(d):
        return remote(stats.at[x], stats.at[x], stat_s.at[d], stat_r.at[d], mp=(x + d) % X)

    for copy in loads_i:
        copy.wait()
    mean_i, squares_i = centred(fi, gi, lhs_i)
    loads_p[1].wait()
    value = dot(lhs_i[...], pi[...])
    own_i[...] = value[:HALF]
    part_i[...] = value[:HALF].astype(bf16)
    pl.semaphore_wait(barrier, XY - 1 + ZC - 1)
    for d in RING:
        share_i(d).start()
    stats[x, 8:16] = lines(value[HALF : HALF + 1] + value[HALF + 1 : HALF + 2])
    for copy in loads_t:
        copy.wait()
    mean_t, squares_t = centred(ft, gt, lhs_t)
    packed = jnp.where(lane == 0, mean_i, 0.0)
    packed = jnp.where(lane == 1, squares_i, packed)
    packed = jnp.where(lane == 2, mean_t, packed)
    packed = jnp.where(lane == 3, squares_t, packed)
    stats[x, :8] = packed.T[:8]
    loads_p[0].wait()
    value = dot(lhs_t[...], pt[...])
    own_t[...] = value[:HALF]
    part_t[...] = value[:HALF].astype(bf16)
    stats[x, 16:] = lines(value[HALF : HALF + 1] + value[HALF + 1 : HALF + 2])
    for d in RING:
        stat_copy(d).start()
    for d in RING:
        share_t(d).start()

    each(1, X, lambda d: stat_copy(d).wait_recv())
    turned = jnp.concatenate([stats[k, :8] for k in range(X)] + [jnp.zeros((96, 128), f32)], axis=0).T
    moments[...] = turned
    moment = moments[pl.ds(pl.multiple_of(x * PIECE, PIECE), PIECE)]

    def unit_of(own, got, which, width):
        means = [moment[:, 8 * k + 2 * which : 8 * k + 2 * which + 1] for k in range(X)]
        squares = [moment[:, 8 * k + 2 * which + 1 : 8 * k + 2 * which + 2] for k in range(X)]
        average = (means[0] + means[1] + means[2] + means[3]) * (1.0 / X)
        spread = (squares[0] + squares[1] + squares[2] + squares[3]) / width - average * average
        value = own[pl.ds(pl.multiple_of(x * PIECE, PIECE), PIECE)]
        for d in range(1, X):
            value = value + got[d].astype(f32)
        for k in range(X):
            gained = stats[k, 8 * (1 + which) : 8 * (2 + which)]
            gained = jnp.concatenate([gained[q : q + 1] for q in range(8)], axis=1)
            value = value + (means[k] - average) * gained
        size = jnp.sum(value * value, axis=1, keepdims=True) + 1e-06 * (spread + epsilon)
        return (value * lax.rsqrt(size)).astype(bf16)

    def slot(buffer, index):
        return buffer.at[pl.ds(pl.multiple_of(index * PIECE, PIECE), PIECE)]

    def half(buffer, index, which):
        return buffer.at[pl.ds(pl.multiple_of(index * PIECE + which * (PIECE // 2), 16), PIECE // 2)]

    def text_x(d):
        mine = slot(tbuf, xy)
        return remote(mine, mine, agx_s.at[d], agx_r.at[d], mp=(x + d) % X)

    def text_y(d):
        mine = slot(tbuf, xy)
        return remote(mine, mine, agy_s.at[d], agy_r.at[d], dp_0=(y + d) % Y)

    def text_xy(d, e):
        held = half(tbuf, y * X + (x + X - d) % X, 0)
        return remote(held, held, axy_s.at[d * 4 + e], axy_r.at[d * 4 + e], dp_0=(y + e) % Y)

    def text_yx(d, e):
        held = half(tbuf, (y + Y - d) % Y * X + x, 1)
        return remote(held, held, ayx_s.at[d * 4 + e], ayx_r.at[d * 4 + e], mp=(x + e) % X)

    def along(d):
        there = (z + d) % Z
        return {"dp_1": there // ZL, "group": there % ZL}

    def image_copy(d):
        mine = slot(ibuf, zc)
        return remote(mine, mine, agi_s.at[d], agi_r.at[d], **along(d))

    def image_on(d):
        held = slot(ibuf, c * Z + (z + Z - (2 if d == 3 else 6)) % Z)
        return remote(held, held, agi_s.at[d], agi_r.at[d], **along(1 if d == 3 else 7))

    def image_half(which):
        held = half(ibuf, c * Z + (z + Z - (2, 6)[which]) % Z, which)
        return remote(held, held, agh_s.at[which], agh_r.at[which], **along((2, 6)[which]))

    def forward(d):
        held = slot(ibuf, c * Z + (z + Z - d) % Z)
        return remote(held, held, fwd_s.at[d], fwd_r.at[d], dp_2=1 - c)

    each(1, X, lambda d: share_i(d).wait_recv())
    ibuf[pl.ds(pl.multiple_of(zc * PIECE, PIECE), PIECE)] = unit_of(own_i, got_i, 0, f32(X * fi.shape[1]))
    for d in (2, 6, 1, 7):
        image_copy(d).start()
    forward(0).start()
    each(1, X, lambda d: share_t(d).wait_recv())
    tbuf[pl.ds(pl.multiple_of(xy * PIECE, PIECE), PIECE)] = unit_of(own_t, got_t, 1, f32(X * ft.shape[1]))
    for d in (1, 3, 2):
        text_x(d).start()
        text_y(d).start()
    for d in (2, 6):
        image_copy(d).wait_recv()
        image_half(0 if d == 2 else 1).start()
        image_on(3 if d == 2 else 5).start()
        forward(d).start()
    for d in (1, 3):
        text_x(d).wait_recv()
        for e in RING:
            text_xy(d, e).start()
        text_y(d).wait_recv()
        for e in RING:
            text_yx(d, e).start()
    for d in (1, 7):
        image_copy(d).wait_recv()
        forward(d).start()
    for d in (2,):
        text_x(d).wait_recv()
        for e in RING:
            text_xy(d, e).start()
        text_y(d).wait_recv()
        for e in RING:
            text_yx(d, e).start()
    for d in (3, 5):
        image_on(d).wait_recv()
        forward(d).start()
    image_half(0).wait_recv()
    image_half(1).wait_recv()
    forward(4).start()
    for d in range(1, X):
        for e in range(1, X):
            text_xy(d, e).wait_recv()
            text_yx(d, e).wait_recv()

    load_scale.wait()
    scale = scale_ref[...]
    quarters = [pl.ds(k * 128, 128) for k in range(BLOCK // 128)]
    packed = jnp.zeros((128, 128), f32)
    for turn in range(4):
        quarter = (c if turn < 2 else 1 - c) * 2 + turn % 2
        rows = pl.ds(pl.multiple_of(quarter * 128, 128), 128)
        if turn == 2:
            each(0, Z, lambda d: forward(d).wait_recv())
        s = scale * dot(ibuf[rows], tbuf[...], ((1,), (1,)))
        scores[rows] = s
        peak = jnp.max(s, axis=1, keepdims=True)
        log_sum = peak + jnp.log(jnp.sum(jnp.exp(s - peak), axis=1, keepdims=True))
        packed = jnp.where(lane == quarter, log_sum, packed)
        high = jnp.max(s, axis=0, keepdims=True)
        if turn == 0:
            peak_c = high
            sum_c = jnp.sum(jnp.exp(s - high), axis=0, keepdims=True)
        else:
            high = jnp.maximum(high, peak_c)
            sum_c = sum_c * jnp.exp(peak_c - high) + jnp.sum(jnp.exp(s - high), axis=0, keepdims=True)
            peak_c = high
    lse_r[zc] = packed.T[:4]

    def lse_r_copy(d):
        return remote(lse_r.at[zc], lse_r.at[zc], lr_s.at[d], lr_r.at[d], **column(d))

    def lse_c_copy(d):
        return remote(lse_c.at[xy], lse_c.at[xy], lc_s.at[d], lc_r.at[d], **plane(d))

    for d in COLUMN:
        lse_r_copy(d).start()
    log_sum = peak_c + jnp.log(sum_c)

    def as_tile(line):
        return jnp.concatenate(
            [line[:, k * 128 : (k + 1) * 128] for k in range(4)], axis=0
        )

    lse_c[xy] = as_tile(log_sum)
    for d in PLANE:
        lse_c_copy(d).start()

    def combined(parts):
        values = parts[...]
        peak = jnp.max(values, axis=0)
        return peak + jnp.log(jnp.sum(jnp.exp(values - peak[None]), axis=0))

    load_pair.wait()
    held = pair[pl.ds(y * 16 + x // 2, 8, stride=2), :]
    held = jnp.where(x % 2 == 1, pltpu.roll(held, 64, 1), held)
    held = jnp.concatenate([held] * 16, axis=0).T
    captions = jnp.concatenate([held[:64, h * C + k : h * C + k + 1] for k in range(C) for h in range(ZH)], axis=0)
    j = lax.broadcasted_iota(jnp.int32, (1, BLOCK), 1)
    ids = ((j // 128) * 8 + zh * C + c) * 256 + ((j // PIECE) % X) * ROWS + zl * PIECE + j % PIECE

    each(1, ZC, lambda d: lse_r_copy(d).wait_recv())
    total_r = combined(lse_r)
    turned = jnp.concatenate([total_r] * 32, axis=0).T
    each(1, XY, lambda d: lse_c_copy(d).wait_recv())
    total_c = combined(lse_c)
    line_c = jnp.concatenate([total_c[k : k + 1] for k in range(4)], axis=1)
    target = jnp.zeros((1, BLOCK), f32)
    for k, rows in enumerate(quarters):
        s = scores[rows]
        flags = (captions[k * 128 : (k + 1) * 128] == ids).astype(f32)
        target = target + jnp.sum(flags * s, axis=0, keepdims=True)
        w = scale * (jnp.exp(s - turned[:, k : k + 1]) + jnp.exp(s - line_c) - 2.0 * flags)
        weights[rows] = w.astype(bf16)
    shared = (total_r + total_c) * (1.0 / 16)
    loss_1[zc] = shared - 2.0 * as_tile(target)

    def loss_1_copy(d):
        return remote(loss_1.at[zc], loss_1.at[zc], l1_s.at[d], l1_r.at[d], **column(d))

    def loss_2_copy(d):
        return remote(loss_2.at[xy], loss_2.at[xy], l2_s.at[d], l2_r.at[d], **plane(d))

    for d in COLUMN:
        loss_1_copy(d).start()

    def grad_x(d):
        there = (x + d) % X
        return remote(txt_send.at[:, there, :, :HALF_E], sum_x.at[d], gx_s.at[d], gx_r.at[d], mp=there)

    def grad_y(d):
        there = (y + d) % Y
        return remote(txt_send.at[there, :, :, HALF_E:], sum_y.at[d], gy_s.at[d], gy_r.at[d], dp_0=there)

    def grad_xy(d):
        there = (y + d) % Y
        return remote(sent_x.at[there], sum_xy.at[d], gxy_s.at[d], gxy_r.at[d], dp_0=there)

    def grad_yx(d):
        there = (x + d) % X
        return remote(sent_y.at[there], sum_yx.at[d], gyx_s.at[d], gyx_r.at[d], mp=there)

    for k in range(4):
        cols = pl.ds(k * 128, 128)
        value = dot(weights[:, cols], ibuf[:, :HALF_E], ((0,), (0,)))
        txt_send[k, :, :, :HALF_E] = value.reshape(X, PIECE, HALF_E).astype(bf16)
    for d in RING:
        grad_x(d).start()
    d2d = remote(img_d2d, img_d2d_got, d2d_s, d2d_r, dp_2=1 - c)
    rows = pl.ds(pl.multiple_of((1 - c) * SIDE, SIDE), SIDE)
    img_d2d[...] = dot(weights[rows], tbuf[...]).astype(bf16)
    d2d.start()

    for k in range(4):
        cols = pl.ds(k * 128, 128)
        value = dot(weights[:, cols], ibuf[:, HALF_E:], ((0,), (0,)))
        txt_send[k, :, :, HALF_E:] = value.reshape(X, PIECE, HALF_E).astype(bf16)
    for d in RING:
        grad_y(d).start()

    def piece(index):
        return img_send.at[pl.ds(pl.multiple_of((z + index) % Z * PIECE, PIECE), PIECE)]

    def img_next(side):
        return remote(piece((1, 7)[side]), img_near.at[side], in_s.at[side], in_r.at[side], **along((1, 7)[side]))

    def img_third(side):
        return remote(piece((3, 5)[side]), img_third_got.at[side], i3_s.at[side], i3_r.at[side], **along((1, 7)[side]))

    def img_fourth(side):
        start = (z + 4) % Z * PIECE + side * (PIECE // 2)
        part = img_send.at[pl.ds(pl.multiple_of(start, 16), PIECE // 2)]
        return remote(part, img_fourth_got.at[side], i4_s.at[side], i4_r.at[side], **along((2, 6)[side]))

    def img_second(side):
        return remote(img_sum.at[side], img_far.at[side], if_s.at[side], if_r.at[side], **along((2, 6)[side]))

    rows = pl.ds(pl.multiple_of(c * SIDE, SIDE), SIDE)
    value = dot(weights[rows], tbuf[...])
    d2d.wait_recv()
    value = value + img_d2d_got[...].astype(f32)
    img_send[...] = value.astype(bf16)
    for send in (img_fourth, img_third, img_next):
        send(0).start()
        send(1).start()

    each(1, ZC, lambda d: loss_1_copy(d).wait_recv())
    loss_2[xy] = jnp.sum(loss_1[...], axis=0)
    for d in PLANE:
        loss_2_copy(d).start()

    def sent_ring(d):
        stat_copy(d).wait_send()
        share_t(d).wait_send()
        share_i(d).wait_send()
        text_x(d).wait_send()
        text_y(d).wait_send()
        for e in range(1, X):
            text_xy(d, e).wait_send()
            text_yx(d, e).wait_send()

    def sent_all(d):
        lse_r_copy(d).wait_send()
        lse_c_copy(d).wait_send()
        loss_1_copy(d).wait_send()

    each(1, X, sent_ring)
    for d in (1, 2, 6, 7):
        image_copy(d).wait_send()
    image_on(3).wait_send()
    image_on(5).wait_send()
    image_half(0).wait_send()
    image_half(1).wait_send()
    each(0, Z, lambda d: forward(d).wait_send())
    each(1, XY, sent_all)
    d2d.wait_send()

    def image_rows(index, start, count):
        return img_send[pl.ds(pl.multiple_of((z + index) % Z * PIECE + start, 16), count)].astype(f32)

    for side in range(2):
        img_fourth(side).wait_recv()
        img_third(side).wait_recv()
        for part in range(2):
            rows = pl.ds(part * (PIECE // 2), PIECE // 2)
            value = image_rows((2, 6)[side], part * (PIECE // 2), PIECE // 2) + img_third_got[side, rows].astype(f32)
            if part == side:
                value = value + img_fourth_got[side].astype(f32)
            img_sum[side, rows] = value.astype(bf16)
        img_second(side).start()

    each(1, X, lambda d: grad_x(d).wait_recv())
    for k in range(Y):
        value = txt_send[k, x, :, :HALF_E].astype(f32)
        for d in range(1, X):
            value = value + sum_x[d, k].astype(f32)
        sent_x[k] = value.astype(bf16)
    for d in RING:
        grad_xy(d).start()
    each(1, Y, lambda d: grad_y(d).wait_recv())
    for k in range(X):
        value = txt_send[y, k, :, HALF_E:].astype(f32)
        for d in range(1, Y):
            value = value + sum_y[d, k].astype(f32)
        sent_y[k] = value.astype(bf16)
    for d in RING:
        grad_yx(d).start()
    def last(part):
        cols = pl.ds(part * HALF_E, HALF_E)
        return remote(fin.at[:, cols], fin_got.at[:, cols], fin_s.at[part], fin_r.at[part], group=1 - zl)

    mine = pl.ds(pl.multiple_of(zl * PIECE, PIECE), PIECE)
    theirs = pl.ds(pl.multiple_of((1 - zl) * PIECE, PIECE), PIECE)
    store = pltpu.make_async_copy(result.at[mine], out.at[0, mine], store_sem.at[0])
    store_theirs = pltpu.make_async_copy(result.at[theirs], out.at[0, theirs], store_sem.at[1])

    def finished_text(part, value):
        cols = pl.ds(part * HALF_E, HALF_E)

        @pl.when(zl == 0)
        def _():
            fin[:, cols] = value.astype(bf16)
            last(part).start()

        @pl.when(zl == 1)
        def _():
            result[PIECE:, cols] = value

    each(1, Y, lambda d: grad_xy(d).wait_recv())
    value = sent_x[y].astype(f32)
    for d in range(1, Y):
        value = value + sum_xy[d].astype(f32)
    finished_text(0, value)
    each(1, X, lambda d: grad_yx(d).wait_recv())
    value = sent_y[x].astype(f32)
    for d in range(1, X):
        value = value + sum_yx[d].astype(f32)
    finished_text(1, value)

    value = image_rows(0, 0, PIECE)
    for side in range(2):
        img_next(side).wait_recv()
        value = value + img_near[side].astype(f32)
    for side in range(2):
        img_second(side).wait_recv()
        value = value + img_far[side].astype(f32)

    @pl.when(zl == 0)
    def _():
        result[:PIECE] = value

    @pl.when(zl == 1)
    def _():
        fin[...] = value.astype(bf16)
        last(0).start()
        last(1).start()

    store.start()
    for side in range(2):
        img_next(side).wait_send()
        img_third(side).wait_send()
        img_fourth(side).wait_send()
    each(1, X, lambda d: grad_x(d).wait_send())
    each(1, X, lambda d: grad_y(d).wait_send())
    each(1, XY, lambda d: loss_2_copy(d).wait_recv())
    total = jnp.sum(jnp.sum(loss_2[...], axis=0), axis=0, keepdims=True)
    loss_ref[...] = jnp.sum(total, axis=1, keepdims=True) * (1.0 / (2 * XY * BLOCK))
    store_loss = pltpu.make_async_copy(loss_ref, loss_out, store_sem.at[2])
    store_loss.start()
    last(0).wait_recv()
    last(1).wait_recv()
    result[theirs] = fin_got[...].astype(f32)
    store_theirs.start()

    each(1, XY, lambda d: loss_2_copy(d).wait_send())
    each(1, X, lambda d: grad_xy(d).wait_send())
    each(1, X, lambda d: grad_yx(d).wait_send())
    for side in range(2):
        img_second(side).wait_send()
        last(side).wait_send()
    store.wait()
    store_loss.wait()
    store_theirs.wait()


def body(
    image_features, text_features, image_gain, text_gain, image_proj, text_proj, pair, logit_scale
):
    width_i, width_t = image_features.shape[1], text_features.shape[1]
    emb = image_proj.shape[1]
    hbm = pl.BlockSpec(memory_space=pl.ANY)
    dma = lambda *n: pltpu.SemaphoreType.DMA(n)
    grads, loss = pl.pallas_call(
        kernel,
        out_shape=(
            jax.ShapeDtypeStruct((1, ROWS, emb), f32),
            jax.ShapeDtypeStruct((1, 1), f32),
        ),
        in_specs=[hbm] * 8,
        out_specs=(hbm, hbm),
        scratch_shapes=[
            pltpu.VMEM((1, 1), f32),
            pltpu.VMEM((ROWS, emb), f32),
            pltpu.VMEM((1, 1), f32),
            pltpu.VMEM((HALF, width_i), bf16),
            pltpu.VMEM((HALF, width_t), bf16),
            pltpu.VMEM((width_i // 128, 128), f32),
            pltpu.VMEM((width_t // 128, 128), f32),
            pltpu.VMEM((pair.size // 128, 128), jnp.int32),
            pltpu.VMEM((width_i, emb), bf16),
            pltpu.VMEM((width_t, emb), bf16),
            pltpu.VMEM((HALF + 16, width_i), bf16),
            pltpu.VMEM((HALF + 16, width_t), bf16),
            pltpu.VMEM((X, 24, 128), f32),
            pltpu.VMEM((128, 128), f32),
            pltpu.VMEM((HALF, emb), bf16),
            pltpu.VMEM((HALF, emb), bf16),
            pltpu.VMEM((HALF, emb), f32),
            pltpu.VMEM((HALF, emb), f32),
            pltpu.VMEM((X, PIECE, emb), bf16),
            pltpu.VMEM((X, PIECE, emb), bf16),
            pltpu.VMEM((BLOCK, emb), bf16),
            pltpu.VMEM((BLOCK, emb), bf16),
            pltpu.VMEM((BLOCK, BLOCK), f32),
            pltpu.VMEM((BLOCK, BLOCK), bf16),
            pltpu.VMEM((ZC, 4, 128), f32),
            pltpu.VMEM((XY, 4, 128), f32),
            pltpu.VMEM((ZC, 4, 128), f32),
            pltpu.VMEM((XY, 4, 128), f32),
            pltpu.VMEM((SIDE, emb), bf16),
            pltpu.VMEM((SIDE, emb), bf16),
            pltpu.VMEM((SIDE, emb), bf16),
            pltpu.VMEM((2, PIECE, emb), bf16),
            pltpu.VMEM((2, PIECE, emb), bf16),
            pltpu.VMEM((2, PIECE // 2, emb), bf16),
            pltpu.VMEM((2, PIECE, emb), bf16),
            pltpu.VMEM((2, PIECE, emb), bf16),
            pltpu.VMEM((Y, X, PIECE, emb), bf16),
            pltpu.VMEM((X, Y, PIECE, HALF_E), bf16),
            pltpu.VMEM((Y, X, PIECE, HALF_E), bf16),
            pltpu.VMEM((Y, PIECE, HALF_E), bf16),
            pltpu.VMEM((X, PIECE, HALF_E), bf16),
            pltpu.VMEM((Y, PIECE, HALF_E), bf16),
            pltpu.VMEM((X, PIECE, HALF_E), bf16),
            pltpu.VMEM((PIECE, emb), bf16),
            pltpu.VMEM((PIECE, emb), bf16),
            dma(2 * X + 6), dma(3),
            dma(X), dma(X), dma(X), dma(X), dma(X), dma(X),
            dma(Z), dma(Z), dma(2), dma(2), dma(Z), dma(Z), dma(X), dma(X), dma(Y), dma(Y),
            dma(XY), dma(XY), dma(XY), dma(XY),
            dma(ZC), dma(ZC), dma(XY), dma(XY), dma(ZC), dma(ZC), dma(XY), dma(XY),
            pltpu.SemaphoreType.DMA, pltpu.SemaphoreType.DMA,
            dma(2), dma(2), dma(2), dma(2), dma(2), dma(2), dma(2), dma(2),
            dma(X), dma(X), dma(Y), dma(Y), dma(Y), dma(Y), dma(X), dma(X),
            dma(2), dma(2),
        ],
        compiler_params=pltpu.CompilerParams(
            collective_id=0, has_side_effects=True, vmem_limit_bytes=67043328
        ),
        name="contrastive",
    )(
        image_features, text_features, image_gain.reshape(-1, 128), text_gain.reshape(-1, 128),
        image_proj, text_proj, pair.reshape(-1, 128), logit_scale.reshape(1, 1),
    )
    return grads, loss.reshape(())


def solution(mesh):
    split = Mesh(
        mesh.devices.reshape(mesh.shape["group"], 4, 4, 2, mesh.shape["mp"]),
        ("group", "dp_0", "dp_1", "dp_2", "mp"),
    )
    placed = (P(DP, "mp"), P(DP, "mp"), P("mp"), P("mp"), P("mp", None), P("mp", None), P(), P())
    return jax.shard_map(
        body, mesh=split, in_specs=placed, out_specs=(P("group", DP_MP, None), P()), check_vma=False
    )
```

```python
import functools

import jax
import jax.numpy as jnp
from jax import lax
from jax.experimental import pallas as pl
from jax.experimental.pallas import tpu as pltpu
from jax.sharding import Mesh
from jax.sharding import PartitionSpec as P

DP_MP = ("dp_0", "dp_1", "dp_2", "mp")
DP = ("dp_0", "dp_1", "dp_2")
MESH = pl.DeviceIdType.MESH

X, Y, ZH, ZL, C = 4, 4, 4, 2, 2
Z = ZH * ZL
XY = X * Y
ZC = Z * C
PIECE = 32
HALF = X * PIECE
BLOCK = XY * PIECE
ROWS = 2 * PIECE
HALF_E = 512
SIDE = Z * PIECE

epsilon = 1e-05
f32 = jnp.float32
bf16 = jnp.bfloat16


def dot(a, b, dims=((1,), (0,))):
    return lax.dot_general(a, b, (dims, ((), ())), preferred_element_type=f32)


def hops(d, size):
    return min(d, size - d)


PLANE = sorted(range(1, XY), key=lambda d: -hops(d % X, X) - hops(d // X, Y))
COLUMN = sorted(range(1, ZC), key=lambda d: -hops(d % Z, Z))
RING = (2, 1, 3)


def each(low, high, step):
    def turn(i, carry):
        step(i)
        return carry

    lax.fori_loop(low, high, turn, 0)


def kernel(
    feat_i, feat_t, gain_i, gain_t, proj_i, proj_t, pair_hbm, scale_hbm,
    out, out_got, loss_out,
    scale_ref, blank, result, loss_ref, fi, ft, gi, gt, pair, pi, pt, lhs_i, lhs_t, stats, moments, part_i, part_t, own_i, own_t, got_i, got_t,
    ibuf, tbuf, scores, weights, lse_r, lse_c, loss_1, loss_2,
    img_d2d, img_d2d_got, img_send, img_near, img_third_got, img_fourth_got, img_sum, img_far,
    txt_a, txt_b, sum_x, sum_y, sent_x, sent_y, sum_xy, sum_yx, fin, fin_got,
    load_sem, store_sem, stat_s, stat_r, rsi_s, rsi_r, rst_s, rst_r,
    agi_s, agi_r, agh_s, agh_r, fwd_s, fwd_r, agx_s, agx_r, agy_s, agy_r, axy_s, axy_r, ayx_s, ayx_r,
    lr_s, lr_r, lc_s, lc_r, l1_s, l1_r, l2_s, l2_r,
    d2d_s, d2d_r, in_s, in_r, i3_s, i3_r, i4_s, i4_r, if_s, if_r, gx_s, gx_r, gy_s, gy_r, gxy_s, gxy_r, gyx_s, gyx_r, fin_s, fin_r,
):
    x, y = lax.axis_index("mp"), lax.axis_index("dp_0")
    zh, c, zl = lax.axis_index("dp_1"), lax.axis_index("dp_2"), lax.axis_index("group")
    z = zh * ZL + zl
    xy = y * X + x
    zc = c * Z + z

    def remote(src, dst, send, recv, **where):
        return pltpu.make_async_remote_copy(
            src_ref=src, dst_ref=dst, send_sem=send, recv_sem=recv,
            device_id=where, device_id_type=MESH,
        )

    def plane(d):
        return {"mp": (x + d % X) % X, "dp_0": (y + d // X) % Y}

    def column(d):
        there = (z + d % Z) % Z
        return {"dp_1": there // ZL, "group": there % ZL, "dp_2": (c + d // Z) % C}

    loads_i, loads_t = [], []
    for k in range(X):
        rows = pl.ds(pl.multiple_of(k * ROWS + zl * PIECE, PIECE), PIECE)
        here = pl.ds(k * PIECE, PIECE)
        loads_i.append(pltpu.make_async_copy(feat_i.at[rows], fi.at[here], load_sem.at[k]))
        loads_t.append(pltpu.make_async_copy(feat_t.at[rows], ft.at[here], load_sem.at[X + k]))
    loads_i.append(pltpu.make_async_copy(gain_i, gi, load_sem.at[2 * X + 2]))
    loads_t.append(pltpu.make_async_copy(gain_t, gt, load_sem.at[2 * X + 3]))
    loads_p = [
        pltpu.make_async_copy(proj_t, pt, load_sem.at[2 * X]),
        pltpu.make_async_copy(proj_i, pi, load_sem.at[2 * X + 1]),
    ]
    load_pair = pltpu.make_async_copy(pair_hbm, pair, load_sem.at[2 * X + 4])
    load_scale = pltpu.make_async_copy(scale_hbm, scale_ref, load_sem.at[2 * X + 5])
    for copy in loads_i + loads_p[1:] + loads_t + loads_p[:1] + [load_pair, load_scale]:
        copy.start()

    barrier = pltpu.get_barrier_semaphore()

    def greet_plane(d):
        pl.semaphore_signal(barrier, inc=1, device_id=plane(d), device_id_type=MESH)

    def greet_column(d):
        pl.semaphore_signal(barrier, inc=1, device_id=column(d), device_id_type=MESH)

    for d in PLANE:
        greet_plane(d)
    for d in COLUMN:
        greet_column(d)

    lane = lax.broadcasted_iota(jnp.int32, (HALF, 128), 1)

    def centred(features, gain, lhs):
        values = features[...].astype(f32)
        mean = jnp.sum(values, axis=1, keepdims=True) * (1.0 / values.shape[1])
        squares = jnp.sum(values * values, axis=1, keepdims=True)
        line = jnp.concatenate([gain[k : k + 1, :] for k in range(gain.shape[0])], axis=1)
        lhs[:HALF] = ((values - mean) * line).astype(bf16)
        coarse = line.astype(bf16)
        fine = (line - coarse.astype(f32)).astype(bf16)
        lhs[HALF:] = jnp.concatenate([coarse, fine, jnp.zeros((14, line.shape[1]), bf16)], axis=0)
        return mean, squares

    def lines(row_of_all):
        return jnp.concatenate([row_of_all[:, k * 128 : (k + 1) * 128] for k in range(8)], axis=0)

    def share_copy(d, part, got, send, recv):
        there = (x + d) % X
        rows = pl.ds(pl.multiple_of(there * PIECE, PIECE), PIECE)
        return remote(part.at[rows], got.at[d], send.at[d], recv.at[d], mp=there)

    share_t = lambda d: share_copy(d, part_t, got_t, rst_s, rst_r)
    share_i = lambda d: share_copy(d, part_i, got_i, rsi_s, rsi_r)

    def stat_copy(d):
        return remote(stats.at[x], stats.at[x], stat_s.at[d], stat_r.at[d], mp=(x + d) % X)

    for copy in loads_i:
        copy.wait()
    mean_i, squares_i = centred(fi, gi, lhs_i)
    loads_p[1].wait()
    value = dot(lhs_i[...], pi[...])
    own_i[...] = value[:HALF]
    part_i[...] = value[:HALF].astype(bf16)
    pl.semaphore_wait(barrier, XY - 1 + ZC - 1)
    for d in RING:
        share_i(d).start()
    stats[x, 8:16] = lines(value[HALF : HALF + 1] + value[HALF + 1 : HALF + 2])
    for copy in loads_t:
        copy.wait()
    mean_t, squares_t = centred(ft, gt, lhs_t)
    packed = jnp.where(lane == 0, mean_i, 0.0)
    packed = jnp.where(lane == 1, squares_i, packed)
    packed = jnp.where(lane == 2, mean_t, packed)
    packed = jnp.where(lane == 3, squares_t, packed)
    stats[x, :8] = packed.T[:8]
    loads_p[0].wait()
    value = dot(lhs_t[...], pt[...])
    own_t[...] = value[:HALF]
    part_t[...] = value[:HALF].astype(bf16)
    stats[x, 16:] = lines(value[HALF : HALF + 1] + value[HALF + 1 : HALF + 2])
    for d in RING:
        stat_copy(d).start()
    for d in RING:
        share_t(d).start()

    each(1, X, lambda d: stat_copy(d).wait_recv())
    turned = jnp.concatenate([stats[k, :8] for k in range(X)] + [jnp.zeros((96, 128), f32)], axis=0).T
    moments[...] = turned
    moment = moments[pl.ds(pl.multiple_of(x * PIECE, PIECE), PIECE)]

    def unit_of(own, got, which, width):
        means = [moment[:, 8 * k + 2 * which : 8 * k + 2 * which + 1] for k in range(X)]
        squares = [moment[:, 8 * k + 2 * which + 1 : 8 * k + 2 * which + 2] for k in range(X)]
        average = (means[0] + means[1] + means[2] + means[3]) * (1.0 / X)
        spread = (squares[0] + squares[1] + squares[2] + squares[3]) / width - average * average
        value = own[pl.ds(pl.multiple_of(x * PIECE, PIECE), PIECE)]
        for d in range(1, X):
            value = value + got[d].astype(f32)
        for k in range(X):
            gained = stats[k, 8 * (1 + which) : 8 * (2 + which)]
            gained = jnp.concatenate([gained[q : q + 1] for q in range(8)], axis=1)
            value = value + (means[k] - average) * gained
        size = jnp.sum(value * value, axis=1, keepdims=True) + 1e-06 * (spread + epsilon)
        return (value * lax.rsqrt(size)).astype(bf16)

    def slot(buffer, index):
        return buffer.at[pl.ds(pl.multiple_of(index * PIECE, PIECE), PIECE)]

    def half(buffer, index, which):
        return buffer.at[pl.ds(pl.multiple_of(index * PIECE + which * (PIECE // 2), 16), PIECE // 2)]

    def text_x(d):
        mine = slot(tbuf, xy)
        return remote(mine, mine, agx_s.at[d], agx_r.at[d], mp=(x + d) % X)

    def text_y(d):
        mine = slot(tbuf, xy)
        return remote(mine, mine, agy_s.at[d], agy_r.at[d], dp_0=(y + d) % Y)

    def text_xy(d, e):
        held = half(tbuf, y * X + (x + X - d) % X, 0)
        return remote(held, held, axy_s.at[d * 4 + e], axy_r.at[d * 4 + e], dp_0=(y + e) % Y)

    def text_yx(d, e):
        held = half(tbuf, (y + Y - d) % Y * X + x, 1)
        return remote(held, held, ayx_s.at[d * 4 + e], ayx_r.at[d * 4 + e], mp=(x + e) % X)

    def along(d):
        there = (z + d) % Z
        return {"dp_1": there // ZL, "group": there % ZL}

    def image_copy(d):
        mine = slot(ibuf, zc)
        return remote(mine, mine, agi_s.at[d], agi_r.at[d], **along(d))

    def image_on(d):
        held = slot(ibuf, c * Z + (z + Z - (2 if d == 3 else 6)) % Z)
        return remote(held, held, agi_s.at[d], agi_r.at[d], **along(1 if d == 3 else 7))

    def image_half(which):
        held = half(ibuf, c * Z + (z + Z - (2, 6)[which]) % Z, which)
        return remote(held, held, agh_s.at[which], agh_r.at[which], **along((2, 6)[which]))

    def forward(d):
        held = slot(ibuf, c * Z + (z + Z - d) % Z)
        return remote(held, held, fwd_s.at[d], fwd_r.at[d], dp_2=1 - c)

    each(1, X, lambda d: share_i(d).wait_recv())
    ibuf[pl.ds(pl.multiple_of(zc * PIECE, PIECE), PIECE)] = unit_of(own_i, got_i, 0, f32(X * fi.shape[1]))
    for d in (2, 6, 1, 7):
        image_copy(d).start()
    forward(0).start()
    each(1, X, lambda d: share_t(d).wait_recv())
    tbuf[pl.ds(pl.multiple_of(xy * PIECE, PIECE), PIECE)] = unit_of(own_t, got_t, 1, f32(X * ft.shape[1]))
    for d in (1, 3, 2):
        text_x(d).start()
        text_y(d).start()
    for d in (2, 6):
        image_copy(d).wait_recv()
        image_half(0 if d == 2 else 1).start()
        image_on(3 if d == 2 else 5).start()
        forward(d).start()
    for d in (1, 3):
        text_x(d).wait_recv()
        for e in RING:
            text_xy(d, e).start()
        text_y(d).wait_recv()
        for e in RING:
            text_yx(d, e).start()
    for d in (1, 7):
        image_copy(d).wait_recv()
        forward(d).start()
    for d in (2,):
        text_x(d).wait_recv()
        for e in RING:
            text_xy(d, e).start()
        text_y(d).wait_recv()
        for e in RING:
            text_yx(d, e).start()
    for d in (3, 5):
        image_on(d).wait_recv()
        forward(d).start()
    image_half(0).wait_recv()
    image_half(1).wait_recv()
    forward(4).start()
    for d in range(1, X):
        for e in range(1, X):
            text_xy(d, e).wait_recv()
            text_yx(d, e).wait_recv()

    load_scale.wait()
    scale = scale_ref[...]
    quarters = [pl.ds(k * 128, 128) for k in range(BLOCK // 128)]
    packed = jnp.zeros((128, 128), f32)
    for turn in range(4):
        quarter = (c if turn < 2 else 1 - c) * 2 + turn % 2
        rows = pl.ds(pl.multiple_of(quarter * 128, 128), 128)
        if turn == 2:
            each(0, Z, lambda d: forward(d).wait_recv())
        s = scale * dot(ibuf[rows], tbuf[...], ((1,), (1,)))
        scores[rows] = s
        peak = jnp.max(s, axis=1, keepdims=True)
        log_sum = peak + jnp.log(jnp.sum(jnp.exp(s - peak), axis=1, keepdims=True))
        packed = jnp.where(lane == quarter, log_sum, packed)
        high = jnp.max(s, axis=0, keepdims=True)
        if turn == 0:
            peak_c = high
            sum_c = jnp.sum(jnp.exp(s - high), axis=0, keepdims=True)
        else:
            high = jnp.maximum(high, peak_c)
            sum_c = sum_c * jnp.exp(peak_c - high) + jnp.sum(jnp.exp(s - high), axis=0, keepdims=True)
            peak_c = high
    lse_r[zc] = packed.T[:4]

    def lse_r_copy(d):
        return remote(lse_r.at[zc], lse_r.at[zc], lr_s.at[d], lr_r.at[d], **column(d))

    def lse_c_copy(d):
        return remote(lse_c.at[xy], lse_c.at[xy], lc_s.at[d], lc_r.at[d], **plane(d))

    for d in COLUMN:
        lse_r_copy(d).start()
    log_sum = peak_c + jnp.log(sum_c)

    def as_tile(line):
        return jnp.concatenate(
            [line[:, k * 128 : (k + 1) * 128] for k in range(4)], axis=0
        )

    lse_c[xy] = as_tile(log_sum)
    for d in PLANE:
        lse_c_copy(d).start()

    def combined(parts):
        values = parts[...]
        peak = jnp.max(values, axis=0)
        return peak + jnp.log(jnp.sum(jnp.exp(values - peak[None]), axis=0))

    load_pair.wait()
    held = pair[pl.ds(y * 16 + x // 2, 8, stride=2), :]
    held = jnp.where(x % 2 == 1, pltpu.roll(held, 64, 1), held)
    held = jnp.concatenate([held] * 16, axis=0).T
    captions = jnp.concatenate([held[:64, h * C + k : h * C + k + 1] for k in range(C) for h in range(ZH)], axis=0)
    j = lax.broadcasted_iota(jnp.int32, (1, BLOCK), 1)
    ids = ((j // 128) * 8 + zh * C + c) * 256 + ((j // PIECE) % X) * ROWS + zl * PIECE + j % PIECE

    each(1, ZC, lambda d: lse_r_copy(d).wait_recv())
    total_r = combined(lse_r)
    turned = jnp.concatenate([total_r] * 32, axis=0).T
    each(1, XY, lambda d: lse_c_copy(d).wait_recv())
    total_c = combined(lse_c)
    line_c = jnp.concatenate([total_c[k : k + 1] for k in range(4)], axis=1)
    target = jnp.zeros((1, BLOCK), f32)
    for k, rows in enumerate(quarters):
        s = scores[rows]
        flags = (captions[k * 128 : (k + 1) * 128] == ids).astype(f32)
        target = target + jnp.sum(flags * s, axis=0, keepdims=True)
        w = scale * (jnp.exp(s - turned[:, k : k + 1]) + jnp.exp(s - line_c) - 2.0 * flags)
        weights[rows] = w.astype(bf16)
    shared = (total_r + total_c) * (1.0 / 16)
    loss_1[zc] = shared - 2.0 * as_tile(target)

    def loss_1_copy(d):
        return remote(loss_1.at[zc], loss_1.at[zc], l1_s.at[d], l1_r.at[d], **column(d))

    def loss_2_copy(d):
        return remote(loss_2.at[xy], loss_2.at[xy], l2_s.at[d], l2_r.at[d], **plane(d))


    def grad_x(d):
        there = (x + d) % X
        return remote(txt_a.at[there], sum_x.at[d], gx_s.at[d], gx_r.at[d], mp=there)

    def grad_y(d):
        there = (y + d) % Y
        return remote(txt_b.at[there], sum_y.at[d], gy_s.at[d], gy_r.at[d], dp_0=there)

    def grad_xy(d):
        there = (y + d) % Y
        return remote(sent_x.at[there], sum_xy.at[d], gxy_s.at[d], gxy_r.at[d], dp_0=there)

    def grad_yx(d):
        there = (x + d) % X
        return remote(sent_y.at[there], sum_yx.at[d], gyx_s.at[d], gyx_r.at[d], mp=there)

    for k in range(4):
        cols = pl.ds(k * 128, 128)
        value = dot(weights[:, cols], ibuf[:, :HALF_E], ((0,), (0,)))
        txt_a[:, k] = value.reshape(X, PIECE, HALF_E).astype(bf16)
    for d in RING:
        grad_x(d).start()
    d2d = remote(img_d2d, img_d2d_got, d2d_s, d2d_r, dp_2=1 - c)
    rows = pl.ds(pl.multiple_of((1 - c) * SIDE, SIDE), SIDE)
    img_d2d[...] = dot(weights[rows], tbuf[...]).astype(bf16)
    d2d.start()
    for d in COLUMN:
        loss_1_copy(d).start()

    for k in range(4):
        cols = pl.ds(k * 128, 128)
        value = dot(weights[:, cols], ibuf[:, HALF_E:], ((0,), (0,)))
        txt_b[k] = value.reshape(X, PIECE, HALF_E).astype(bf16)
    for d in RING:
        grad_y(d).start()

    def piece(index):
        return img_send.at[pl.ds(pl.multiple_of((z + index) % Z * PIECE, PIECE), PIECE)]

    def img_next(side):
        return remote(piece((1, 7)[side]), img_near.at[side], in_s.at[side], in_r.at[side], **along((1, 7)[side]))

    def img_third(side):
        return remote(piece((3, 5)[side]), img_third_got.at[side], i3_s.at[side], i3_r.at[side], **along((1, 7)[side]))

    def img_fourth(side):
        start = (z + 4) % Z * PIECE + side * (PIECE // 2)
        part = img_send.at[pl.ds(pl.multiple_of(start, 16), PIECE // 2)]
        return remote(part, img_fourth_got.at[side], i4_s.at[side], i4_r.at[side], **along((2, 6)[side]))

    def img_second(side):
        return remote(img_sum.at[side], img_far.at[side], if_s.at[side], if_r.at[side], **along((2, 6)[side]))

    rows = pl.ds(pl.multiple_of(c * SIDE, SIDE), SIDE)
    value = dot(weights[rows], tbuf[...])
    d2d.wait_recv()
    value = value + img_d2d_got[...].astype(f32)
    img_send[...] = value.astype(bf16)
    for send in (img_fourth, img_third, img_next):
        send(0).start()
        send(1).start()

    each(1, ZC, lambda d: loss_1_copy(d).wait_recv())
    loss_2[xy] = jnp.sum(loss_1[...], axis=0)
    for d in PLANE:
        loss_2_copy(d).start()

    def sent_ring(d):
        stat_copy(d).wait_send()
        share_t(d).wait_send()
        share_i(d).wait_send()
        text_x(d).wait_send()
        text_y(d).wait_send()
        for e in range(1, X):
            text_xy(d, e).wait_send()
            text_yx(d, e).wait_send()

    def sent_all(d):
        lse_r_copy(d).wait_send()
        lse_c_copy(d).wait_send()
        loss_1_copy(d).wait_send()

    each(1, X, sent_ring)
    for d in (1, 2, 6, 7):
        image_copy(d).wait_send()
    image_on(3).wait_send()
    image_on(5).wait_send()
    image_half(0).wait_send()
    image_half(1).wait_send()
    each(0, Z, lambda d: forward(d).wait_send())
    each(1, XY, sent_all)
    d2d.wait_send()

    mine = pl.ds(pl.multiple_of(zl * PIECE, PIECE), PIECE)
    theirs = pl.ds(pl.multiple_of((1 - zl) * PIECE, PIECE), PIECE)
    store = pltpu.make_async_copy(result.at[mine], out.at[0, mine], store_sem.at[0])
    store_theirs = pltpu.make_async_copy(fin_got, out_got.at[0, theirs], store_sem.at[1])
    blank[...] = jnp.zeros_like(blank)
    result[theirs] = jnp.zeros((PIECE, result.shape[1]), f32)
    blanks = [
        pltpu.make_async_copy(blank, out_got.at[0, mine], store_sem.at[3]),
        pltpu.make_async_copy(result.at[theirs], out.at[0, theirs], store_sem.at[4]),
    ]
    for copy in blanks:
        copy.start()

    def image_rows(index, start, count):
        return img_send[pl.ds(pl.multiple_of((z + index) % Z * PIECE + start, 16), count)].astype(f32)

    for side in range(2):
        img_fourth(side).wait_recv()
        img_third(side).wait_recv()
        for part in range(2):
            rows = pl.ds(part * (PIECE // 2), PIECE // 2)
            value = image_rows((2, 6)[side], part * (PIECE // 2), PIECE // 2) + img_third_got[side, rows].astype(f32)
            if part == side:
                value = value + img_fourth_got[side].astype(f32)
            img_sum[side, rows] = value.astype(bf16)
        img_second(side).start()

    each(1, X, lambda d: grad_x(d).wait_recv())
    for e in RING + (0,):
        k = (y + e) % Y
        value = txt_a[x, k].astype(f32)
        for d in range(1, X):
            value = value + sum_x[d, k].astype(f32)
        sent_x[k] = value.astype(bf16)
        if e:
            grad_xy(e).start()
    each(1, Y, lambda d: grad_y(d).wait_recv())
    for e in RING + (0,):
        k = (x + e) % X
        value = txt_b[y, k].astype(f32)
        for d in range(1, Y):
            value = value + sum_y[d, k].astype(f32)
        sent_y[k] = value.astype(bf16)
        if e:
            grad_yx(e).start()
    def last(part):
        cols = pl.ds(part * HALF_E, HALF_E)
        return remote(fin.at[:, cols], fin_got.at[:, cols], fin_s.at[part], fin_r.at[part], group=1 - zl)

    def finished_text(part, value):
        cols = pl.ds(part * HALF_E, HALF_E)

        @pl.when(zl == 0)
        def _():
            fin[:, cols] = value.astype(bf16)
            last(part).start()

        @pl.when(zl == 1)
        def _():
            result[PIECE:, cols] = value

    each(1, Y, lambda d: grad_xy(d).wait_recv())
    value = sent_x[y].astype(f32)
    for d in range(1, Y):
        value = value + sum_xy[d].astype(f32)
    finished_text(0, value)
    each(1, X, lambda d: grad_yx(d).wait_recv())
    value = sent_y[x].astype(f32)
    for d in range(1, X):
        value = value + sum_yx[d].astype(f32)
    finished_text(1, value)

    value = image_rows(0, 0, PIECE)
    for side in range(2):
        img_next(side).wait_recv()
        value = value + img_near[side].astype(f32)
    for side in range(2):
        img_second(side).wait_recv()
        value = value + img_far[side].astype(f32)

    @pl.when(zl == 0)
    def _():
        result[:PIECE] = value

    @pl.when(zl == 1)
    def _():
        fin[...] = value.astype(bf16)
        last(0).start()
        last(1).start()

    store.start()
    for side in range(2):
        img_next(side).wait_send()
        img_third(side).wait_send()
        img_fourth(side).wait_send()
    each(1, X, lambda d: grad_x(d).wait_send())
    each(1, X, lambda d: grad_y(d).wait_send())
    each(1, XY, lambda d: loss_2_copy(d).wait_recv())
    total = jnp.sum(jnp.sum(loss_2[...], axis=0), axis=0, keepdims=True)
    loss_ref[...] = jnp.sum(total, axis=1, keepdims=True) * (1.0 / (2 * XY * BLOCK))
    store_loss = pltpu.make_async_copy(loss_ref, loss_out, store_sem.at[2])
    store_loss.start()
    last(0).wait_recv()
    last(1).wait_recv()
    store_theirs.start()

    each(1, XY, lambda d: loss_2_copy(d).wait_send())
    each(1, X, lambda d: grad_xy(d).wait_send())
    each(1, X, lambda d: grad_yx(d).wait_send())
    for side in range(2):
        img_second(side).wait_send()
        last(side).wait_send()
    for copy in blanks:
        copy.wait()
    store.wait()
    store_loss.wait()
    store_theirs.wait()


def body(
    image_features, text_features, image_gain, text_gain, image_proj, text_proj, pair, logit_scale
):
    width_i, width_t = image_features.shape[1], text_features.shape[1]
    emb = image_proj.shape[1]
    hbm = pl.BlockSpec(memory_space=pl.ANY)
    dma = lambda *n: pltpu.SemaphoreType.DMA(n)
    grads, got, loss = pl.pallas_call(
        kernel,
        out_shape=(
            jax.ShapeDtypeStruct((1, ROWS, emb), f32),
            jax.ShapeDtypeStruct((1, ROWS, emb), bf16),
            jax.ShapeDtypeStruct((1, 1), f32),
        ),
        in_specs=[hbm] * 8,
        out_specs=(hbm, hbm, hbm),
        scratch_shapes=[
            pltpu.VMEM((1, 1), f32),
            pltpu.VMEM((PIECE, emb), bf16),
            pltpu.VMEM((ROWS, emb), f32),
            pltpu.VMEM((1, 1), f32),
            pltpu.VMEM((HALF, width_i), bf16),
            pltpu.VMEM((HALF, width_t), bf16),
            pltpu.VMEM((width_i // 128, 128), f32),
            pltpu.VMEM((width_t // 128, 128), f32),
            pltpu.VMEM((pair.size // 128, 128), jnp.int32),
            pltpu.VMEM((width_i, emb), bf16),
            pltpu.VMEM((width_t, emb), bf16),
            pltpu.VMEM((HALF + 16, width_i), bf16),
            pltpu.VMEM((HALF + 16, width_t), bf16),
            pltpu.VMEM((X, 24, 128), f32),
            pltpu.VMEM((128, 128), f32),
            pltpu.VMEM((HALF, emb), bf16),
            pltpu.VMEM((HALF, emb), bf16),
            pltpu.VMEM((HALF, emb), f32),
            pltpu.VMEM((HALF, emb), f32),
            pltpu.VMEM((X, PIECE, emb), bf16),
            pltpu.VMEM((X, PIECE, emb), bf16),
            pltpu.VMEM((BLOCK, emb), bf16),
            pltpu.VMEM((BLOCK, emb), bf16),
            pltpu.VMEM((BLOCK, BLOCK), f32),
            pltpu.VMEM((BLOCK, BLOCK), bf16),
            pltpu.VMEM((ZC, 4, 128), f32),
            pltpu.VMEM((XY, 4, 128), f32),
            pltpu.VMEM((ZC, 4, 128), f32),
            pltpu.VMEM((XY, 4, 128), f32),
            pltpu.VMEM((SIDE, emb), bf16),
            pltpu.VMEM((SIDE, emb), bf16),
            pltpu.VMEM((SIDE, emb), bf16),
            pltpu.VMEM((2, PIECE, emb), bf16),
            pltpu.VMEM((2, PIECE, emb), bf16),
            pltpu.VMEM((2, PIECE // 2, emb), bf16),
            pltpu.VMEM((2, PIECE, emb), bf16),
            pltpu.VMEM((2, PIECE, emb), bf16),
            pltpu.VMEM((X, Y, PIECE, HALF_E), bf16),
            pltpu.VMEM((Y, X, PIECE, HALF_E), bf16),
            pltpu.VMEM((X, Y, PIECE, HALF_E), bf16),
            pltpu.VMEM((Y, X, PIECE, HALF_E), bf16),
            pltpu.VMEM((Y, PIECE, HALF_E), bf16),
            pltpu.VMEM((X, PIECE, HALF_E), bf16),
            pltpu.VMEM((Y, PIECE, HALF_E), bf16),
            pltpu.VMEM((X, PIECE, HALF_E), bf16),
            pltpu.VMEM((PIECE, emb), bf16),
            pltpu.VMEM((PIECE, emb), bf16),
            dma(2 * X + 6), dma(5),
            dma(X), dma(X), dma(X), dma(X), dma(X), dma(X),
            dma(Z), dma(Z), dma(2), dma(2), dma(Z), dma(Z), dma(X), dma(X), dma(Y), dma(Y),
            dma(XY), dma(XY), dma(XY), dma(XY),
            dma(ZC), dma(ZC), dma(XY), dma(XY), dma(ZC), dma(ZC), dma(XY), dma(XY),
            pltpu.SemaphoreType.DMA, pltpu.SemaphoreType.DMA,
            dma(2), dma(2), dma(2), dma(2), dma(2), dma(2), dma(2), dma(2),
            dma(X), dma(X), dma(Y), dma(Y), dma(Y), dma(Y), dma(X), dma(X),
            dma(2), dma(2),
        ],
        compiler_params=pltpu.CompilerParams(
            collective_id=0, has_side_effects=True, vmem_limit_bytes=67043328
        ),
        name="contrastive",
    )(
        image_features, text_features, image_gain.reshape(-1, 128), text_gain.reshape(-1, 128),
        image_proj, text_proj, pair.reshape(-1, 128), logit_scale.reshape(1, 1),
    )
    return grads + got.astype(f32), loss.reshape(())


def solution(mesh):
    split = Mesh(
        mesh.devices.reshape(mesh.shape["group"], 4, 4, 2, mesh.shape["mp"]),
        ("group", "dp_0", "dp_1", "dp_2", "mp"),
    )
    placed = (P(DP, "mp"), P(DP, "mp"), P("mp"), P("mp"), P("mp", None), P("mp", None), P(), P())
    return jax.shard_map(
        body, mesh=split, in_specs=placed, out_specs=(P("group", DP_MP, None), P()), check_vma=False
    )
```

```python
import functools

import jax
import jax.numpy as jnp
from jax import lax
from jax.experimental import pallas as pl
from jax.experimental.pallas import tpu as pltpu
from jax.sharding import Mesh
from jax.sharding import PartitionSpec as P

DP_MP = ("dp_0", "dp_1", "dp_2", "mp")
DP = ("dp_0", "dp_1", "dp_2")
MESH = pl.DeviceIdType.MESH

X, Y, ZH, ZL, C = 4, 4, 4, 2, 2
Z = ZH * ZL
XY = X * Y
ZC = Z * C
PIECE = 32
HALF = X * PIECE
BLOCK = XY * PIECE
ROWS = 2 * PIECE
HALF_E = 512
SIDE = Z * PIECE

epsilon = 1e-05
f32 = jnp.float32
bf16 = jnp.bfloat16


def dot(a, b, dims=((1,), (0,))):
    return lax.dot_general(a, b, (dims, ((), ())), preferred_element_type=f32)


def hops(d, size):
    return min(d, size - d)


PLANE = sorted(range(1, XY), key=lambda d: -hops(d % X, X) - hops(d // X, Y))
COLUMN = sorted(range(1, ZC), key=lambda d: -hops(d % Z, Z))
RING = (2, 1, 3)


def each(low, high, step):
    def turn(i, carry):
        step(i)
        return carry

    lax.fori_loop(low, high, turn, 0)


def kernel(
    feat_i, feat_t, gain_i, gain_t, proj_i, proj_t, pair_hbm, scale_hbm,
    out, loss_out,
    scale_ref, result, loss_ref, fi, ft, gi, gt, pair, pi, pt, lhs_i, lhs_t, stats, moments, part_i, part_t, own_i, own_t, got_i, got_t,
    ibuf, tbuf, scores, weights, lse_r, lse_c, loss_1, loss_2, loss_3,
    img_d2d, img_d2d_got, img_send, img_near, img_third_got, img_fourth_got, img_sum, img_far,
    txt_send, sum_x, sum_y, sent_x, sent_y, sum_xy, sum_yx, fin, fin_got,
    load_sem, store_sem, stat_s, stat_r, rsi_s, rsi_r, rst_s, rst_r,
    agi_s, agi_r, agh_s, agh_r, fwd_s, fwd_r, agx_s, agx_r, agy_s, agy_r, axy_s, axy_r, ayx_s, ayx_r,
    lr_s, lr_r, lc_s, lc_r, l1_s, l1_r, l2_s, l2_r, l3_s, l3_r,
    d2d_s, d2d_r, in_s, in_r, i3_s, i3_r, i4_s, i4_r, if_s, if_r, gx_s, gx_r, gy_s, gy_r, gxy_s, gxy_r, gyx_s, gyx_r, fin_s, fin_r,
):
    x, y = lax.axis_index("mp"), lax.axis_index("dp_0")
    zh, c, zl = lax.axis_index("dp_1"), lax.axis_index("dp_2"), lax.axis_index("group")
    z = zh * ZL + zl
    xy = y * X + x
    zc = c * Z + z

    def remote(src, dst, send, recv, **where):
        return pltpu.make_async_remote_copy(
            src_ref=src, dst_ref=dst, send_sem=send, recv_sem=recv,
            device_id=where, device_id_type=MESH,
        )

    def plane(d):
        return {"mp": (x + d % X) % X, "dp_0": (y + d // X) % Y}

    def column(d):
        there = (z + d % Z) % Z
        return {"dp_1": there // ZL, "group": there % ZL, "dp_2": (c + d // Z) % C}

    loads_i, loads_t = [], []
    for k in range(X):
        rows = pl.ds(pl.multiple_of(k * ROWS + zl * PIECE, PIECE), PIECE)
        here = pl.ds(k * PIECE, PIECE)
        loads_i.append(pltpu.make_async_copy(feat_i.at[rows], fi.at[here], load_sem.at[k]))
        loads_t.append(pltpu.make_async_copy(feat_t.at[rows], ft.at[here], load_sem.at[X + k]))
    loads_i.append(pltpu.make_async_copy(gain_i, gi, load_sem.at[2 * X + 2]))
    loads_t.append(pltpu.make_async_copy(gain_t, gt, load_sem.at[2 * X + 3]))
    loads_p = [
        pltpu.make_async_copy(proj_t, pt, load_sem.at[2 * X]),
        pltpu.make_async_copy(proj_i, pi, load_sem.at[2 * X + 1]),
    ]
    load_pair = pltpu.make_async_copy(pair_hbm, pair, load_sem.at[2 * X + 4])
    load_scale = pltpu.make_async_copy(scale_hbm, scale_ref, load_sem.at[2 * X + 5])
    for copy in loads_i + loads_p[1:] + loads_t + loads_p[:1] + [load_pair, load_scale]:
        copy.start()

    barrier = pltpu.get_barrier_semaphore()

    def greet_plane(d):
        pl.semaphore_signal(barrier, inc=1, device_id=plane(d), device_id_type=MESH)

    def greet_column(d):
        pl.semaphore_signal(barrier, inc=1, device_id=column(d), device_id_type=MESH)

    for d in PLANE:
        greet_plane(d)
    for d in COLUMN:
        greet_column(d)

    lane = lax.broadcasted_iota(jnp.int32, (HALF, 128), 1)

    def centred(features, gain, lhs):
        values = features[...].astype(f32)
        mean = jnp.sum(values, axis=1, keepdims=True) * (1.0 / values.shape[1])
        squares = jnp.sum(values * values, axis=1, keepdims=True)
        line = jnp.concatenate([gain[k : k + 1, :] for k in range(gain.shape[0])], axis=1)
        lhs[:HALF] = ((values - mean) * line).astype(bf16)
        coarse = line.astype(bf16)
        fine = (line - coarse.astype(f32)).astype(bf16)
        lhs[HALF:] = jnp.concatenate([coarse, fine, jnp.zeros((14, line.shape[1]), bf16)], axis=0)
        return mean, squares

    def lines(row_of_all):
        return jnp.concatenate([row_of_all[:, k * 128 : (k + 1) * 128] for k in range(8)], axis=0)

    def share_copy(d, part, got, send, recv):
        there = (x + d) % X
        rows = pl.ds(pl.multiple_of(there * PIECE, PIECE), PIECE)
        return remote(part.at[rows], got.at[d], send.at[d], recv.at[d], mp=there)

    share_t = lambda d: share_copy(d, part_t, got_t, rst_s, rst_r)
    share_i = lambda d: share_copy(d, part_i, got_i, rsi_s, rsi_r)

    def stat_copy(d):
        return remote(stats.at[x], stats.at[x], stat_s.at[d], stat_r.at[d], mp=(x + d) % X)

    for copy in loads_i:
        copy.wait()
    mean_i, squares_i = centred(fi, gi, lhs_i)
    loads_p[1].wait()
    value = dot(lhs_i[...], pi[...])
    own_i[...] = value[:HALF]
    part_i[...] = value[:HALF].astype(bf16)
    pl.semaphore_wait(barrier, XY - 1 + ZC - 1)
    for d in RING:
        share_i(d).start()
    stats[x, 8:16] = lines(value[HALF : HALF + 1] + value[HALF + 1 : HALF + 2])
    for copy in loads_t:
        copy.wait()
    mean_t, squares_t = centred(ft, gt, lhs_t)
    packed = jnp.where(lane == 0, mean_i, 0.0)
    packed = jnp.where(lane == 1, squares_i, packed)
    packed = jnp.where(lane == 2, mean_t, packed)
    packed = jnp.where(lane == 3, squares_t, packed)
    stats[x, :8] = packed.T[:8]
    loads_p[0].wait()
    value = dot(lhs_t[...], pt[...])
    own_t[...] = value[:HALF]
    part_t[...] = value[:HALF].astype(bf16)
    stats[x, 16:] = lines(value[HALF : HALF + 1] + value[HALF + 1 : HALF + 2])
    for d in RING:
        stat_copy(d).start()
    for d in RING:
        share_t(d).start()

    each(1, X, lambda d: stat_copy(d).wait_recv())
    turned = jnp.concatenate([stats[k, :8] for k in range(X)] + [jnp.zeros((96, 128), f32)], axis=0).T
    moments[...] = turned
    moment = moments[pl.ds(pl.multiple_of(x * PIECE, PIECE), PIECE)]

    def unit_of(own, got, which, width):
        means = [moment[:, 8 * k + 2 * which : 8 * k + 2 * which + 1] for k in range(X)]
        squares = [moment[:, 8 * k + 2 * which + 1 : 8 * k + 2 * which + 2] for k in range(X)]
        average = (means[0] + means[1] + means[2] + means[3]) * (1.0 / X)
        spread = (squares[0] + squares[1] + squares[2] + squares[3]) / width - average * average
        value = own[pl.ds(pl.multiple_of(x * PIECE, PIECE), PIECE)]
        for d in range(1, X):
            value = value + got[d].astype(f32)
        for k in range(X):
            gained = stats[k, 8 * (1 + which) : 8 * (2 + which)]
            gained = jnp.concatenate([gained[q : q + 1] for q in range(8)], axis=1)
            value = value + (means[k] - average) * gained
        size = jnp.sum(value * value, axis=1, keepdims=True) + 1e-06 * (spread + epsilon)
        return (value * lax.rsqrt(size)).astype(bf16)

    def slot(buffer, index):
        return buffer.at[pl.ds(pl.multiple_of(index * PIECE, PIECE), PIECE)]

    def half(buffer, index, which):
        return buffer.at[pl.ds(pl.multiple_of(index * PIECE + which * (PIECE // 2), 16), PIECE // 2)]

    def text_x(d):
        mine = slot(tbuf, xy)
        return remote(mine, mine, agx_s.at[d], agx_r.at[d], mp=(x + d) % X)

    def text_y(d):
        mine = slot(tbuf, xy)
        return remote(mine, mine, agy_s.at[d], agy_r.at[d], dp_0=(y + d) % Y)

    def text_xy(d, e):
        held = half(tbuf, y * X + (x + X - d) % X, 0)
        return remote(held, held, axy_s.at[d * 4 + e], axy_r.at[d * 4 + e], dp_0=(y + e) % Y)

    def text_yx(d, e):
        held = half(tbuf, (y + Y - d) % Y * X + x, 1)
        return remote(held, held, ayx_s.at[d * 4 + e], ayx_r.at[d * 4 + e], mp=(x + e) % X)

    def along(d):
        there = (z + d) % Z
        return {"dp_1": there // ZL, "group": there % ZL}

    def image_copy(d):
        mine = slot(ibuf, zc)
        return remote(mine, mine, agi_s.at[d], agi_r.at[d], **along(d))

    def image_on(d):
        held = slot(ibuf, c * Z + (z + Z - (2 if d == 3 else 6)) % Z)
        return remote(held, held, agi_s.at[d], agi_r.at[d], **along(1 if d == 3 else 7))

    def image_half(which):
        held = half(ibuf, c * Z + (z + Z - (2, 6)[which]) % Z, which)
        return remote(held, held, agh_s.at[which], agh_r.at[which], **along((2, 6)[which]))

    def forward(d):
        held = slot(ibuf, c * Z + (z + Z - d) % Z)
        return remote(held, held, fwd_s.at[d], fwd_r.at[d], dp_2=1 - c)

    each(1, X, lambda d: share_i(d).wait_recv())
    ibuf[pl.ds(pl.multiple_of(zc * PIECE, PIECE), PIECE)] = unit_of(own_i, got_i, 0, f32(X * fi.shape[1]))
    for d in (2, 6, 1, 7):
        image_copy(d).start()
    forward(0).start()
    each(1, X, lambda d: share_t(d).wait_recv())
    tbuf[pl.ds(pl.multiple_of(xy * PIECE, PIECE), PIECE)] = unit_of(own_t, got_t, 1, f32(X * ft.shape[1]))
    for d in (1, 3, 2):
        text_x(d).start()
        text_y(d).start()
    for d in (2, 6):
        image_copy(d).wait_recv()
        image_half(0 if d == 2 else 1).start()
        image_on(3 if d == 2 else 5).start()
        forward(d).start()
    for d in (1, 3):
        text_x(d).wait_recv()
        for e in RING:
            text_xy(d, e).start()
        text_y(d).wait_recv()
        for e in RING:
            text_yx(d, e).start()
    for d in (1, 7):
        image_copy(d).wait_recv()
        forward(d).start()
    for d in (2,):
        text_x(d).wait_recv()
        for e in RING:
            text_xy(d, e).start()
        text_y(d).wait_recv()
        for e in RING:
            text_yx(d, e).start()
    for d in (3, 5):
        image_on(d).wait_recv()
        forward(d).start()
    image_half(0).wait_recv()
    image_half(1).wait_recv()
    forward(4).start()
    for d in range(1, X):
        for e in range(1, X):
            text_xy(d, e).wait_recv()
            text_yx(d, e).wait_recv()

    load_scale.wait()
    scale = scale_ref[...]
    quarters = [pl.ds(k * 128, 128) for k in range(BLOCK // 128)]
    packed = jnp.zeros((128, 128), f32)
    for turn in range(4):
        quarter = (c if turn < 2 else 1 - c) * 2 + turn % 2
        rows = pl.ds(pl.multiple_of(quarter * 128, 128), 128)
        if turn == 2:
            each(0, Z, lambda d: forward(d).wait_recv())
        s = scale * dot(ibuf[rows], tbuf[...], ((1,), (1,)))
        scores[rows] = s
        peak = jnp.max(s, axis=1, keepdims=True)
        log_sum = peak + jnp.log(jnp.sum(jnp.exp(s - peak), axis=1, keepdims=True))
        packed = jnp.where(lane == quarter, log_sum, packed)
        high = jnp.max(s, axis=0, keepdims=True)
        if turn == 0:
            peak_c = high
            sum_c = jnp.sum(jnp.exp(s - high), axis=0, keepdims=True)
        else:
            high = jnp.maximum(high, peak_c)
            sum_c = sum_c * jnp.exp(peak_c - high) + jnp.sum(jnp.exp(s - high), axis=0, keepdims=True)
            peak_c = high
    lse_r[zc] = packed.T[:4]

    def lse_r_copy(d):
        return remote(lse_r.at[zc], lse_r.at[zc], lr_s.at[d], lr_r.at[d], **column(d))

    def lse_c_copy(d):
        return remote(lse_c.at[xy], lse_c.at[xy], lc_s.at[d], lc_r.at[d], **plane(d))

    for d in COLUMN:
        lse_r_copy(d).start()
    log_sum = peak_c + jnp.log(sum_c)

    def as_tile(line):
        return jnp.concatenate(
            [line[:, k * 128 : (k + 1) * 128] for k in range(4)], axis=0
        )

    lse_c[xy] = as_tile(log_sum)
    for d in PLANE:
        lse_c_copy(d).start()

    def combined(parts):
        values = parts[...]
        peak = jnp.max(values, axis=0)
        return peak + jnp.log(jnp.sum(jnp.exp(values - peak[None]), axis=0))

    load_pair.wait()
    held = pair[pl.ds(y * 16 + x // 2, 8, stride=2), :]
    held = jnp.where(x % 2 == 1, pltpu.roll(held, 64, 1), held)
    held = jnp.concatenate([held] * 16, axis=0).T
    captions = jnp.concatenate([held[:64, h * C + k : h * C + k + 1] for k in range(C) for h in range(ZH)], axis=0)
    j = lax.broadcasted_iota(jnp.int32, (1, BLOCK), 1)
    ids = ((j // 128) * 8 + zh * C + c) * 256 + ((j // PIECE) % X) * ROWS + zl * PIECE + j % PIECE

    def loss_1_copy(d):
        return remote(loss_1.at[zc], loss_1.at[zc], l1_s.at[d], l1_r.at[d], **column(d))

    def loss_2_copy(d):
        return remote(loss_2.at[xy], loss_2.at[xy], l2_s.at[d], l2_r.at[d], **plane(d))

    def loss_3_copy(d):
        return remote(loss_3.at[zc], loss_3.at[zc], l3_s.at[d], l3_r.at[d], **column(d))

    target = jnp.zeros((1, BLOCK), f32)
    for k, rows in enumerate(quarters):
        flags = (captions[k * 128 : (k + 1) * 128] == ids).astype(f32)
        target = target + jnp.sum(flags * scores[rows], axis=0, keepdims=True)
    loss_1[zc] = -2.0 * as_tile(target)
    for d in COLUMN:
        loss_1_copy(d).start()

    each(1, ZC, lambda d: lse_r_copy(d).wait_recv())
    total_r = combined(lse_r)
    turned = jnp.concatenate([total_r] * 32, axis=0).T
    each(1, XY, lambda d: lse_c_copy(d).wait_recv())
    total_c = combined(lse_c)
    line_c = jnp.concatenate([total_c[k : k + 1] for k in range(4)], axis=1)
    loss_3[zc] = total_c
    for d in COLUMN:
        loss_3_copy(d).start()
    for k, rows in enumerate(quarters):
        s = scores[rows]
        flags = (captions[k * 128 : (k + 1) * 128] == ids).astype(f32)
        w = scale * (jnp.exp(s - turned[:, k : k + 1]) + jnp.exp(s - line_c) - 2.0 * flags)
        weights[rows] = w.astype(bf16)
    each(1, ZC, lambda d: loss_1_copy(d).wait_recv())
    loss_2[xy] = total_r + jnp.sum(loss_1[...], axis=0)
    for d in PLANE:
        loss_2_copy(d).start()

    def grad_x(d):
        there = (x + d) % X
        return remote(txt_send.at[:, there, :, :HALF_E], sum_x.at[d], gx_s.at[d], gx_r.at[d], mp=there)

    def grad_y(d):
        there = (y + d) % Y
        return remote(txt_send.at[there, :, :, HALF_E:], sum_y.at[d], gy_s.at[d], gy_r.at[d], dp_0=there)

    def grad_xy(d):
        there = (y + d) % Y
        return remote(sent_x.at[there], sum_xy.at[d], gxy_s.at[d], gxy_r.at[d], dp_0=there)

    def grad_yx(d):
        there = (x + d) % X
        return remote(sent_y.at[there], sum_yx.at[d], gyx_s.at[d], gyx_r.at[d], mp=there)

    for k in range(4):
        cols = pl.ds(k * 128, 128)
        value = dot(weights[:, cols], ibuf[:, :HALF_E], ((0,), (0,)))
        txt_send[k, :, :, :HALF_E] = value.reshape(X, PIECE, HALF_E).astype(bf16)
    for d in RING:
        grad_x(d).start()
    d2d = remote(img_d2d, img_d2d_got, d2d_s, d2d_r, dp_2=1 - c)
    rows = pl.ds(pl.multiple_of((1 - c) * SIDE, SIDE), SIDE)
    img_d2d[...] = dot(weights[rows], tbuf[...]).astype(bf16)
    d2d.start()

    for k in range(4):
        cols = pl.ds(k * 128, 128)
        value = dot(weights[:, cols], ibuf[:, HALF_E:], ((0,), (0,)))
        txt_send[k, :, :, HALF_E:] = value.reshape(X, PIECE, HALF_E).astype(bf16)
    for d in RING:
        grad_y(d).start()

    def piece(index):
        return img_send.at[pl.ds(pl.multiple_of((z + index) % Z * PIECE, PIECE), PIECE)]

    def img_next(side):
        return remote(piece((1, 7)[side]), img_near.at[side], in_s.at[side], in_r.at[side], **along((1, 7)[side]))

    def img_third(side):
        return remote(piece((3, 5)[side]), img_third_got.at[side], i3_s.at[side], i3_r.at[side], **along((1, 7)[side]))

    def img_fourth(side):
        start = (z + 4) % Z * PIECE + side * (PIECE // 2)
        part = img_send.at[pl.ds(pl.multiple_of(start, 16), PIECE // 2)]
        return remote(part, img_fourth_got.at[side], i4_s.at[side], i4_r.at[side], **along((2, 6)[side]))

    def img_second(side):
        return remote(img_sum.at[side], img_far.at[side], if_s.at[side], if_r.at[side], **along((2, 6)[side]))

    rows = pl.ds(pl.multiple_of(c * SIDE, SIDE), SIDE)
    value = dot(weights[rows], tbuf[...])
    d2d.wait_recv()
    value = value + img_d2d_got[...].astype(f32)
    img_send[...] = value.astype(bf16)
    for send in (img_fourth, img_third, img_next):
        send(0).start()
        send(1).start()

    def sent_ring(d):
        stat_copy(d).wait_send()
        share_t(d).wait_send()
        share_i(d).wait_send()
        text_x(d).wait_send()
        text_y(d).wait_send()
        for e in range(1, X):
            text_xy(d, e).wait_send()
            text_yx(d, e).wait_send()

    def sent_all(d):
        lse_r_copy(d).wait_send()
        lse_c_copy(d).wait_send()
        loss_1_copy(d).wait_send()
        loss_3_copy(d).wait_send()

    each(1, X, sent_ring)
    for d in (1, 2, 6, 7):
        image_copy(d).wait_send()
    image_on(3).wait_send()
    image_on(5).wait_send()
    image_half(0).wait_send()
    image_half(1).wait_send()
    each(0, Z, lambda d: forward(d).wait_send())
    each(1, XY, sent_all)
    d2d.wait_send()

    def image_rows(index, start, count):
        return img_send[pl.ds(pl.multiple_of((z + index) % Z * PIECE + start, 16), count)].astype(f32)

    for side in range(2):
        img_fourth(side).wait_recv()
        img_third(side).wait_recv()
        for part in range(2):
            rows = pl.ds(part * (PIECE // 2), PIECE // 2)
            value = image_rows((2, 6)[side], part * (PIECE // 2), PIECE // 2) + img_third_got[side, rows].astype(f32)
            if part == side:
                value = value + img_fourth_got[side].astype(f32)
            img_sum[side, rows] = value.astype(bf16)
        img_second(side).start()

    each(1, X, lambda d: grad_x(d).wait_recv())
    for k in range(Y):
        value = txt_send[k, x, :, :HALF_E].astype(f32)
        for d in range(1, X):
            value = value + sum_x[d, k].astype(f32)
        sent_x[k] = value.astype(bf16)
    for d in RING:
        grad_xy(d).start()
    each(1, Y, lambda d: grad_y(d).wait_recv())
    for k in range(X):
        value = txt_send[y, k, :, HALF_E:].astype(f32)
        for d in range(1, Y):
            value = value + sum_y[d, k].astype(f32)
        sent_y[k] = value.astype(bf16)
    for d in RING:
        grad_yx(d).start()
    def last(part):
        cols = pl.ds(part * HALF_E, HALF_E)
        return remote(fin.at[:, cols], fin_got.at[:, cols], fin_s.at[part], fin_r.at[part], group=1 - zl)

    mine = pl.ds(pl.multiple_of(zl * PIECE, PIECE), PIECE)
    theirs = pl.ds(pl.multiple_of((1 - zl) * PIECE, PIECE), PIECE)
    store = pltpu.make_async_copy(result.at[mine], out.at[0, mine], store_sem.at[0])
    store_theirs = pltpu.make_async_copy(result.at[theirs], out.at[0, theirs], store_sem.at[1])

    def finished_text(part, value):
        cols = pl.ds(part * HALF_E, HALF_E)

        @pl.when(zl == 0)
        def _():
            fin[:, cols] = value.astype(bf16)
            last(part).start()

        @pl.when(zl == 1)
        def _():
            result[PIECE:, cols] = value

    each(1, Y, lambda d: grad_xy(d).wait_recv())
    value = sent_x[y].astype(f32)
    for d in range(1, Y):
        value = value + sum_xy[d].astype(f32)
    finished_text(0, value)
    each(1, X, lambda d: grad_yx(d).wait_recv())
    value = sent_y[x].astype(f32)
    for d in range(1, X):
        value = value + sum_yx[d].astype(f32)
    finished_text(1, value)

    value = image_rows(0, 0, PIECE)
    for side in range(2):
        img_next(side).wait_recv()
        value = value + img_near[side].astype(f32)
    for side in range(2):
        img_second(side).wait_recv()
        value = value + img_far[side].astype(f32)

    @pl.when(zl == 0)
    def _():
        result[:PIECE] = value

    @pl.when(zl == 1)
    def _():
        fin[...] = value.astype(bf16)
        last(0).start()
        last(1).start()

    store.start()
    for side in range(2):
        img_next(side).wait_send()
        img_third(side).wait_send()
        img_fourth(side).wait_send()
    each(1, X, lambda d: grad_x(d).wait_send())
    each(1, X, lambda d: grad_y(d).wait_send())
    each(1, XY, lambda d: loss_2_copy(d).wait_recv())
    each(1, ZC, lambda d: loss_3_copy(d).wait_recv())
    total = jnp.sum(jnp.sum(loss_2[...], axis=0) + jnp.sum(loss_3[...], axis=0), axis=0, keepdims=True)
    loss_ref[...] = jnp.sum(total, axis=1, keepdims=True) * (1.0 / (2 * XY * BLOCK))
    store_loss = pltpu.make_async_copy(loss_ref, loss_out, store_sem.at[2])
    store_loss.start()
    last(0).wait_recv()
    last(1).wait_recv()
    result[theirs] = fin_got[...].astype(f32)
    store_theirs.start()

    each(1, XY, lambda d: loss_2_copy(d).wait_send())
    each(1, X, lambda d: grad_xy(d).wait_send())
    each(1, X, lambda d: grad_yx(d).wait_send())
    for side in range(2):
        img_second(side).wait_send()
        last(side).wait_send()
    store.wait()
    store_loss.wait()
    store_theirs.wait()


def body(
    image_features, text_features, image_gain, text_gain, image_proj, text_proj, pair, logit_scale
):
    width_i, width_t = image_features.shape[1], text_features.shape[1]
    emb = image_proj.shape[1]
    hbm = pl.BlockSpec(memory_space=pl.ANY)
    dma = lambda *n: pltpu.SemaphoreType.DMA(n)
    grads, loss = pl.pallas_call(
        kernel,
        out_shape=(
            jax.ShapeDtypeStruct((1, ROWS, emb), f32),
            jax.ShapeDtypeStruct((1, 1), f32),
        ),
        in_specs=[hbm] * 8,
        out_specs=(hbm, hbm),
        scratch_shapes=[
            pltpu.VMEM((1, 1), f32),
            pltpu.VMEM((ROWS, emb), f32),
            pltpu.VMEM((1, 1), f32),
            pltpu.VMEM((HALF, width_i), bf16),
            pltpu.VMEM((HALF, width_t), bf16),
            pltpu.VMEM((width_i // 128, 128), f32),
            pltpu.VMEM((width_t // 128, 128), f32),
            pltpu.VMEM((pair.size // 128, 128), jnp.int32),
            pltpu.VMEM((width_i, emb), bf16),
            pltpu.VMEM((width_t, emb), bf16),
            pltpu.VMEM((HALF + 16, width_i), bf16),
            pltpu.VMEM((HALF + 16, width_t), bf16),
            pltpu.VMEM((X, 24, 128), f32),
            pltpu.VMEM((128, 128), f32),
            pltpu.VMEM((HALF, emb), bf16),
            pltpu.VMEM((HALF, emb), bf16),
            pltpu.VMEM((HALF, emb), f32),
            pltpu.VMEM((HALF, emb), f32),
            pltpu.VMEM((X, PIECE, emb), bf16),
            pltpu.VMEM((X, PIECE, emb), bf16),
            pltpu.VMEM((BLOCK, emb), bf16),
            pltpu.VMEM((BLOCK, emb), bf16),
            pltpu.VMEM((BLOCK, BLOCK), f32),
            pltpu.VMEM((BLOCK, BLOCK), bf16),
            pltpu.VMEM((ZC, 4, 128), f32),
            pltpu.VMEM((XY, 4, 128), f32),
            pltpu.VMEM((ZC, 4, 128), f32),
            pltpu.VMEM((XY, 4, 128), f32),
            pltpu.VMEM((ZC, 4, 128), f32),
            pltpu.VMEM((SIDE, emb), bf16),
            pltpu.VMEM((SIDE, emb), bf16),
            pltpu.VMEM((SIDE, emb), bf16),
            pltpu.VMEM((2, PIECE, emb), bf16),
            pltpu.VMEM((2, PIECE, emb), bf16),
            pltpu.VMEM((2, PIECE // 2, emb), bf16),
            pltpu.VMEM((2, PIECE, emb), bf16),
            pltpu.VMEM((2, PIECE, emb), bf16),
            pltpu.VMEM((Y, X, PIECE, emb), bf16),
            pltpu.VMEM((X, Y, PIECE, HALF_E), bf16),
            pltpu.VMEM((Y, X, PIECE, HALF_E), bf16),
            pltpu.VMEM((Y, PIECE, HALF_E), bf16),
            pltpu.VMEM((X, PIECE, HALF_E), bf16),
            pltpu.VMEM((Y, PIECE, HALF_E), bf16),
            pltpu.VMEM((X, PIECE, HALF_E), bf16),
            pltpu.VMEM((PIECE, emb), bf16),
            pltpu.VMEM((PIECE, emb), bf16),
            dma(2 * X + 6), dma(3),
            dma(X), dma(X), dma(X), dma(X), dma(X), dma(X),
            dma(Z), dma(Z), dma(2), dma(2), dma(Z), dma(Z), dma(X), dma(X), dma(Y), dma(Y),
            dma(XY), dma(XY), dma(XY), dma(XY),
            dma(ZC), dma(ZC), dma(XY), dma(XY), dma(ZC), dma(ZC), dma(XY), dma(XY), dma(ZC), dma(ZC),
            pltpu.SemaphoreType.DMA, pltpu.SemaphoreType.DMA,
            dma(2), dma(2), dma(2), dma(2), dma(2), dma(2), dma(2), dma(2),
            dma(X), dma(X), dma(Y), dma(Y), dma(Y), dma(Y), dma(X), dma(X),
            dma(2), dma(2),
        ],
        compiler_params=pltpu.CompilerParams(
            collective_id=0, has_side_effects=True, vmem_limit_bytes=67043328
        ),
        name="contrastive",
    )(
        image_features, text_features, image_gain.reshape(-1, 128), text_gain.reshape(-1, 128),
        image_proj, text_proj, pair.reshape(-1, 128), logit_scale.reshape(1, 1),
    )
    return grads, loss.reshape(())


def solution(mesh):
    split = Mesh(
        mesh.devices.reshape(mesh.shape["group"], 4, 4, 2, mesh.shape["mp"]),
        ("group", "dp_0", "dp_1", "dp_2", "mp"),
    )
    placed = (P(DP, "mp"), P(DP, "mp"), P("mp"), P("mp"), P("mp", None), P("mp", None), P(), P())
    return jax.shard_map(
        body, mesh=split, in_specs=placed, out_specs=(P("group", DP_MP, None), P()), check_vma=False
    )
```
